128 devices in a mesh: sp: 16 (over z, y), dp: 8 (over x, core).
Axes of the slice: x: 4, y: 4, z: 4, core: 2. Of those that a mesh axis runs over, the one named last changes fastest.
Arguments:
- node_lat: bfloat16 [32, 4096, 256], P('dp', 'sp')
- edge_lat: bfloat16 [32, 24576, 256], P('dp', 'sp')
- senders: int32 [24576], P('sp')
- edge_mask: int32 [24576], P('sp')
- node_cot: bfloat16 [32, 4096, 256], P('dp', 'sp')
- edge_cot: bfloat16 [32, 24576, 256], P('dp', 'sp')
- w_edge1: float32 [2, 768, 256], P(None, 'dp')
- w_edge2: float32 [2, 256, 256], P(None, 'dp')
- w_node1: float32 [2, 512, 256], P(None, 'dp')
- w_node2: float32 [2, 256, 256], P(None, 'dp')
- norm_par: float32 [2, 4, 256], P(None, None, 'dp')
- mom_edge1: float32 [2, 768, 256], P(None, 'dp')
- mom_edge2: float32 [2, 256, 256], P(None, 'dp')
- mom_node1: float32 [2, 512, 256], P(None, 'dp')
- mom_node2: float32 [2, 256, 256], P(None, 'dp')
- mom_norm: float32 [2, 4, 256], P(None, None, 'dp')
- vel_edge1: float32 [2, 768, 256], P(None, 'dp')
- vel_edge2: float32 [2, 256, 256], P(None, 'dp')
- vel_node1: float32 [2, 512, 256], P(None, 'dp')
- vel_node2: float32 [2, 256, 256], P(None, 'dp')
- vel_norm: float32 [2, 4, 256], P(None, None, 'dp')
Outputs:
- output 1: float32 [2, 768, 256], P(None, 'dp')
- output 2: float32 [2, 256, 256], P(None, 'dp')
- output 3: float32 [2, 512, 256], P(None, 'dp')
- output 4: float32 [2, 256, 256], P(None, 'dp')
- output 5: float32 [2, 4, 256], P(None, None, 'dp')
- output 6: float32 [2, 768, 256], P(None, 'dp')
- output 7: float32 [2, 256, 256], P(None, 'dp')
- output 8: float32 [2, 512, 256], P(None, 'dp')
- output 9: float32 [2, 256, 256], P(None, 'dp')
- output 10: float32 [2, 4, 256], P(None, None, 'dp')
- output 11: float32 [2, 768, 256], P(None, 'dp')
- output 12: float32 [2, 256, 256], P(None, 'dp')
- output 13: float32 [2, 512, 256], P(None, 'dp')
- output 14: float32 [2, 256, 256], P(None, 'dp')
- output 15: float32 [2, 4, 256], P(None, None, 'dp')
- output 16: bfloat16 [32, 4096, 256], P('dp', 'sp')
- output 17: bfloat16 [32, 24576, 256], P('dp', 'sp')
All inputs are finite; a program needn't handle non-finite values.
Results may differ from the reference program's by a relative error of at most 0.02.
Values are sent between devices in bfloat16 or wider.
A program may use at most 1 GiB of HBM per device.

```python
import jax
import jax.numpy as jnp
from jax import lax

BATCH = 32
TILES = 16
NODES_TILE = 256
DEG = 6
LATENT = 256
HIDDEN = 256
LAYERS = 2
STEP = 10
NODES = TILES * NODES_TILE
EDGES = NODES * DEG
LEARN_RATE = 1e-3
BETA_ONE = 0.9
BETA_TWO = 0.95
ADAM_EPS = 1e-8
DECAY = 0.1
NORM_EPS = 1e-5


def draw_senders(base_key):
    share_key, coin_key, shift_key, local_key = jax.random.split(base_key, 4)
    tile_edges = NODES_TILE * DEG
    share_num = jax.random.randint(share_key, (TILES, 1), 1, 8)
    coin_draw = jax.random.randint(coin_key, (TILES, tile_edges), 0, 16)
    remote = (coin_draw < share_num).astype(jnp.int32)
    tile_shift = jax.random.randint(shift_key, (TILES, tile_edges), 1, TILES)
    own_tile = jnp.arange(TILES, dtype=jnp.int32)[:, None]
    src_tile = (own_tile + remote * tile_shift) % TILES
    local_id = jax.random.randint(local_key, (TILES, tile_edges), 0, NODES_TILE)
    sender_ids = (src_tile * NODES_TILE + local_id).reshape(EDGES).astype(jnp.int32)
    return sender_ids.at[0].set(NODES - 1).at[EDGES - 1].set(0)


def setup_inputs(seed: int = 0) -> dict:
    sub_keys = jax.random.split(jax.random.key(seed), 24)
    lat_shape = (BATCH, NODES, LATENT)
    edge_shape = (BATCH, EDGES, LATENT)
    node_lat = jax.random.normal(sub_keys[0], lat_shape, jnp.float32).astype(jnp.bfloat16)
    edge_lat = jax.random.normal(sub_keys[1], edge_shape, jnp.float32).astype(jnp.bfloat16)
    senders = draw_senders(sub_keys[2])
    edge_mask = (jax.random.randint(sub_keys[3], (EDGES,), 0, 8) != 0).astype(jnp.int32)
    node_cot = jax.random.normal(sub_keys[4], lat_shape, jnp.float32).astype(jnp.bfloat16)
    edge_cot = jax.random.normal(sub_keys[5], edge_shape, jnp.float32).astype(jnp.bfloat16)
    mat_shapes = [(LAYERS, 3 * LATENT, HIDDEN), (LAYERS, HIDDEN, LATENT), (LAYERS, 2 * LATENT, HIDDEN), (LAYERS, HIDDEN, LATENT)]
    masters = [jax.random.normal(sub_keys[6 + slot], mat_shape, jnp.float32) * mat_shape[1] ** -0.5 for slot, mat_shape in enumerate(mat_shapes)]
    norm_base = jnp.array([1.0, 0.0, 1.0, 0.0], jnp.float32)[None, :, None]
    masters.append(norm_base + 0.2 * jax.random.normal(sub_keys[10], (LAYERS, 4, LATENT), jnp.float32))
    edge_rows = float(BATCH * EDGES)
    node_rows = float(BATCH * NODES)
    norm_rows = jnp.array([edge_rows, edge_rows, node_rows, node_rows], jnp.float32)[None, :, None]
    row_counts = [edge_rows, edge_rows, node_rows, node_rows, norm_rows]
    moments_one = [0.1 * jnp.sqrt(row_counts[slot]) * jax.random.normal(sub_keys[11 + slot], masters[slot].shape, jnp.float32) for slot in range(5)]
    moments_two = [0.1 * row_counts[slot] * jax.random.uniform(sub_keys[16 + slot], masters[slot].shape, jnp.float32, 0.5, 1.5) for slot in range(5)]
    return dict(node_lat=node_lat, edge_lat=edge_lat, senders=senders, edge_mask=edge_mask, node_cot=node_cot, edge_cot=edge_cot, w_edge1=masters[0], w_edge2=masters[1], w_node1=masters[2], w_node2=masters[3], norm_par=masters[4], mom_edge1=moments_one[0], mom_edge2=moments_one[1], mom_node1=moments_one[2], mom_node2=moments_one[3], mom_norm=moments_one[4], vel_edge1=moments_two[0], vel_edge2=moments_two[1], vel_node1=moments_two[2], vel_node2=moments_two[3], vel_norm=moments_two[4])


def snap_bf16(values):
    return values.astype(jnp.bfloat16).astype(jnp.float32)


def layer_norm(values, norm_gain, norm_bias):
    row_mean = jnp.mean(values, axis=-1, keepdims=True)
    centered = values - row_mean
    row_var = jnp.mean(centered * centered, axis=-1, keepdims=True)
    return centered * lax.rsqrt(row_var + NORM_EPS) * norm_gain + norm_bias


def mlp_branch(features, w_one, w_two, norm_gain, norm_bias):
    pre_act = snap_bf16(jnp.dot(features, w_one, preferred_element_type=jnp.float32))
    hidden_act = snap_bf16(jax.nn.silu(pre_act))
    out_b = snap_bf16(jnp.dot(hidden_act, w_two, preferred_element_type=jnp.float32))
    return layer_norm(out_b, norm_gain, norm_bias)


def processor_layer(layer_carry, layer_wts, senders, mask_f):
    node_x, edge_x = layer_carry
    w_e1, w_e2, w_n1, w_n2, norm_rows = layer_wts
    sender_lat = jnp.take(node_x, senders, axis=0)
    recv_lat = jnp.repeat(node_x, DEG, axis=0)
    edge_in = jnp.concatenate([edge_x, sender_lat, recv_lat], axis=1)
    edge_new = snap_bf16(edge_x + mlp_branch(edge_in, w_e1, w_e2, norm_rows[0], norm_rows[1]))
    node_sum = snap_bf16(jnp.sum((edge_new * mask_f[:, None]).reshape(NODES, DEG, LATENT), axis=1))
    node_in = jnp.concatenate([node_x, node_sum], axis=1)
    node_new = snap_bf16(node_x + mlp_branch(node_in, w_n1, w_n2, norm_rows[2], norm_rows[3]))
    return node_new, edge_new


def sample_objective(all_wts, node_b, edge_b, node_g, edge_g, senders, mask_f):
    def layer_step(layer_carry, layer_wts):
        return processor_layer(layer_carry, layer_wts, senders, mask_f), None
    final_carry, _ = lax.scan(layer_step, (node_b.astype(jnp.float32), edge_b.astype(jnp.float32)), all_wts)
    node_out, edge_out = final_carry
    return jnp.sum(node_out * node_g.astype(jnp.float32)) + jnp.sum(edge_out * edge_g.astype(jnp.float32))


def adamw_update(master, grad_sum, moment_one, moment_two):
    corr_one = 1.0 - BETA_ONE ** STEP
    corr_two = 1.0 - BETA_TWO ** STEP
    one_new = BETA_ONE * moment_one + (1.0 - BETA_ONE) * grad_sum
    two_new = BETA_TWO * moment_two + (1.0 - BETA_TWO) * grad_sum * grad_sum
    direction = (one_new / corr_one) / (jnp.sqrt(two_new / corr_two) + ADAM_EPS)
    return master - LEARN_RATE * (direction + DECAY * master), one_new, two_new


def reference(node_lat, edge_lat, senders, edge_mask, node_cot, edge_cot, w_edge1, w_edge2, w_node1, w_node2, norm_par, mom_edge1, mom_edge2, mom_node1, mom_node2, mom_norm, vel_edge1, vel_edge2, vel_node1, vel_node2, vel_norm):
    masters = (w_edge1, w_edge2, w_node1, w_node2, norm_par)
    moments_one = (mom_edge1, mom_edge2, mom_node1, mom_node2, mom_norm)
    moments_two = (vel_edge1, vel_edge2, vel_node1, vel_node2, vel_norm)
    compute = tuple(snap_bf16(master) for master in masters)
    mask_f = edge_mask.astype(jnp.float32)

    def per_sample(grad_total, sample):
        node_b, edge_b, node_g, edge_g = sample

        def objective(all_wts, node_in, edge_in):
            return sample_objective(all_wts, node_in, edge_in, node_g, edge_g, senders, mask_f)
        _, pullback = jax.vjp(objective, compute, node_b, edge_b)
        d_wts, d_node, d_edge = pullback(jnp.ones((), jnp.float32))
        grad_total = tuple(run_sum + part for run_sum, part in zip(grad_total, d_wts))
        return grad_total, (d_node, d_edge)

    zero_grads = tuple(jnp.zeros_like(weight) for weight in compute)
    grads, sample_grads = lax.scan(per_sample, zero_grads, (node_lat, edge_lat, node_cot, edge_cot))
    new_state = [adamw_update(masters[slot], grads[slot], moments_one[slot], moments_two[slot]) for slot in range(5)]
    return (new_state[0][0], new_state[1][0], new_state[2][0], new_state[3][0], new_state[4][0], new_state[0][1], new_state[1][1], new_state[2][1], new_state[3][1], new_state[4][1], new_state[0][2], new_state[1][2], new_state[2][2], new_state[3][2], new_state[4][2], sample_grads[0], sample_grads[1])
```

```python
import functools

import jax
import jax.numpy as jnp
from jax import lax
from jax.experimental import pallas as pl
from jax.experimental.pallas import tpu as pltpu
from jax.sharding import PartitionSpec as P

NORM_EPS = 1e-5
LEARN_RATE = 1e-3
BETA_ONE = 0.9
BETA_TWO = 0.95
ADAM_EPS = 1e-8
DECAY = 0.1
STEP = 10

BF = jnp.bfloat16
F32 = jnp.float32
SLOTS = 80
MESH_ID = pl.DeviceIdType.MESH


def ring_gap(offset, count):
    return min(offset % count, -offset % count)


def far_first(tiles):
    side = int(tiles ** 0.5)
    return sorted(range(1, tiles), key=lambda offset: -ring_gap(offset // side, side) - ring_gap(offset, side))


def line_first(count):
    return sorted(range(1, count), key=lambda offset: -ring_gap(offset, count))

LANES = 128
SHARD_ROWS = (96, 32, 64, 32)
SHARD_OFF = (0, 96, 128, 192)
NORM_OFF = 224
PART_ROWS = 240
FULL_ROWS = 256
GRAD_ROWS = 1800


def contract(left_op, right_op, left_dims, right_dims):
    return lax.dot_general(left_op, right_op, ((left_dims, right_dims), ((), ())), preferred_element_type=jnp.float32)


def norm_forward(out_b, norm_gain, norm_bias):
    values = out_b.astype(jnp.float32)
    centered = values - jnp.mean(values, axis=-1, keepdims=True)
    inv_std = lax.rsqrt(jnp.mean(centered * centered, axis=-1, keepdims=True) + NORM_EPS)
    normed = centered * inv_std
    return normed * norm_gain + norm_bias, normed, inv_std


def mlp_tail(pre_act, w_two, norm_gain, norm_bias):
    pre_b = pre_act.astype(jnp.bfloat16)
    hidden_act = jax.nn.silu(pre_b.astype(jnp.float32)).astype(jnp.bfloat16)
    last_dim = hidden_act.ndim - 1
    out_b = contract(hidden_act, w_two, (last_dim,), (0,)).astype(jnp.bfloat16)
    branch, normed, inv_std = norm_forward(out_b, norm_gain, norm_bias)
    return branch, (pre_b, hidden_act, normed, inv_std)


def mlp_back(d_branch, saved, w_one, w_two, norm_gain):
    pre_b, hidden_act, normed, inv_std = saved
    last_dim = hidden_act.ndim - 1
    lead_dims = tuple(range(last_dim))
    d_gain = jnp.sum(d_branch * normed, axis=lead_dims)
    d_bias = jnp.sum(d_branch, axis=lead_dims)
    d_norm = d_branch * norm_gain
    d_out = (inv_std * (d_norm - jnp.mean(d_norm, axis=-1, keepdims=True) - normed * jnp.mean(d_norm * normed, axis=-1, keepdims=True))).astype(jnp.bfloat16)
    d_two = contract(hidden_act, d_out, lead_dims, lead_dims)
    d_act = contract(d_out, w_two, (last_dim,), (1,)).astype(jnp.bfloat16)
    pre_f = pre_b.astype(jnp.float32)
    gate_sig = jax.nn.sigmoid(pre_f)
    d_pre = (d_act.astype(jnp.float32) * gate_sig * (1.0 + pre_f * (1.0 - gate_sig))).astype(jnp.bfloat16)
    d_in = contract(d_pre, w_one, (last_dim,), (1,))
    return d_pre, d_in, d_two, d_gain, d_bias


def layer_forward(node_x, node_all, edge_x, senders, mask_b, layer_wts):
    w_e1, w_e2, w_n1, w_n2, norm_rows = layer_wts
    lat_width = node_x.shape[-1]
    sender_lat = jnp.take(node_all, senders, axis=1).reshape(edge_x.shape)
    pre_e = (contract(edge_x, w_e1[:lat_width], (3,), (0,))
             + contract(sender_lat, w_e1[lat_width:2 * lat_width], (3,), (0,))
             + contract(node_x, w_e1[2 * lat_width:], (2,), (0,))[:, :, None, :])
    branch_e, saved_e = mlp_tail(pre_e, w_e2, norm_rows[0], norm_rows[1])
    edge_new = (edge_x.astype(jnp.float32) + branch_e).astype(jnp.bfloat16)
    node_sum = jnp.einsum('bngd,ng->bnd', edge_new, mask_b, preferred_element_type=jnp.float32).astype(jnp.bfloat16)
    pre_n = contract(node_x, w_n1[:lat_width], (2,), (0,)) + contract(node_sum, w_n1[lat_width:], (2,), (0,))
    branch_n, saved_n = mlp_tail(pre_n, w_n2, norm_rows[2], norm_rows[3])
    node_new = (node_x.astype(jnp.float32) + branch_n).astype(jnp.bfloat16)
    return node_new, edge_new, (sender_lat, node_sum, saved_e, saved_n)


def layer_backward(d_node_new, d_edge_new, node_x, edge_x, senders, mask_f, saved, layer_wts, total_nodes):
    w_e1, w_e2, w_n1, w_n2, norm_rows = layer_wts
    sender_lat, node_sum, saved_e, saved_n = saved
    batch_size, tile_nodes, degree, lat_width = edge_x.shape
    d_res_n = d_node_new.astype(jnp.float32)
    d_pre_n, d_in_n, d_wn2, d_gain_n, d_bias_n = mlp_back(d_res_n, saved_n, w_n1, w_n2, norm_rows[2])
    d_wn1 = jnp.concatenate([contract(node_x, d_pre_n, (0, 1), (0, 1)), contract(node_sum, d_pre_n, (0, 1), (0, 1))], axis=0)
    d_sum = d_in_n[..., lat_width:].astype(jnp.bfloat16)
    d_res_e = (d_edge_new.astype(jnp.float32) + d_sum.astype(jnp.float32)[:, :, None, :] * mask_f[None, :, :, None]).astype(jnp.bfloat16).astype(jnp.float32)
    d_pre_e, d_in_e, d_we2, d_gain_e, d_bias_e = mlp_back(d_res_e, saved_e, w_e1, w_e2, norm_rows[0])
    recv_grad = contract(node_x, d_pre_e.reshape(batch_size, tile_nodes, -1), (0, 1), (0, 1))
    d_we1 = jnp.concatenate([contract(edge_x, d_pre_e, (0, 1, 2), (0, 1, 2)), contract(sender_lat, d_pre_e, (0, 1, 2), (0, 1, 2)), recv_grad.reshape(lat_width, degree, -1).sum(axis=1)], axis=0)
    d_edge_x = (d_res_e + d_in_e[..., :lat_width]).astype(jnp.bfloat16)
    d_sender = d_in_e[..., lat_width:2 * lat_width].reshape(batch_size, tile_nodes * degree, lat_width)
    scattered = jnp.zeros((batch_size, total_nodes, lat_width), jnp.float32).at[:, senders].add(d_sender)
    d_local = d_res_n + d_in_n[..., :lat_width] + d_in_e[..., 2 * lat_width:].sum(axis=2)
    grads = (d_we1, d_we2, d_wn1, d_wn2, jnp.stack([d_gain_e, d_bias_e, d_gain_n, d_bias_n]))
    return d_local, scattered, d_edge_x, grads


def adamw_update(master, grad_sum, moment_one, moment_two):
    corr_one = 1.0 - BETA_ONE ** STEP
    corr_two = 1.0 - BETA_TWO ** STEP
    one_new = BETA_ONE * moment_one + (1.0 - BETA_ONE) * grad_sum
    two_new = BETA_TWO * moment_two + (1.0 - BETA_TWO) * grad_sum * grad_sum
    direction = (one_new / corr_one) / (jnp.sqrt(two_new / corr_two) + ADAM_EPS)
    return master - LEARN_RATE * (direction + DECAY * master), one_new, two_new


def dot_nn(left_op, right_op):
    return lax.dot_general(left_op, right_op, (((1,), (0,)), ((), ())), preferred_element_type=F32)


def dot_nt(left_op, right_op):
    return lax.dot_general(left_op, right_op, (((1,), (1,)), ((), ())), preferred_element_type=F32)


def dot_tn(left_op, right_op):
    return lax.dot_general(left_op, right_op, (((0,), (0,)), ((), ())), preferred_element_type=F32)


def split_three(values):
    high = values.astype(BF)
    rest = values - high.astype(F32)
    mid = rest.astype(BF)
    low = (rest - mid.astype(F32)).astype(BF)
    return high, mid, low


def to_bf(cond):
    return jnp.where(cond, 1.0, 0.0).astype(BF)


def onehot_cols(col_ids, first, width):
    rows = col_ids.shape[0]
    lane = lax.broadcasted_iota(jnp.int32, (rows, LANES), 1)
    parts = [to_bf(col_ids == lane + (first + LANES * i)) for i in range(width // LANES)]
    return jnp.concatenate(parts, axis=1)


def onehot_rows(row_ids, first, height):
    width = row_ids.shape[1]
    sub = lax.broadcasted_iota(jnp.int32, (height, width), 0) + first
    return to_bf(row_ids == sub)


def norm_parts(out_b):
    values = out_b.astype(F32)
    centered = values - jnp.mean(values, axis=-1, keepdims=True)
    inv_std = lax.rsqrt(jnp.mean(centered * centered, axis=-1, keepdims=True) + NORM_EPS)
    return centered * inv_std, inv_std


def branch_forward(pre_act, w_two, gain, bias):
    pre_b = pre_act.astype(BF)
    pre_f = pre_b.astype(F32)
    sig = jax.nn.sigmoid(pre_f)
    act = (pre_f * sig).astype(BF)
    out_b = dot_nn(act, w_two).astype(BF)
    normed, inv_std = norm_parts(out_b)
    return normed * gain + bias, (pre_b, act, sig, normed, inv_std, out_b)


def branch_backward(d_branch, pre_b, act, sig, normed, inv_std, w_two, gain):
    d_norm = d_branch * gain
    mean_one = jnp.mean(d_norm, axis=-1, keepdims=True)
    mean_two = jnp.mean(d_norm * normed, axis=-1, keepdims=True)
    d_out = (inv_std * (d_norm - mean_one - normed * mean_two)).astype(BF)
    d_two = dot_tn(act, d_out)
    d_act = dot_nt(d_out, w_two).astype(BF)
    pre_f = pre_b.astype(F32)
    d_pre = (d_act.astype(F32) * sig * (1.0 + pre_f * (1.0 - sig))).astype(BF)
    d_gain = jnp.sum(d_branch * normed, axis=0, keepdims=True)
    d_bias = jnp.sum(d_branch, axis=0, keepdims=True)
    return d_pre, d_two, d_gain, d_bias


def load_weights(part_ref, wts, norm_ref):
    norm = jnp.zeros((PART_ROWS - NORM_OFF, norm_ref.shape[1]), F32)
    for shard in range(part_ref.shape[0]):
        for ref, rows, off in zip(wts, SHARD_ROWS, SHARD_OFF):
            ref[shard * rows:(shard + 1) * rows, :] = part_ref[shard, off:off + rows, :]
        norm += part_ref[shard, NORM_OFF:, :].astype(F32)
    norm_ref[...] = norm[:8]


def peer_tile(me, offset, side):
    row = lax.rem(me // side + offset // side, side)
    col = lax.rem(lax.rem(me, side) + offset % side, side)
    return row * side + col


def greet(peers):
    barrier = pltpu.get_barrier_semaphore()
    for peer in peers:
        pl.semaphore_signal(barrier, inc=1, device_id=peer, device_id_type=MESH_ID)


def greeted(count):
    pl.semaphore_wait(pltpu.get_barrier_semaphore(), count)


def tile_peers(tiles):
    me = lax.axis_index('sp')
    dp = lax.axis_index('dp')
    side = int(tiles ** 0.5)
    return [(peer_tile(me, offset, side), dp) for offset in far_first(tiles)]


def slot_copy(src_ref, dst_ref, sample, spot, send_sem, recv_sem, peer, me):
    return pltpu.make_async_remote_copy(src_ref=src_ref.at[peer[0], sample], dst_ref=dst_ref.at[me, sample], send_sem=send_sem.at[sample, spot], recv_sem=recv_sem.at[sample, spot], device_id=peer, device_id_type=MESH_ID)


def slots_start(src_ref, dst_ref, sample, send_sem, recv_sem, self_sem, tiles):
    me = lax.axis_index('sp')
    pltpu.make_async_copy(src_ref.at[me, sample], dst_ref.at[me, sample], self_sem.at[sample]).start()
    for spot, peer in enumerate(tile_peers(tiles)):
        slot_copy(src_ref, dst_ref, sample, spot, send_sem, recv_sem, peer, me).start()


def slots_wait(src_ref, dst_ref, sample, send_sem, recv_sem, self_sem, tiles):
    me = lax.axis_index('sp')
    pltpu.make_async_copy(src_ref.at[me, sample], dst_ref.at[me, sample], self_sem.at[sample]).wait()
    for spot, peer in enumerate(tile_peers(tiles)):
        slot_copy(src_ref, dst_ref, sample, spot, send_sem, recv_sem, peer, me).wait()


def slots_wait_all(src_ref, dst_ref, samples, send_sem, recv_sem, self_sem, tiles):
    def one(sample, carry):
        slots_wait(src_ref, dst_ref, sample, send_sem, recv_sem, self_sem, tiles)
        return carry
    lax.fori_loop(0, samples, one, 0)


def shard_peers(count):
    me = lax.axis_index('sp')
    dp = lax.axis_index('dp')
    return [(me, lax.rem(dp + offset, count)) for offset in line_first(count)]


def shard_copy(src_ref, dst_ref, spot, send_sem, recv_sem, peer, scatter):
    dp = lax.axis_index('dp')
    src = src_ref.at[peer[1]] if scatter else src_ref
    return pltpu.make_async_remote_copy(src_ref=src, dst_ref=dst_ref.at[dp], send_sem=send_sem.at[spot], recv_sem=recv_sem.at[spot], device_id=peer, device_id_type=MESH_ID)


def shards_start(src_ref, dst_ref, send_sem, recv_sem, self_sem, count, scatter):
    dp = lax.axis_index('dp')
    pltpu.make_async_copy(src_ref.at[dp] if scatter else src_ref, dst_ref.at[dp], self_sem).start()
    for spot, peer in enumerate(shard_peers(count)):
        shard_copy(src_ref, dst_ref, spot, send_sem, recv_sem, peer, scatter).start()


def shards_wait(src_ref, dst_ref, send_sem, recv_sem, self_sem, count, scatter):
    dp = lax.axis_index('dp')
    pltpu.make_async_copy(src_ref.at[dp] if scatter else src_ref, dst_ref.at[dp], self_sem).wait()
    for spot, peer in enumerate(shard_peers(count)):
        shard_copy(src_ref, dst_ref, spot, send_sem, recv_sem, peer, scatter).wait()


def chunk_maps(degree, mask_rows, mask_col):
    chunk = mask_rows.shape[1]
    nodes = chunk // degree
    sub_w = lax.broadcasted_iota(jnp.int32, (nodes, chunk), 0) * degree
    lane_w = lax.broadcasted_iota(jnp.int32, (nodes, chunk), 1)
    wide = (lane_w >= sub_w) & (lane_w < sub_w + degree)
    sub_t = lax.broadcasted_iota(jnp.int32, (chunk, nodes), 0)
    lane_t = lax.broadcasted_iota(jnp.int32, (chunk, nodes), 1) * degree
    tall = (sub_t >= lane_t) & (sub_t < lane_t + degree)
    out = dict(tall=to_bf(tall), wide=to_bf(wide), sum=jnp.where(wide, mask_rows[:1], 0.0).astype(BF))
    if mask_col is not None:
        out['spread'] = jnp.where(tall, jnp.concatenate([mask_col] * (nodes // LANES), axis=1), 0.0).astype(BF)
    return out


def make_tables(tiles, slots, tile_nodes, send_ids, mask_ref, node_ref, gcol_ref, grow_ref, nrow_ref, mcol_ref, pack_ref, out_ref):
    me = lax.axis_index('sp')
    ids = send_ids[...]
    edges = ids.shape[1]
    tile_of = ids // tile_nodes
    local = (ids - tile_of * tile_nodes).astype(F32)
    row = lax.broadcasted_iota(jnp.int32, (tiles, edges), 0)
    is_me = row == me
    own_tile = jnp.sum(jnp.where(is_me, tile_of, 0), axis=0, keepdims=True)
    own_local = jnp.sum(jnp.where(is_me, local, 0.0), axis=0, keepdims=True)
    own = jnp.where(own_tile == row, 1.0, 0.0)
    inc = jnp.where((tile_of == me) & jnp.logical_not(is_me), 1.0, 0.0)
    both = jnp.concatenate([own, inc], axis=0).astype(BF)
    rank = jnp.zeros((2 * tiles, edges), F32)
    step = 256
    for blk in range(edges // step):
        first = lax.broadcasted_iota(jnp.int32, (step, edges), 0) + blk * step
        second = lax.broadcasted_iota(jnp.int32, (step, edges), 1)
        rank += dot_nn(both[:, blk * step:(blk + 1) * step], to_bf(first < second))
    slot_id = jnp.where(is_me, own_local, rank[:tiles] + (row * slots + tile_nodes).astype(F32))
    gidx = jnp.sum(own * slot_id, axis=0, keepdims=True)
    grow_ref[...] = jnp.broadcast_to(gidx, grow_ref.shape).astype(jnp.int32)
    gcol_ref[...] = jnp.transpose(jnp.broadcast_to(gidx, (LANES, edges))).astype(jnp.int32)
    mcol_ref[...] = jnp.transpose(jnp.broadcast_to(mask_ref[0:1, :], (LANES, edges)))
    slot_row = lax.broadcasted_iota(jnp.int32, (slots, edges), 0).astype(F32)
    cols = []
    for peer in range(tiles):
        hit = (slot_row == rank[tiles + peer:tiles + peer + 1]) & (inc[peer:peer + 1] > 0.5)
        found = jnp.sum(jnp.where(hit, local[peer:peer + 1] + 1.0, 0.0), axis=1, keepdims=True) - 1.0
        cols.append(jnp.broadcast_to(found, (slots, LANES)))
    ncol_f = jnp.concatenate(cols, axis=0)
    ncol = ncol_f.astype(jnp.int32)
    nrow_ref[...] = jnp.transpose(ncol_f)[:8].astype(jnp.int32)
    group = 4
    for part in range(tiles // group):
        rows = group * slots
        pick = onehot_cols(ncol[part * rows:(part + 1) * rows], 0, tile_nodes)
        pack_ref[part * rows:(part + 1) * rows, :] = pick
        for sample in range(out_ref.shape[1]):
            got = dot_nn(pick, node_ref[sample]).astype(BF)
            out_ref[part * group:(part + 1) * group, sample] = got.reshape(group, slots, got.shape[1])


def fwd_sample(maps, v_c, e_c, pick_ref, rows_ref, wts, norm_ref):
    w_e1, w_e2, w_n1, w_n2 = wts
    width = e_c.shape[-1]
    w_edge, w_send, w_recv = (w_e1[i * width:(i + 1) * width, :] for i in range(w_e1.shape[0] // width))
    sent = dot_nn(pick_ref[...], rows_ref[...]).astype(BF)
    recv = dot_nn(maps['tall'], v_c).astype(BF)
    pre = dot_nn(e_c, w_edge) + dot_nn(sent, w_send) + dot_nn(recv, w_recv)
    rows = [norm_ref[i:i + 1, :] for i in range(len(SHARD_ROWS))]
    branch, edge_s = branch_forward(pre, w_e2[...], rows[0], rows[1])
    e_new = (e_c.astype(F32) + branch).astype(BF)
    sums = dot_nn(maps['sum'], e_new).astype(BF)
    pre_n = dot_nn(v_c, w_n1[:width, :]) + dot_nn(sums, w_n1[width:, :])
    branch_n, node_s = branch_forward(pre_n, w_n2[...], rows[2], rows[3])
    return e_new, sums, branch_n, edge_s, node_s


def fill_rows(rows_ref, node_ref, got, tile_nodes):
    rows_ref[:tile_nodes, :] = node_ref[0]
    rows_ref[tile_nodes:, :] = got.reshape(got.shape[0] * got.shape[1], got.shape[2])


def build_pick(gcol_ref, pick_ref):
    step = 128 * 3

    def build(i, carry):
        base = pl.multiple_of(i * step, step)
        pick_ref[pl.ds(base, step), :] = onehot_cols(gcol_ref[pl.ds(base, step), :], 0, pick_ref.shape[1])
        return carry
    lax.fori_loop(0, pick_ref.shape[0] // step, build, 0)


def ids_kernel(tiles, mine_ref, out_ref, send_sem, recv_sem):
    me = lax.axis_index('sp')
    peers = tile_peers(tiles)
    greet(peers)
    out_ref[me] = mine_ref[...]
    greeted(len(peers))
    copies = [pltpu.make_async_remote_copy(src_ref=mine_ref, dst_ref=out_ref.at[me], send_sem=send_sem.at[spot], recv_sem=recv_sem.at[spot], device_id=peer, device_id_type=MESH_ID) for spot, peer in enumerate(peers)]
    for copy in copies:
        copy.start()
    for copy in copies:
        copy.wait()


def open_kernel(cfg, shards, send_ids, mrow_ref, nodes_ref, node_ref, edge_ref, part_one, part_two,
                vout_ref, eout_ref, he_ref, ye_ref, sum_ref, hn_ref, yn_ref, gcol_ref, grow_ref, nrow_ref, mcol_ref, recv_out, gat_one, gat_two,
                pick_ref, pack_ref, rows_ref, out_buf, in_buf, next_buf, gat_buf, w_e1, w_e2, w_n1, w_n2, norm_ref,
                send_a, recv_a, self_a, send_b, recv_b, self_b, send_w, recv_w, self_w, send_x, recv_x, self_x, load_sem):
    tiles, slots, tile_nodes, degree = cfg
    edges = edge_ref.shape[1]
    samples = nodes_ref.shape[0]
    wts = (w_e1, w_e2, w_n1, w_n2)
    step = pl.program_id(0)

    @pl.when(step == 0)
    def _():
        peers = tile_peers(tiles) + shard_peers(shards)
        greet(peers)
        greeted(len(peers))
        shards_start(part_one, gat_one, send_w, recv_w, self_w, shards, False)
        shards_start(part_two, gat_two, send_x, recv_x, self_x, shards, False)
        make_tables(tiles, slots, tile_nodes, send_ids, mrow_ref, nodes_ref, gcol_ref, grow_ref, nrow_ref, mcol_ref, pack_ref, out_buf)
        for sample in range(samples):
            slots_start(out_buf, in_buf, sample, send_a, recv_a, self_a, tiles)
        build_pick(gcol_ref, pick_ref)
        shards_wait(part_one, gat_one, send_w, recv_w, self_w, shards, False)
        load = pltpu.make_async_copy(gat_one, gat_buf, load_sem)
        load.start()
        load.wait()
        load_weights(gat_buf, wts, norm_ref)

    slots_wait(out_buf, in_buf, step, send_a, recv_a, self_a, tiles)
    fill_rows(rows_ref, node_ref, in_buf[:, step], tile_nodes)

    node, edge = node_ref[0], edge_ref[0]
    e_new, sums, branch_n, edge_s, node_s = fwd_sample(chunk_maps(degree, mrow_ref[...], None), node, edge, pick_ref, rows_ref, wts, norm_ref)
    for ref, value in ((eout_ref, e_new), (he_ref, edge_s[0]), (ye_ref, edge_s[-1]), (sum_ref, sums), (hn_ref, node_s[0]), (yn_ref, node_s[-1]), (vout_ref, (node.astype(F32) + branch_n).astype(BF))):
        ref[0] = value

    def pack(i, carry):
        rows = 4 * slots
        base = pl.multiple_of(i * rows, rows)
        got = dot_nn(pack_ref[pl.ds(base, rows), :], vout_ref[0]).astype(BF)
        next_buf[pl.ds(i * 4, 4), step] = got.reshape(4, slots, got.shape[1])
        return carry
    lax.fori_loop(0, tiles // 4, pack, 0)
    slots_start(next_buf, recv_out, step, send_b, recv_b, self_b, tiles)

    @pl.when(step == samples - 1)
    def _():
        shards_wait(part_two, gat_two, send_x, recv_x, self_x, shards, False)
        slots_wait_all(next_buf, recv_out, samples, send_b, recv_b, self_b, tiles)


def back_sample(maps, v_c, e_c, sums, edge_s, node_s, dnode_ref, dedge_ref, wts, norm_ref, grad_ref, dpre_ref, de_ref, dloc_ref):
    w_e1, w_e2, w_n1, w_n2 = wts
    width = e_c.shape[-1]
    w_edge, w_send, w_recv = (w_e1[i * width:(i + 1) * width, :] for i in range(w_e1.shape[0] // width))
    d_node = dnode_ref[0].astype(F32)
    d_pre_n, d_wn2, d_gain_n, d_bias_n = branch_backward(d_node, *node_s, w_n2[...], norm_ref[2:3, :])
    d_in_v = dot_nt(d_pre_n, w_n1[:width, :])
    d_sum = dot_nt(d_pre_n, w_n1[width:, :]).astype(BF)
    d_res = (dedge_ref[0].astype(F32) + dot_nn(maps['spread'], d_sum)).astype(BF).astype(F32)
    d_pre, d_we2, d_gain_e, d_bias_e = branch_backward(d_res, *edge_s, w_e2[...], norm_ref[0:1, :])
    dpre_ref[...] = d_pre
    de_ref[0] = (d_res + dot_nt(d_pre, w_edge)).astype(BF)
    recv = split_three(dot_nn(maps['wide'], d_pre))
    dloc_ref[0] = d_node + d_in_v + sum(dot_nt(piece, w_recv) for piece in recv)
    blocks = [dot_tn(e_c, d_pre), None, sum(dot_tn(v_c, piece) for piece in recv), d_we2, dot_tn(v_c, d_pre_n), dot_tn(sums, d_pre_n), d_wn2]
    for i, block in enumerate(blocks):
        if block is not None:
            grad_ref[i * width:(i + 1) * width, :] += block
    rows = [d_gain_e, d_bias_e, d_gain_n, d_bias_n]
    grad_ref[len(blocks) * width:, :] += jnp.concatenate(rows + [jnp.zeros((len(rows), width), F32)], axis=0)


def back_pack(dpre_ref, drop_ref, sloc_ref, send_buf, step, tiles, slots, tile_nodes):
    sloc_ref[0] = dot_nn(drop_ref[:tile_nodes, :], dpre_ref[...])

    def pack(i, carry):
        rows = 4 * slots
        base = pl.multiple_of(tile_nodes + i * rows, 64)
        got = dot_nn(drop_ref[pl.ds(base, rows), :], dpre_ref[...]).astype(BF)
        send_buf[pl.ds(i * 4, 4), step] = got.reshape(4, slots, got.shape[1])
        return carry
    lax.fori_loop(0, tiles // 4, pack, 0)


def build_drop(grow_ref, drop_ref):
    step = 256

    def build(i, carry):
        base = pl.multiple_of(i * step, step)
        drop_ref[pl.ds(base, step), :] = onehot_rows(grow_ref[0:1, :], base, step)
        return carry
    lax.fori_loop(0, drop_ref.shape[0] // step, build, 0)


def turn_kernel(cfg, samples, node_ref, edge_ref, recv_ref, gcol_ref, grow_ref, mrow_ref, mcol_ref, gat_ref, dnode_ref, dedge_ref,
                de_ref, dloc_ref, sloc_ref, grad_ref, recv_out,
                pick_ref, drop_ref, rows_ref, dpre_ref, send_buf, w_e1, w_e2, w_n1, w_n2, norm_ref, send_b, recv_b, self_b):
    tiles, slots, tile_nodes, degree = cfg
    edges = edge_ref.shape[1]
    wts = (w_e1, w_e2, w_n1, w_n2)
    step = pl.program_id(0)

    @pl.when(step == 0)
    def _():
        greet(tile_peers(tiles))
        load_weights(gat_ref, wts, norm_ref)
        build_pick(gcol_ref, pick_ref)
        build_drop(grow_ref, drop_ref)
        grad_ref[...] = jnp.zeros_like(grad_ref)

    fill_rows(rows_ref, node_ref, recv_ref[:, 0], tile_nodes)

    maps = chunk_maps(degree, mrow_ref[...], mcol_ref[...])
    node, edge = node_ref[0], edge_ref[0]
    e_new, sums, branch_n, edge_s, node_s = fwd_sample(maps, node, edge, pick_ref, rows_ref, wts, norm_ref)
    back_sample(maps, node, edge, sums, edge_s[:-1], node_s[:-1], dnode_ref, dedge_ref, wts, norm_ref, grad_ref, dpre_ref, de_ref, dloc_ref)
    back_pack(dpre_ref, drop_ref, sloc_ref, send_buf, step, tiles, slots, tile_nodes)

    @pl.when(step == 0)
    def _():
        greeted(tiles - 1)
    slots_start(send_buf, recv_out, step, send_b, recv_b, self_b, tiles)

    @pl.when(step == samples - 1)
    def _():
        slots_wait_all(send_buf, recv_out, samples, send_b, recv_b, self_b, tiles)


def again(pre_b, out_b):
    pre_f = pre_b.astype(F32)
    sig = jax.nn.sigmoid(pre_f)
    act = (pre_f * sig).astype(BF)
    normed, inv_std = norm_parts(out_b)
    return pre_b, act, sig, normed, inv_std


def backward_kernel(cfg, samples, shards, node_ref, edge_ref, he_ref, ye_ref, sum_ref, hn_ref, yn_ref, grow_ref, mrow_ref, mcol_ref, gat_ref, dnode_ref, dedge_ref, full_ref,
                    de_ref, dloc_ref, sloc_ref, grad_ref, recv_out, part_out,
                    drop_ref, dpre_ref, send_buf, w_e1, w_e2, w_n1, w_n2, norm_ref, send_b, recv_b, self_b, send_w, recv_w, self_w):
    tiles, slots, tile_nodes, degree = cfg
    edges = edge_ref.shape[1]
    wts = (w_e1, w_e2, w_n1, w_n2)
    step = pl.program_id(0)

    @pl.when(step == 0)
    def _():
        greet(tile_peers(tiles) + shard_peers(shards))
        load_weights(gat_ref, wts, norm_ref)
        build_drop(grow_ref, drop_ref)
        grad_ref[...] = jnp.zeros_like(grad_ref)
        greeted(tiles - 1 + shards - 1)
        shards_start(full_ref, part_out, send_w, recv_w, self_w, shards, True)

    maps = chunk_maps(degree, mrow_ref[...], mcol_ref[...])
    edge_s = again(he_ref[0], ye_ref[0])
    node_s = again(hn_ref[0], yn_ref[0])
    back_sample(maps, node_ref[0], edge_ref[0], sum_ref[0], edge_s, node_s, dnode_ref, dedge_ref, wts, norm_ref, grad_ref, dpre_ref, de_ref, dloc_ref)
    back_pack(dpre_ref, drop_ref, sloc_ref, send_buf, step, tiles, slots, tile_nodes)
    slots_start(send_buf, recv_out, step, send_b, recv_b, self_b, tiles)

    @pl.when(step == samples - 1)
    def _():
        shards_wait(full_ref, part_out, send_w, recv_w, self_w, shards, True)
        slots_wait_all(send_buf, recv_out, samples, send_b, recv_b, self_b, tiles)


def finish_kernel(cfg, samples, shards, node_ref, dloc_ref, sloc_ref, recv_ref, nrow_ref, gat_ref, grad_ref, dv_ref, full_ref, fold_ref, gsend_ref, w_e1, w_e2, w_n1, w_n2, norm_ref):
    tiles, slots, tile_nodes, degree = cfg
    width = node_ref.shape[-1]
    step = pl.program_id(0)

    @pl.when(step == 0)
    def _():
        load_weights(gat_ref, (w_e1, w_e2, w_n1, w_n2), norm_ref)
        fold_ref[...] = onehot_rows(nrow_ref[0:1, :], 0, tile_nodes)
        gsend_ref[...] = jnp.zeros_like(gsend_ref)

    got = recv_ref[:, 0]
    total = sloc_ref[0] + dot_nn(fold_ref[...], got.reshape(tiles * slots, width))
    pieces = split_three(total)
    w_send = w_e1[width:2 * width, :]
    d_v = dloc_ref[0] + dot_nt(pieces[0], w_send) + dot_nt(pieces[1], w_send) + dot_nt(pieces[2], w_send)
    dv_ref[0] = d_v.astype(BF)
    node = node_ref[0]
    gsend_ref[...] += dot_tn(node, pieces[0]) + dot_tn(node, pieces[1]) + dot_tn(node, pieces[2])

    @pl.when(step == samples - 1)
    def _():
        sources = ((grad_ref, 0), (gsend_ref, 0), (grad_ref, 2 * width))
        for shard in range(shards):
            row = SHARD_ROWS[0] * shard
            last = row + SHARD_ROWS[0]
            spot = 0
            while row < last:
                block = row // width
                count = min(last, (block + 1) * width) - row
                ref, base = sources[block]
                base = base + row - block * width
                full_ref[shard, spot:spot + count, :] = ref[base:base + count, :]
                row += count
                spot += count
            first = 3 * width
            for rows, off, span in zip(SHARD_ROWS[1:], SHARD_OFF[1:], (1, 2, 1)):
                full_ref[shard, off:off + rows, :] = grad_ref[first + shard * rows:first + (shard + 1) * rows, :]
                first += span * width
            full_ref[shard, NORM_OFF:NORM_OFF + 8, :] = grad_ref[7 * width:7 * width + 8, :]
            full_ref[shard, NORM_OFF + 8:, :] = jnp.zeros((FULL_ROWS - NORM_OFF - 8, width), F32)


def tail_kernel(tiles, shards, full_ref, part_ref, out_ref, half_buf, x_buf, own, rs_buf, piece, gath, s0, r0, s1, r1, s2, r2, s3, r3):
    me = lax.axis_index('sp')
    dp = lax.axis_index('dp')
    core = lax.rem(dp, 2)
    chip = dp // 2
    chips = shards // 2
    partner = (me, dp + 1 - 2 * core)
    away = line_first(chips)
    spots = [lax.rem(chip + offset, chips) for offset in away]
    line = [(me, spot * 2 + core) for spot in spots]
    plane = tile_peers(tiles)
    greet([partner] + line + plane)
    greeted(1 + len(line) + len(plane))

    pair = [pltpu.make_async_remote_copy(src_ref=full_ref.at[spot * 2 + 1 - core], dst_ref=half_buf.at[spot], send_sem=s0.at[k], recv_sem=r0.at[k], device_id=partner, device_id_type=MESH_ID) for k, spot in enumerate(spots + [chip])]
    for copy in pair:
        copy.start()
    total = part_ref[0]
    for shard in range(1, shards):
        total += part_ref[shard]
    own[1] = total
    hops = []
    for k, spot in enumerate(spots):
        pair[k].wait()
        half_buf[spot] += full_ref[spot * 2 + core]
        hop = pltpu.make_async_remote_copy(src_ref=half_buf.at[spot], dst_ref=x_buf.at[chip], send_sem=s1.at[k], recv_sem=r1.at[k], device_id=line[k], device_id_type=MESH_ID)
        hop.start()
        hops.append(hop)
    pair[-1].wait()
    total = half_buf[chip] + full_ref[dp]
    for hop, offset in zip(hops, away):
        hop.wait()
        total += x_buf[lax.rem(chip + chips - offset, chips)]
    own[0] = total

    rows = FULL_ROWS // tiles
    cuts = []
    for k, peer in enumerate(plane):
        cut = pltpu.make_async_remote_copy(src_ref=own.at[:, pl.ds(pl.multiple_of(peer[0] * rows, rows), rows)], dst_ref=rs_buf.at[me], send_sem=s2.at[k], recv_sem=r2.at[k], device_id=peer, device_id_type=MESH_ID)
        cut.start()
        cuts.append(cut)
    here = pl.ds(pl.multiple_of(me * rows, rows), rows)
    for cut in cuts:
        cut.wait()
    total = own[:, here, :]
    for offset in range(1, tiles):
        total += rs_buf[lax.rem(me + offset, tiles)]
    piece[...] = total
    gath[:, here, :] = total
    sends = []
    for k, peer in enumerate(plane):
        send = pltpu.make_async_remote_copy(src_ref=piece, dst_ref=gath.at[:, here], send_sem=s3.at[k], recv_sem=r3.at[k], device_id=peer, device_id_type=MESH_ID)
        send.start()
        sends.append(send)
    for send in sends:
        send.wait()
    out_ref[...] = gath[...]


def whole(shape):
    zeros = (0,) * len(shape)
    return pl.BlockSpec(shape, lambda s: zeros)


def per_sample(rows, width):
    return pl.BlockSpec((1, rows, width), lambda s: (s, 0, 0))


def slot_spec(tiles, slots, width):
    return pl.BlockSpec((tiles, 1, slots, width), lambda s: (0, s, 0, 0))


def weight_scratch(width):
    return [pltpu.VMEM((3 * width, width), BF), pltpu.VMEM((width, width), BF), pltpu.VMEM((2 * width, width), BF), pltpu.VMEM((width, width), BF), pltpu.VMEM((8, width), F32)]


PARAMS = dict(vmem_limit_bytes=60 * 1024 * 1024)


def grid_params():
    return pltpu.CompilerParams(dimension_semantics=("arbitrary",), **PARAMS)


def remote_params(number):
    return pltpu.CompilerParams(collective_id=number, has_side_effects=True, **PARAMS)


def slot_sems(samples, tiles):
    return [pltpu.SemaphoreType.DMA((samples, tiles)), pltpu.SemaphoreType.DMA((samples, tiles)), pltpu.SemaphoreType.DMA((samples,))]


def shard_sems(shards):
    return [pltpu.SemaphoreType.DMA((shards,)), pltpu.SemaphoreType.DMA((shards,)), pltpu.SemaphoreType.DMA]


def solution(mesh):
    lat_spec = P('dp', 'sp', None)
    edge_spec = P('sp')
    mat_spec = P(None, 'dp', None)
    norm_spec = P(None, None, 'dp')
    param_specs = (mat_spec, mat_spec, mat_spec, mat_spec, norm_spec)
    tiles = mesh.shape['sp']
    dp_size = mesh.shape['dp']

    def spread(value, axis):
        count = mesh.shape[axis]
        return lax.all_to_all(jnp.broadcast_to(value[None], (count,) + value.shape), axis, 0, 0, tiled=True)

    def join(stacked, dim):
        moved = jnp.moveaxis(stacked, 0, dim)
        return moved.reshape(moved.shape[:dim] + (moved.shape[dim] * moved.shape[dim + 1],) + moved.shape[dim + 2:])

    def scatter_sum(value, axis, dim):
        count = mesh.shape[axis]
        split = value.reshape(value.shape[:dim] + (count, value.shape[dim] // count) + value.shape[dim + 1:])
        return jnp.sum(lax.all_to_all(jnp.moveaxis(split, dim, 0), axis, 0, 0, tiled=True), axis=0)

    def gather_weights(masters, layer_idx):
        mat_list = [join(spread(master[layer_idx].astype(BF), 'dp'), 0) for master in masters[:4]]
        norm_rows = join(spread(masters[4][layer_idx].astype(BF), 'dp'), 1).astype(F32)
        return mat_list[0], mat_list[1], mat_list[2], mat_list[3], norm_rows

    def reduce_grads(grads):
        parts = [scatter_sum(grad_full, 'dp', 0) for grad_full in grads[:4]] + [scatter_sum(grads[4], 'dp', 1)]
        return tuple(jnp.sum(spread(part, 'sp'), axis=0) for part in parts)

    def general_step(node_lat, edge_lat, senders, edge_mask, node_cot, edge_cot, masters):
        batch_size, tile_nodes, lat_width = node_lat.shape
        degree = edge_lat.shape[1] // tile_nodes
        layers = masters[0].shape[0]
        mask_f = edge_mask.astype(F32).reshape(tile_nodes, degree)
        mask_b = mask_f.astype(BF)
        node_x = node_lat
        edge_x = edge_lat.reshape(batch_size, tile_nodes, degree, lat_width)
        records = []
        for layer_idx in range(layers):
            layer_wts = gather_weights(masters, layer_idx)
            node_all = join(spread(node_x, 'sp'), 1)
            node_new, edge_new, saved = layer_forward(node_x, node_all, edge_x, senders, mask_b, layer_wts)
            records.append((node_x, edge_x, saved))
            node_x = node_new
            edge_x = edge_new
        d_node = node_cot
        d_edge = edge_cot.reshape(batch_size, tile_nodes, degree, lat_width)
        grads_rev = []
        for layer_idx in reversed(range(layers)):
            layer_wts = gather_weights(masters, layer_idx)
            node_in, edge_in, saved = records[layer_idx]
            d_local, scattered, d_edge, grads = layer_backward(d_node, d_edge, node_in, edge_in, senders, mask_f, saved, layer_wts, tile_nodes * tiles)
            returned = scatter_sum(scattered, 'sp', 1)
            d_node = (d_local + returned).astype(BF)
            grads_rev.append(reduce_grads(grads))
        layer_grads = grads_rev[::-1]
        sums = tuple(jnp.stack([per_layer[slot] for per_layer in layer_grads], axis=0) for slot in range(5))
        return sums + (d_node, d_edge.reshape(edge_lat.shape))

    def compact_step(node_lat, edge_lat, send_all, edge_mask, node_cot, edge_cot, masters):
        samples, tile_nodes, width = node_lat.shape
        edges = edge_lat.shape[1]
        degree = edges // tile_nodes
        cfg = (tiles, SLOTS, tile_nodes, degree)
        cols = tile_nodes + tiles * SLOTS
        lanes = width // dp_size
        dp = lax.axis_index('dp')
        mask_row = jnp.broadcast_to(edge_mask.astype(F32)[None, :], (8, edges))

        def part_of(layer):
            norm = lax.dynamic_update_slice(jnp.zeros((PART_ROWS - NORM_OFF, width), BF), masters[4][layer].astype(BF), (0, dp * lanes))
            return jnp.concatenate([master[layer].astype(BF) for master in masters[:4]] + [norm], axis=0)

        sd = jax.ShapeDtypeStruct
        i32 = jnp.int32
        vmem = pl.BlockSpec(memory_space=pltpu.VMEM)
        hbm = pl.BlockSpec(memory_space=pl.ANY)
        node_s = per_sample(tile_nodes, width)
        edge_s = per_sample(edges, width)
        slot_s = slot_spec(tiles, SLOTS, width)
        gat_s = whole((dp_size, PART_ROWS, width))
        gcol_s = whole((edges, LANES))
        grow_s = whole((8, edges))
        nrow_s = whole((8, tiles * SLOTS))
        grad_s = whole((GRAD_ROWS, width))
        full_s = whole((dp_size, FULL_ROWS, width))
        node_b = sd((samples, tile_nodes, width), BF)
        node_f = sd((samples, tile_nodes, width), F32)
        edge_b = sd((samples, edges, width), BF)
        grad_f = sd((GRAD_ROWS, width), F32)
        slot_b = sd((tiles, samples, SLOTS, width), BF)
        gat_b = sd((dp_size, PART_ROWS, width), BF)
        full_f = sd((dp_size, FULL_ROWS, width), F32)
        slot_v = pltpu.VMEM((tiles, samples, SLOTS, width), BF)
        pick_v = pltpu.VMEM((edges, cols), BF)
        drop_v = pltpu.VMEM((cols, edges), BF)
        rows_v = pltpu.VMEM((cols, width), BF)
        dpre_v = pltpu.VMEM((edges, width), BF)

        (v_one, e_one, h_e, y_e, sums, h_n, y_n, gcol, grow, nrow, mcol, recv_two, gat_one, gat_two) = pl.pallas_call(
            functools.partial(open_kernel, cfg, dp_size), grid=(samples,),
            out_shape=(node_b, edge_b, edge_b, edge_b, node_b, node_b, node_b, sd((edges, LANES), i32), sd((8, edges), i32), sd((8, tiles * SLOTS), i32), sd((edges, LANES), F32), slot_b, gat_b, gat_b),
            in_specs=[whole((tiles, edges)), grow_s, whole((samples, tile_nodes, width)), node_s, edge_s, hbm, hbm],
            out_specs=(node_s, edge_s, edge_s, edge_s, node_s, node_s, node_s, gcol_s, grow_s, nrow_s, gcol_s, hbm, hbm, hbm),
            scratch_shapes=[pick_v, pltpu.VMEM((tiles * SLOTS, tile_nodes), BF), rows_v, slot_v, slot_v, slot_v, pltpu.VMEM((dp_size, PART_ROWS, width), BF)] + weight_scratch(width)
            + slot_sems(samples, tiles) + slot_sems(samples, tiles) + shard_sems(dp_size) + shard_sems(dp_size) + [pltpu.SemaphoreType.DMA],
            name='open', compiler_params=remote_params(1))(send_all, mask_row, node_lat, node_lat, edge_lat, part_of(0), part_of(1))

        d_edge, d_loc, s_loc, grad_two, recv_three = pl.pallas_call(
            functools.partial(turn_kernel, cfg, samples), grid=(samples,),
            out_shape=(edge_b, node_f, node_f, grad_f, slot_b),
            in_specs=[node_s, edge_s, slot_s, gcol_s, grow_s, grow_s, gcol_s, gat_s, node_s, edge_s],
            out_specs=(edge_s, node_s, node_s, grad_s, hbm),
            scratch_shapes=[pick_v, drop_v, rows_v, dpre_v, slot_v] + weight_scratch(width) + slot_sems(samples, tiles),
            name='turn', compiler_params=remote_params(2))(v_one, e_one, recv_two, gcol, grow, mask_row, mcol, gat_two, node_cot, edge_cot)

        def finish(label, node_x, d_loc, s_loc, recv, gat, grad):
            return pl.pallas_call(
                functools.partial(finish_kernel, cfg, samples, dp_size), grid=(samples,),
                out_shape=(node_b, full_f),
                in_specs=[node_s, node_s, node_s, slot_s, nrow_s, gat_s, grad_s],
                out_specs=(node_s, full_s),
                scratch_shapes=[pltpu.VMEM((tile_nodes, tiles * SLOTS), BF), pltpu.VMEM((width, width), F32)] + weight_scratch(width),
                name=label, compiler_params=grid_params())(node_x, d_loc, s_loc, recv, nrow, gat, grad)

        d_node, full_two = finish('finish_two', v_one, d_loc, s_loc, recv_three, gat_two, grad_two)

        d_edge0, d_loc0, s_loc0, grad_one, recv_four, part_two = pl.pallas_call(
            functools.partial(backward_kernel, cfg, samples, dp_size), grid=(samples,),
            out_shape=(edge_b, node_f, node_f, grad_f, slot_b, full_f),
            in_specs=[node_s, edge_s, edge_s, edge_s, node_s, node_s, node_s, grow_s, grow_s, gcol_s, gat_s, node_s, edge_s, hbm],
            out_specs=(edge_s, node_s, node_s, grad_s, hbm, hbm),
            scratch_shapes=[drop_v, dpre_v, slot_v] + weight_scratch(width) + slot_sems(samples, tiles) + shard_sems(dp_size),
            name='backward_one', compiler_params=remote_params(3))(node_lat, edge_lat, h_e, y_e, sums, h_n, y_n, grow, mask_row, mcol, gat_one, d_node, d_edge, full_two)
        d_node0, full_one = finish('finish_one', node_lat, d_loc0, s_loc0, recv_four, gat_one, grad_one)

        rows = FULL_ROWS // tiles
        dma = pltpu.SemaphoreType.DMA
        both = pl.pallas_call(
            functools.partial(tail_kernel, tiles, dp_size),
            out_shape=sd((2, FULL_ROWS, width), F32),
            in_specs=[vmem, vmem], out_specs=vmem,
            scratch_shapes=[pltpu.VMEM((dp_size // 2, FULL_ROWS, width), F32), pltpu.VMEM((dp_size // 2, FULL_ROWS, width), F32), pltpu.VMEM((2, FULL_ROWS, width), F32),
                            pltpu.VMEM((tiles, 2, rows, width), F32), pltpu.VMEM((2, rows, width), F32), pltpu.VMEM((2, FULL_ROWS, width), F32),
                            dma((4,)), dma((4,)), dma((4,)), dma((4,)), dma((tiles,)), dma((tiles,)), dma((tiles,)), dma((tiles,))],
            name='tail', compiler_params=remote_params(4))(full_one, part_two)

        sums_out = [both[:, off:off + count, :] for count, off in zip(SHARD_ROWS, SHARD_OFF)]
        sums_out.append(lax.dynamic_slice(both, (0, NORM_OFF, dp * lanes), (2, 4, lanes)))
        return tuple(sums_out) + (d_node0, d_edge0)

    def train_step(node_lat, edge_lat, senders, edge_mask, node_cot, edge_cot, w_edge1, w_edge2, w_node1, w_node2, norm_par, mom_edge1, mom_edge2, mom_node1, mom_node2, mom_norm, vel_edge1, vel_edge2, vel_node1, vel_node2, vel_norm):
        masters = (w_edge1, w_edge2, w_node1, w_node2, norm_par)
        moments_one = (mom_edge1, mom_edge2, mom_node1, mom_node2, mom_norm)
        moments_two = (vel_edge1, vel_edge2, vel_node1, vel_node2, vel_norm)
        tile_nodes = node_lat.shape[1]
        count = senders.shape[0]
        lines = -(-count // (16 * LANES)) * 16
        mine = jnp.pad(senders, (0, lines * LANES - count)).reshape(lines, LANES)
        vmem = pl.BlockSpec(memory_space=pltpu.VMEM)
        send_all = pl.pallas_call(
            functools.partial(ids_kernel, tiles), out_shape=jax.ShapeDtypeStruct((tiles, lines, LANES), jnp.int32),
            in_specs=[vmem], out_specs=vmem, scratch_shapes=[pltpu.SemaphoreType.DMA((tiles,)), pltpu.SemaphoreType.DMA((tiles,))],
            name='ids', compiler_params=remote_params(0))(mine).reshape(tiles, lines * LANES)[:, :count]
        tile_of = send_all // tile_nodes
        tile_ids = jnp.arange(tiles, dtype=jnp.int32)
        counts = jnp.sum((tile_of[:, None, :] == tile_ids[None, :, None]).astype(jnp.int32), axis=2)
        counts = jnp.where(tile_ids[:, None] == tile_ids[None, :], 0, counts)
        fits = jnp.max(counts) <= SLOTS

        def fast():
            return compact_step(node_lat, edge_lat, send_all, edge_mask, node_cot, edge_cot, masters)

        def slow():
            return general_step(node_lat, edge_lat, senders, edge_mask, node_cot, edge_cot, masters)

        result = lax.cond(fits, fast, slow)
        new_state = [adamw_update(masters[slot], result[slot], moments_one[slot], moments_two[slot]) for slot in range(5)]
        return tuple(item[0] for item in new_state) + tuple(item[1] for item in new_state) + tuple(item[2] for item in new_state) + (result[5], result[6])

    return jax.shard_map(train_step, mesh=mesh, in_specs=(lat_spec, lat_spec, edge_spec, edge_spec, lat_spec, lat_spec) + param_specs + param_specs + param_specs, out_specs=param_specs + param_specs + param_specs + (lat_spec, lat_spec), check_vma=False)
```

```python
import functools

import jax
import jax.numpy as jnp
from jax import lax
from jax.experimental import pallas as pl
from jax.experimental.pallas import tpu as pltpu
from jax.sharding import PartitionSpec as P

NORM_EPS = 1e-5
LEARN_RATE = 1e-3
BETA_ONE = 0.9
BETA_TWO = 0.95
ADAM_EPS = 1e-8
DECAY = 0.1
STEP = 10

BF = jnp.bfloat16
F32 = jnp.float32
SLOTS = 80
MESH_ID = pl.DeviceIdType.MESH


def ring_gap(offset, count):
    return min(offset % count, -offset % count)


def far_first(tiles):
    side = int(tiles ** 0.5)
    return sorted(range(1, tiles), key=lambda offset: -ring_gap(offset // side, side) - ring_gap(offset, side))


def line_first(count):
    return sorted(range(1, count), key=lambda offset: -ring_gap(offset, count))

LANES = 128
SHARD_ROWS = (96, 32, 64, 32)
SHARD_OFF = (0, 96, 128, 192)
NORM_OFF = 224
PART_ROWS = 240
FULL_ROWS = 256
GRAD_ROWS = 1800


def contract(left_op, right_op, left_dims, right_dims):
    return lax.dot_general(left_op, right_op, ((left_dims, right_dims), ((), ())), preferred_element_type=jnp.float32)


def norm_forward(out_b, norm_gain, norm_bias):
    values = out_b.astype(jnp.float32)
    centered = values - jnp.mean(values, axis=-1, keepdims=True)
    inv_std = lax.rsqrt(jnp.mean(centered * centered, axis=-1, keepdims=True) + NORM_EPS)
    normed = centered * inv_std
    return normed * norm_gain + norm_bias, normed, inv_std


def mlp_tail(pre_act, w_two, norm_gain, norm_bias):
    pre_b = pre_act.astype(jnp.bfloat16)
    hidden_act = jax.nn.silu(pre_b.astype(jnp.float32)).astype(jnp.bfloat16)
    last_dim = hidden_act.ndim - 1
    out_b = contract(hidden_act, w_two, (last_dim,), (0,)).astype(jnp.bfloat16)
    branch, normed, inv_std = norm_forward(out_b, norm_gain, norm_bias)
    return branch, (pre_b, hidden_act, normed, inv_std)


def mlp_back(d_branch, saved, w_one, w_two, norm_gain):
    pre_b, hidden_act, normed, inv_std = saved
    last_dim = hidden_act.ndim - 1
    lead_dims = tuple(range(last_dim))
    d_gain = jnp.sum(d_branch * normed, axis=lead_dims)
    d_bias = jnp.sum(d_branch, axis=lead_dims)
    d_norm = d_branch * norm_gain
    d_out = (inv_std * (d_norm - jnp.mean(d_norm, axis=-1, keepdims=True) - normed * jnp.mean(d_norm * normed, axis=-1, keepdims=True))).astype(jnp.bfloat16)
    d_two = contract(hidden_act, d_out, lead_dims, lead_dims)
    d_act = contract(d_out, w_two, (last_dim,), (1,)).astype(jnp.bfloat16)
    pre_f = pre_b.astype(jnp.float32)
    gate_sig = jax.nn.sigmoid(pre_f)
    d_pre = (d_act.astype(jnp.float32) * gate_sig * (1.0 + pre_f * (1.0 - gate_sig))).astype(jnp.bfloat16)
    d_in = contract(d_pre, w_one, (last_dim,), (1,))
    return d_pre, d_in, d_two, d_gain, d_bias


def layer_forward(node_x, node_all, edge_x, senders, mask_b, layer_wts):
    w_e1, w_e2, w_n1, w_n2, norm_rows = layer_wts
    lat_width = node_x.shape[-1]
    sender_lat = jnp.take(node_all, senders, axis=1).reshape(edge_x.shape)
    pre_e = (contract(edge_x, w_e1[:lat_width], (3,), (0,))
             + contract(sender_lat, w_e1[lat_width:2 * lat_width], (3,), (0,))
             + contract(node_x, w_e1[2 * lat_width:], (2,), (0,))[:, :, None, :])
    branch_e, saved_e = mlp_tail(pre_e, w_e2, norm_rows[0], norm_rows[1])
    edge_new = (edge_x.astype(jnp.float32) + branch_e).astype(jnp.bfloat16)
    node_sum = jnp.einsum('bngd,ng->bnd', edge_new, mask_b, preferred_element_type=jnp.float32).astype(jnp.bfloat16)
    pre_n = contract(node_x, w_n1[:lat_width], (2,), (0,)) + contract(node_sum, w_n1[lat_width:], (2,), (0,))
    branch_n, saved_n = mlp_tail(pre_n, w_n2, norm_rows[2], norm_rows[3])
    node_new = (node_x.astype(jnp.float32) + branch_n).astype(jnp.bfloat16)
    return node_new, edge_new, (sender_lat, node_sum, saved_e, saved_n)


def layer_backward(d_node_new, d_edge_new, node_x, edge_x, senders, mask_f, saved, layer_wts, total_nodes):
    w_e1, w_e2, w_n1, w_n2, norm_rows = layer_wts
    sender_lat, node_sum, saved_e, saved_n = saved
    batch_size, tile_nodes, degree, lat_width = edge_x.shape
    d_res_n = d_node_new.astype(jnp.float32)
    d_pre_n, d_in_n, d_wn2, d_gain_n, d_bias_n = mlp_back(d_res_n, saved_n, w_n1, w_n2, norm_rows[2])
    d_wn1 = jnp.concatenate([contract(node_x, d_pre_n, (0, 1), (0, 1)), contract(node_sum, d_pre_n, (0, 1), (0, 1))], axis=0)
    d_sum = d_in_n[..., lat_width:].astype(jnp.bfloat16)
    d_res_e = (d_edge_new.astype(jnp.float32) + d_sum.astype(jnp.float32)[:, :, None, :] * mask_f[None, :, :, None]).astype(jnp.bfloat16).astype(jnp.float32)
    d_pre_e, d_in_e, d_we2, d_gain_e, d_bias_e = mlp_back(d_res_e, saved_e, w_e1, w_e2, norm_rows[0])
    recv_grad = contract(node_x, d_pre_e.reshape(batch_size, tile_nodes, -1), (0, 1), (0, 1))
    d_we1 = jnp.concatenate([contract(edge_x, d_pre_e, (0, 1, 2), (0, 1, 2)), contract(sender_lat, d_pre_e, (0, 1, 2), (0, 1, 2)), recv_grad.reshape(lat_width, degree, -1).sum(axis=1)], axis=0)
    d_edge_x = (d_res_e + d_in_e[..., :lat_width]).astype(jnp.bfloat16)
    d_sender = d_in_e[..., lat_width:2 * lat_width].reshape(batch_size, tile_nodes * degree, lat_width)
    scattered = jnp.zeros((batch_size, total_nodes, lat_width), jnp.float32).at[:, senders].add(d_sender)
    d_local = d_res_n + d_in_n[..., :lat_width] + d_in_e[..., 2 * lat_width:].sum(axis=2)
    grads = (d_we1, d_we2, d_wn1, d_wn2, jnp.stack([d_gain_e, d_bias_e, d_gain_n, d_bias_n]))
    return d_local, scattered, d_edge_x, grads


def adamw_update(master, grad_sum, moment_one, moment_two):
    corr_one = 1.0 - BETA_ONE ** STEP
    corr_two = 1.0 - BETA_TWO ** STEP
    one_new = BETA_ONE * moment_one + (1.0 - BETA_ONE) * grad_sum
    two_new = BETA_TWO * moment_two + (1.0 - BETA_TWO) * grad_sum * grad_sum
    direction = (one_new / corr_one) / (jnp.sqrt(two_new / corr_two) + ADAM_EPS)
    return master - LEARN_RATE * (direction + DECAY * master), one_new, two_new


def dot_nn(left_op, right_op):
    return lax.dot_general(left_op, right_op, (((1,), (0,)), ((), ())), preferred_element_type=F32)


def dot_nt(left_op, right_op):
    return lax.dot_general(left_op, right_op, (((1,), (1,)), ((), ())), preferred_element_type=F32)


def dot_tn(left_op, right_op):
    return lax.dot_general(left_op, right_op, (((0,), (0,)), ((), ())), preferred_element_type=F32)


def split_three(values):
    high = values.astype(BF)
    rest = values - high.astype(F32)
    mid = rest.astype(BF)
    low = (rest - mid.astype(F32)).astype(BF)
    return high, mid, low


def to_bf(cond):
    return jnp.where(cond, 1.0, 0.0).astype(BF)


def onehot_cols(col_ids, first, width):
    rows = col_ids.shape[0]
    lane = lax.broadcasted_iota(jnp.int32, (rows, LANES), 1)
    parts = [to_bf(col_ids == lane + (first + LANES * i)) for i in range(width // LANES)]
    return jnp.concatenate(parts, axis=1)


def onehot_rows(row_ids, first, height):
    width = row_ids.shape[1]
    sub = lax.broadcasted_iota(jnp.int32, (height, width), 0) + first
    return to_bf(row_ids == sub)


def norm_parts(out_b):
    values = out_b.astype(F32)
    centered = values - jnp.mean(values, axis=-1, keepdims=True)
    inv_std = lax.rsqrt(jnp.mean(centered * centered, axis=-1, keepdims=True) + NORM_EPS)
    return centered * inv_std, inv_std


def branch_forward(pre_act, w_two, gain, bias):
    pre_b = pre_act.astype(BF)
    pre_f = pre_b.astype(F32)
    sig = jax.nn.sigmoid(pre_f)
    act = (pre_f * sig).astype(BF)
    out_b = dot_nn(act, w_two).astype(BF)
    normed, inv_std = norm_parts(out_b)
    return normed * gain + bias, (pre_b, act, sig, normed, inv_std, out_b)


def branch_backward(d_branch, pre_b, act, sig, normed, inv_std, w_two, gain):
    d_norm = d_branch * gain
    mean_one = jnp.mean(d_norm, axis=-1, keepdims=True)
    mean_two = jnp.mean(d_norm * normed, axis=-1, keepdims=True)
    d_out = (inv_std * (d_norm - mean_one - normed * mean_two)).astype(BF)
    d_two = dot_tn(act, d_out)
    d_act = dot_nt(d_out, w_two).astype(BF)
    pre_f = pre_b.astype(F32)
    d_pre = (d_act.astype(F32) * sig * (1.0 + pre_f * (1.0 - sig))).astype(BF)
    d_gain = jnp.sum(d_branch * normed, axis=0, keepdims=True)
    d_bias = jnp.sum(d_branch, axis=0, keepdims=True)
    return d_pre, d_two, d_gain, d_bias


def load_weights(part_ref, layer, all_wts, norm_ref):
    norm = jnp.zeros((PART_ROWS - NORM_OFF, part_ref.shape[-1]), F32)
    for shard in range(part_ref.shape[0]):
        for ref, rows, off in zip(all_wts, SHARD_ROWS, SHARD_OFF):
            ref[layer, shard * rows:(shard + 1) * rows, :] = part_ref[shard, off:off + rows, :]
        norm += part_ref[shard, NORM_OFF:, :].astype(F32)
    norm_ref[layer] = norm[:8]


def cast_parts(master_refs, part_ref):
    dp = lax.axis_index('dp')
    layers, gains, lanes = master_refs[-1].shape
    width = part_ref.shape[-1]
    spot = lax.broadcasted_iota(jnp.int32, (lanes, width), 1) - lanes * dp
    place = to_bf(spot == lax.broadcasted_iota(jnp.int32, (lanes, width), 0))
    for layer in range(layers):
        for ref, rows, off in zip(master_refs, SHARD_ROWS, SHARD_OFF):
            part_ref[layer, off:off + rows, :] = ref[layer].astype(BF)
        norm = jnp.concatenate([master_refs[-1][layer], jnp.zeros((PART_ROWS - NORM_OFF - gains, lanes), F32)], axis=0)
        part_ref[layer, NORM_OFF:, :] = dot_nn(norm.astype(BF), place).astype(BF)


def peer_tile(me, offset, side):
    row = lax.rem(me // side + offset // side, side)
    col = lax.rem(lax.rem(me, side) + offset % side, side)
    return row * side + col


def greet(peers):
    barrier = pltpu.get_barrier_semaphore()
    for peer in peers:
        pl.semaphore_signal(barrier, inc=1, device_id=peer, device_id_type=MESH_ID)


def greeted(count):
    pl.semaphore_wait(pltpu.get_barrier_semaphore(), count)


def tile_peers(tiles):
    me = lax.axis_index('sp')
    dp = lax.axis_index('dp')
    side = int(tiles ** 0.5)
    return [(peer_tile(me, offset, side), dp) for offset in far_first(tiles)]


def slot_copy(src_ref, dst_ref, sample, spot, send_sem, recv_sem, peer, me):
    return pltpu.make_async_remote_copy(src_ref=src_ref.at[peer[0], sample], dst_ref=dst_ref.at[me, sample], send_sem=send_sem.at[sample, spot], recv_sem=recv_sem.at[sample, spot], device_id=peer, device_id_type=MESH_ID)


def slots_start(src_ref, dst_ref, sample, send_sem, recv_sem, self_sem, tiles):
    me = lax.axis_index('sp')
    pltpu.make_async_copy(src_ref.at[me, sample], dst_ref.at[me, sample], self_sem.at[sample]).start()
    for spot, peer in enumerate(tile_peers(tiles)):
        slot_copy(src_ref, dst_ref, sample, spot, send_sem, recv_sem, peer, me).start()


def slots_wait(src_ref, dst_ref, sample, send_sem, recv_sem, self_sem, tiles):
    me = lax.axis_index('sp')
    pltpu.make_async_copy(src_ref.at[me, sample], dst_ref.at[me, sample], self_sem.at[sample]).wait()
    for spot, peer in enumerate(tile_peers(tiles)):
        slot_copy(src_ref, dst_ref, sample, spot, send_sem, recv_sem, peer, me).wait()


def slots_wait_all(src_ref, dst_ref, samples, send_sem, recv_sem, self_sem, tiles):
    def one(sample, carry):
        slots_wait(src_ref, dst_ref, sample, send_sem, recv_sem, self_sem, tiles)
        return carry
    lax.fori_loop(0, samples, one, 0)


def shard_peers(count):
    me = lax.axis_index('sp')
    dp = lax.axis_index('dp')
    return [(me, lax.rem(dp + offset, count)) for offset in line_first(count)]


def shard_copy(src_ref, dst_ref, spot, send_sem, recv_sem, peer, scatter):
    dp = lax.axis_index('dp')
    src = src_ref.at[peer[1]] if scatter else src_ref
    return pltpu.make_async_remote_copy(src_ref=src, dst_ref=dst_ref.at[dp], send_sem=send_sem.at[spot], recv_sem=recv_sem.at[spot], device_id=peer, device_id_type=MESH_ID)


def shards_start(src_ref, dst_ref, send_sem, recv_sem, self_sem, count, scatter):
    dp = lax.axis_index('dp')
    pltpu.make_async_copy(src_ref.at[dp] if scatter else src_ref, dst_ref.at[dp], self_sem).start()
    for spot, peer in enumerate(shard_peers(count)):
        shard_copy(src_ref, dst_ref, spot, send_sem, recv_sem, peer, scatter).start()


def shards_wait(src_ref, dst_ref, send_sem, recv_sem, self_sem, count, scatter):
    dp = lax.axis_index('dp')
    pltpu.make_async_copy(src_ref.at[dp] if scatter else src_ref, dst_ref.at[dp], self_sem).wait()
    for spot, peer in enumerate(shard_peers(count)):
        shard_copy(src_ref, dst_ref, spot, send_sem, recv_sem, peer, scatter).wait()


def chunk_maps(degree, mask_rows, mask_col):
    chunk = mask_rows.shape[1]
    nodes = chunk // degree
    sub_w = lax.broadcasted_iota(jnp.int32, (nodes, chunk), 0) * degree
    lane_w = lax.broadcasted_iota(jnp.int32, (nodes, chunk), 1)
    wide = (lane_w >= sub_w) & (lane_w < sub_w + degree)
    sub_t = lax.broadcasted_iota(jnp.int32, (chunk, nodes), 0)
    lane_t = lax.broadcasted_iota(jnp.int32, (chunk, nodes), 1) * degree
    tall = (sub_t >= lane_t) & (sub_t < lane_t + degree)
    out = dict(tall=to_bf(tall), wide=to_bf(wide), sum=jnp.where(wide, mask_rows[:1], 0.0).astype(BF))
    if mask_col is not None:
        out['spread'] = jnp.where(tall, jnp.concatenate([mask_col] * (nodes // LANES), axis=1), 0.0).astype(BF)
    return out


def make_tables(tiles, slots, tile_nodes, send_ids, mask_ref, node_ref, gcol_ref, grow_ref, nrow_ref, mcol_ref, mrow_ref, pack_ref, out_ref):
    me = lax.axis_index('sp')
    ids = send_ids[...]
    edges = ids.shape[1]
    tile_of = ids // tile_nodes
    local = (ids - tile_of * tile_nodes).astype(F32)
    row = lax.broadcasted_iota(jnp.int32, (tiles, edges), 0)
    is_me = row == me
    own_tile = jnp.sum(jnp.where(is_me, tile_of, 0), axis=0, keepdims=True)
    own_local = jnp.sum(jnp.where(is_me, local, 0.0), axis=0, keepdims=True)
    own = jnp.where(own_tile == row, 1.0, 0.0)
    inc = jnp.where((tile_of == me) & jnp.logical_not(is_me), 1.0, 0.0)
    both = jnp.concatenate([own, inc], axis=0).astype(BF)
    rank = jnp.zeros((2 * tiles, edges), F32)
    step = 256
    for blk in range(edges // step):
        first = lax.broadcasted_iota(jnp.int32, (step, edges), 0) + blk * step
        second = lax.broadcasted_iota(jnp.int32, (step, edges), 1)
        rank += dot_nn(both[:, blk * step:(blk + 1) * step], to_bf(first < second))
    slot_id = jnp.where(is_me, own_local, rank[:tiles] + (row * slots + tile_nodes).astype(F32))
    gidx = jnp.sum(own * slot_id, axis=0, keepdims=True)
    grow_ref[...] = jnp.broadcast_to(gidx, grow_ref.shape).astype(jnp.int32)
    gcol_ref[...] = jnp.transpose(jnp.broadcast_to(gidx, (LANES, edges))).astype(jnp.int32)
    mask = mask_ref[...].astype(F32)
    mrow_ref[...] = jnp.broadcast_to(mask, mrow_ref.shape)
    mcol_ref[...] = jnp.transpose(jnp.broadcast_to(mask, (LANES, edges)))
    slot_row = lax.broadcasted_iota(jnp.int32, (slots, edges), 0).astype(F32)
    cols = []
    for peer in range(tiles):
        hit = (slot_row == rank[tiles + peer:tiles + peer + 1]) & (inc[peer:peer + 1] > 0.5)
        found = jnp.sum(jnp.where(hit, local[peer:peer + 1] + 1.0, 0.0), axis=1, keepdims=True) - 1.0
        cols.append(jnp.broadcast_to(found, (slots, LANES)))
    ncol_f = jnp.concatenate(cols, axis=0)
    ncol = ncol_f.astype(jnp.int32)
    nrow_ref[...] = jnp.transpose(ncol_f)[:8].astype(jnp.int32)
    group = 4
    for part in range(tiles // group):
        rows = group * slots
        pick = onehot_cols(ncol[part * rows:(part + 1) * rows], 0, tile_nodes)
        pack_ref[part * rows:(part + 1) * rows, :] = pick
        for sample in range(out_ref.shape[1]):
            got = dot_nn(pick, node_ref[sample]).astype(BF)
            out_ref[part * group:(part + 1) * group, sample] = got.reshape(group, slots, got.shape[1])


def fill_rows(rows_ref, node, got, tile_nodes):
    rows_ref[:tile_nodes, :] = node
    rows_ref[tile_nodes:, :] = got.reshape(got.shape[0] * got.shape[1], got.shape[2])


def build_pick(gcol_ref, pick_ref):
    step = 128 * 3

    def build(i, carry):
        base = pl.multiple_of(i * step, step)
        pick_ref[pl.ds(base, step), :] = onehot_cols(gcol_ref[pl.ds(base, step), :], 0, pick_ref.shape[1])
        return carry
    lax.fori_loop(0, pick_ref.shape[0] // step, build, 0)


def fwd_sample(maps, v_c, e_c, pick_ref, rows_ref, wts, norm_ref):
    w_e1, w_e2, w_n1, w_n2 = wts
    width = e_c.shape[-1]
    w_edge, w_send, w_recv = (w_e1[i * width:(i + 1) * width, :] for i in range(w_e1.shape[0] // width))
    sent = dot_nn(pick_ref[...], rows_ref[...]).astype(BF)
    recv = dot_nn(maps['tall'], v_c).astype(BF)
    pre = dot_nn(e_c, w_edge) + dot_nn(sent, w_send) + dot_nn(recv, w_recv)
    rows = [norm_ref[i:i + 1, :] for i in range(len(SHARD_ROWS))]
    branch, edge_s = branch_forward(pre, w_e2[...], rows[0], rows[1])
    e_new = (e_c.astype(F32) + branch).astype(BF)
    sums = dot_nn(maps['sum'], e_new).astype(BF)
    pre_n = dot_nn(v_c, w_n1[:width, :]) + dot_nn(sums, w_n1[width:, :])
    branch_n, node_s = branch_forward(pre_n, w_n2[...], rows[2], rows[3])
    return e_new, sums, branch_n, edge_s, node_s


def ids_kernel(tiles, slots, tile_nodes, mine_ref, ids_ref, most_ref, wide, send_sem, recv_sem):
    me = lax.axis_index('sp')
    peers = tile_peers(tiles)
    greet(peers)
    wide[me] = mine_ref[...]
    greeted(len(peers))
    copies = [pltpu.make_async_remote_copy(src_ref=mine_ref, dst_ref=wide.at[me], send_sem=send_sem.at[spot], recv_sem=recv_sem.at[spot], device_id=peer, device_id_type=MESH_ID) for spot, peer in enumerate(peers)]
    for copy in copies:
        copy.start()
    for copy in copies:
        copy.wait()
    for line in range(wide.shape[1]):
        ids_ref[:, line * LANES:(line + 1) * LANES] = wide[:, line, :]
    tile_of = ids_ref[...] // tile_nodes
    row = lax.broadcasted_iota(jnp.int32, (tiles, LANES), 0)
    most = jnp.zeros((tiles, LANES), F32)
    for peer in range(tiles):
        count = jnp.sum(jnp.where(tile_of == peer, 1.0, 0.0), axis=1, keepdims=True)
        most = jnp.maximum(most, jnp.where(row == peer, 0.0, count))
    most_ref[...] = jnp.broadcast_to(jnp.max(most, axis=0, keepdims=True), most_ref.shape)


def open_kernel(cfg, shards, send_ids, mask_ref, nodes_ref, node_ref, edge_ref, dnode_ref, dedge_ref, m_e1, m_e2, m_n1, m_n2, m_norm,
                vout_ref, he_ref, ye_ref, sum_ref, hn_ref, yn_ref, de_ref, dloc_ref, sloc_ref, grad_ref, grow_ref, nrow_ref, mcol_ref, mrow_ref, w_e1, w_e2, w_n1, w_n2, norm_ref, recv_out,
                gcol_ref, pick_ref, drop_ref, pack_ref, rows_ref, dpre_ref, e_two, v_two, out_buf, in_buf, next_buf, in_two, part_ref, gat_ref,
                send_a, recv_a, self_a, send_b, recv_b, self_b, send_c, recv_c, self_c, send_w, recv_w, self_w, send_x, recv_x, self_x):
    tiles, slots, tile_nodes, degree = cfg
    samples = nodes_ref.shape[0]
    all_wts = (w_e1, w_e2, w_n1, w_n2)
    step = pl.program_id(0)
    weight_sems = ((send_w, recv_w, self_w), (send_x, recv_x, self_x))

    def take_weights(layer):
        shards_wait(part_ref.at[layer], gat_ref.at[layer], *weight_sems[layer], shards, False)
        load_weights(gat_ref.at[layer], layer, all_wts, norm_ref)

    @pl.when(step == 0)
    def _():
        peers = tile_peers(tiles) + shard_peers(shards)
        greet(peers)
        cast_parts((m_e1, m_e2, m_n1, m_n2, m_norm), part_ref)
        make_tables(tiles, slots, tile_nodes, send_ids, mask_ref, nodes_ref, gcol_ref, grow_ref, nrow_ref, mcol_ref, mrow_ref, pack_ref, out_buf)
        greeted(len(peers))
        for sample in range(samples):
            slots_start(out_buf, in_buf, sample, send_a, recv_a, self_a, tiles)
        for layer, sems in enumerate(weight_sems):
            shards_start(part_ref.at[layer], gat_ref.at[layer], *sems, shards, False)
        build_pick(gcol_ref, pick_ref)
        take_weights(0)

    @pl.when(step < samples)
    def _():
        slots_wait(out_buf, in_buf, step, send_a, recv_a, self_a, tiles)
        fill_rows(rows_ref, node_ref[0], in_buf[:, step], tile_nodes)
        node, edge = node_ref[0], edge_ref[0]
        e_new, sums, branch_n, edge_s, node_s = fwd_sample(chunk_maps(degree, mrow_ref[...], None), node, edge, pick_ref, rows_ref, [ref.at[0] for ref in all_wts], norm_ref.at[0])
        v_new = (node.astype(F32) + branch_n).astype(BF)
        for ref, value in ((he_ref, edge_s[0]), (ye_ref, edge_s[-1]), (sum_ref, sums), (hn_ref, node_s[0]), (yn_ref, node_s[-1]), (vout_ref, v_new)):
            ref[0] = value
        e_two[step] = e_new
        v_two[step] = v_new

        def pack(i, carry):
            rows = 4 * slots
            base = pl.multiple_of(i * rows, rows)
            got = dot_nn(pack_ref[pl.ds(base, rows), :], vout_ref[0]).astype(BF)
            next_buf[pl.ds(i * 4, 4), step] = got.reshape(4, slots, got.shape[1])
            return carry
        lax.fori_loop(0, tiles // 4, pack, 0)
        slots_start(next_buf, in_two, step, send_b, recv_b, self_b, tiles)

    @pl.when(step == samples)
    def _():
        take_weights(1)
        build_drop(grow_ref, drop_ref)
        grad_ref[...] = jnp.zeros_like(grad_ref)

    @pl.when(step >= samples)
    def _():
        sample = step - samples
        slots_wait(next_buf, in_two, sample, send_b, recv_b, self_b, tiles)
        node, edge = v_two[sample], e_two[sample]
        fill_rows(rows_ref, node, in_two[:, sample], tile_nodes)
        wts, norm = [ref.at[1] for ref in all_wts], norm_ref.at[1]
        maps = chunk_maps(degree, mrow_ref[...], mcol_ref[...])
        e_new, sums, branch_n, edge_s, node_s = fwd_sample(maps, node, edge, pick_ref, rows_ref, wts, norm)
        back_sample(maps, node, edge, sums, edge_s[:-1], node_s[:-1], dnode_ref[0].astype(F32), dedge_ref, wts, norm, grad_ref, dpre_ref, de_ref, dloc_ref)
        back_pack(dpre_ref, drop_ref, sloc_ref, out_buf, sample, tiles, slots, tile_nodes)
        slots_start(out_buf, recv_out, sample, send_c, recv_c, self_c, tiles)

    @pl.when(step == 2 * samples - 1)
    def _():
        slots_wait_all(out_buf, recv_out, samples, send_c, recv_c, self_c, tiles)


def back_sample(maps, v_c, e_c, sums, edge_s, node_s, d_node, dedge_ref, wts, norm_ref, grad_ref, dpre_ref, de_ref, dloc_ref):
    w_e1, w_e2, w_n1, w_n2 = wts
    width = e_c.shape[-1]
    w_edge, w_send, w_recv = (w_e1[i * width:(i + 1) * width, :] for i in range(w_e1.shape[0] // width))
    d_pre_n, d_wn2, d_gain_n, d_bias_n = branch_backward(d_node, *node_s, w_n2[...], norm_ref[2:3, :])
    d_in_v = dot_nt(d_pre_n, w_n1[:width, :])
    d_sum = dot_nt(d_pre_n, w_n1[width:, :]).astype(BF)
    d_res = (dedge_ref[0].astype(F32) + dot_nn(maps['spread'], d_sum)).astype(BF).astype(F32)
    d_pre, d_we2, d_gain_e, d_bias_e = branch_backward(d_res, *edge_s, w_e2[...], norm_ref[0:1, :])
    dpre_ref[...] = d_pre
    de_ref[0] = (d_res + dot_nt(d_pre, w_edge)).astype(BF)
    recv = split_three(dot_nn(maps['wide'], d_pre))
    dloc_ref[0] = d_node + d_in_v + sum(dot_nt(piece, w_recv) for piece in recv)
    blocks = [dot_tn(e_c, d_pre), None, sum(dot_tn(v_c, piece) for piece in recv), d_we2, dot_tn(v_c, d_pre_n), dot_tn(sums, d_pre_n), d_wn2]
    for i, block in enumerate(blocks):
        if block is not None:
            grad_ref[i * width:(i + 1) * width, :] += block
    rows = [d_gain_e, d_bias_e, d_gain_n, d_bias_n]
    grad_ref[len(blocks) * width:, :] += jnp.concatenate(rows + [jnp.zeros((len(rows), width), F32)], axis=0)


def back_pack(dpre_ref, drop_ref, sloc_ref, send_buf, step, tiles, slots, tile_nodes):
    sloc_ref[0] = dot_nn(drop_ref[:tile_nodes, :], dpre_ref[...])

    def pack(i, carry):
        rows = 4 * slots
        base = pl.multiple_of(tile_nodes + i * rows, 64)
        got = dot_nn(drop_ref[pl.ds(base, rows), :], dpre_ref[...]).astype(BF)
        send_buf[pl.ds(i * 4, 4), step] = got.reshape(4, slots, got.shape[1])
        return carry
    lax.fori_loop(0, tiles // 4, pack, 0)


def build_drop(grow_ref, drop_ref):
    step = 256

    def build(i, carry):
        base = pl.multiple_of(i * step, step)
        drop_ref[pl.ds(base, step), :] = onehot_rows(grow_ref[0:1, :], base, step)
        return carry
    lax.fori_loop(0, drop_ref.shape[0] // step, build, 0)


def again(pre_b, out_b):
    pre_f = pre_b.astype(F32)
    sig = jax.nn.sigmoid(pre_f)
    act = (pre_f * sig).astype(BF)
    normed, inv_std = norm_parts(out_b)
    return pre_b, act, sig, normed, inv_std


def backward_kernel(cfg, shards, node_ref, edge_ref, he_ref, ye_ref, sum_ref, hn_ref, yn_ref, dedge_ref, grow_ref, mrow_ref, mcol_ref, nrow_ref, w_e1, w_e2, w_n1, w_n2, norms_ref, vall_ref, dlall_ref, slall_ref, recv_ref, gtwo_ref,
                    de_ref, dloc_ref, sloc_ref, grad_ref, recv_out, part_out,
                    drop_ref, dpre_ref, fold_ref, gsend_ref, dv_ref, full_ref, send_buf, send_b, recv_b, self_b, send_w, recv_w, self_w):
    tiles, slots, tile_nodes, degree = cfg
    samples = vall_ref.shape[0]
    step = pl.program_id(0)

    @pl.when(step == 0)
    def _():
        peers = tile_peers(tiles) + shard_peers(shards)
        greet(peers)
        fold_ref[...] = onehot_rows(nrow_ref[:1], 0, tile_nodes)
        gsend_ref[...] = jnp.zeros_like(gsend_ref)

        def finish(sample, carry):
            dv_ref[sample] = finish_sample(vall_ref[sample], dlall_ref[sample], slall_ref[sample], recv_ref[:, sample], fold_ref, gsend_ref, w_e1.at[1])
            return carry
        lax.fori_loop(0, samples, finish, 0)
        lay_grads(full_ref, gtwo_ref, gsend_ref)
        greeted(len(peers))
        shards_start(full_ref, part_out, send_w, recv_w, self_w, shards, True)
        build_drop(grow_ref, drop_ref)
        grad_ref[...] = jnp.zeros_like(grad_ref)

    maps = chunk_maps(degree, mrow_ref[...], mcol_ref[...])
    edge_s = again(he_ref[0], ye_ref[0])
    node_s = again(hn_ref[0], yn_ref[0])
    back_sample(maps, node_ref[0], edge_ref[0], sum_ref[0], edge_s, node_s, dv_ref[step].astype(F32), dedge_ref, [ref.at[0] for ref in (w_e1, w_e2, w_n1, w_n2)], norms_ref.at[0], grad_ref, dpre_ref, de_ref, dloc_ref)
    back_pack(dpre_ref, drop_ref, sloc_ref, send_buf, step, tiles, slots, tile_nodes)
    slots_start(send_buf, recv_out, step, send_b, recv_b, self_b, tiles)

    @pl.when(step == samples - 1)
    def _():
        shards_wait(full_ref, part_out, send_w, recv_w, self_w, shards, True)
        slots_wait_all(send_buf, recv_out, samples, send_b, recv_b, self_b, tiles)


def finish_sample(node, d_loc, s_loc, got, fold_ref, gsend_ref, w_e1):
    width = node.shape[-1]
    total = s_loc + dot_nn(fold_ref[...], got.reshape(got.shape[0] * got.shape[1], width))
    pieces = split_three(total)
    w_send = w_e1[width:2 * width, :]
    gsend_ref[...] += sum(dot_tn(node, piece) for piece in pieces)
    return (d_loc + sum(dot_nt(piece, w_send) for piece in pieces)).astype(BF)


def lay_grads(full_ref, grad_ref, gsend_ref):
    shards, rows_all, width = full_ref.shape
    sources = ((grad_ref, 0), (gsend_ref, 0), (grad_ref, 2 * width))
    for shard in range(shards):
        row = SHARD_ROWS[0] * shard
        last = row + SHARD_ROWS[0]
        spot = 0
        while row < last:
            block = row // width
            count = min(last, (block + 1) * width) - row
            ref, base = sources[block]
            base = base + row - block * width
            full_ref[shard, spot:spot + count, :] = ref[base:base + count, :]
            row += count
            spot += count
        first = 3 * width
        for rows, off in zip(SHARD_ROWS[1:], SHARD_OFF[1:]):
            full_ref[shard, off:off + rows, :] = grad_ref[first + shard * rows:first + (shard + 1) * rows, :]
            first += rows * shards
        full_ref[shard, NORM_OFF:NORM_OFF + 8, :] = grad_ref[first:first + 8, :]
        full_ref[shard, NORM_OFF + 8:, :] = jnp.zeros((rows_all - NORM_OFF - 8, width), F32)


def finish_kernel(cfg, samples, node_ref, dloc_ref, sloc_ref, recv_ref, de_ref, nrow_ref, w_e1, grad_ref, dv_ref, dout_ref, full_ref, fold_ref, gsend_ref):
    tile_nodes = node_ref.shape[1]
    step = pl.program_id(0)

    @pl.when(step == 0)
    def _():
        fold_ref[...] = onehot_rows(nrow_ref[:1], 0, tile_nodes)
        gsend_ref[...] = jnp.zeros_like(gsend_ref)

    dv_ref[0] = finish_sample(node_ref[0], dloc_ref[0], sloc_ref[0], recv_ref[:, 0], fold_ref, gsend_ref, w_e1.at[0])
    dout_ref[0] = de_ref[0]

    @pl.when(step == samples - 1)
    def _():
        lay_grads(full_ref, grad_ref, gsend_ref)


def adam_kernel(shards, both_ref, *refs):
    dp = lax.axis_index('dp')
    masters, ones, twos, new_masters, new_ones, new_twos = (refs[i:i + 5] for i in range(0, len(refs), 5))
    layers, gains, lanes = masters[-1].shape
    norm = both_ref[:, NORM_OFF:NORM_OFF + gains, :lanes]
    for shard in range(1, shards):
        norm = jnp.where(dp == shard, both_ref[:, NORM_OFF:NORM_OFF + gains, shard * lanes:(shard + 1) * lanes], norm)
    sums = [both_ref[:, off:off + rows, :] for rows, off in zip(SHARD_ROWS, SHARD_OFF)] + [norm]
    for slot, grad_sum in enumerate(sums):
        results = adamw_update(masters[slot][...], grad_sum, ones[slot][...], twos[slot][...])
        for ref, value in zip((new_masters[slot], new_ones[slot], new_twos[slot]), results):
            ref[...] = value


def tail_kernel(tiles, shards, full_ref, part_ref, out_ref, half_buf, x_buf, own, rs_buf, piece, gath, s0, r0, s1, r1, s2, r2, s3, r3):
    me = lax.axis_index('sp')
    dp = lax.axis_index('dp')
    core = lax.rem(dp, 2)
    chip = dp // 2
    chips = shards // 2
    partner = (me, dp + 1 - 2 * core)
    away = line_first(chips)
    spots = [lax.rem(chip + offset, chips) for offset in away]
    line = [(me, spot * 2 + core) for spot in spots]
    plane = tile_peers(tiles)
    greet([partner] + line + plane)
    greeted(1 + len(line) + len(plane))

    pair = [pltpu.make_async_remote_copy(src_ref=full_ref.at[spot * 2 + 1 - core], dst_ref=half_buf.at[spot], send_sem=s0.at[k], recv_sem=r0.at[k], device_id=partner, device_id_type=MESH_ID) for k, spot in enumerate(spots + [chip])]
    for copy in pair:
        copy.start()
    total = part_ref[0]
    for shard in range(1, shards):
        total += part_ref[shard]
    own[1] = total
    hops = []
    for k, spot in enumerate(spots):
        pair[k].wait()
        half_buf[spot] += full_ref[spot * 2 + core]
        hop = pltpu.make_async_remote_copy(src_ref=half_buf.at[spot], dst_ref=x_buf.at[chip], send_sem=s1.at[k], recv_sem=r1.at[k], device_id=line[k], device_id_type=MESH_ID)
        hop.start()
        hops.append(hop)
    pair[-1].wait()
    total = half_buf[chip] + full_ref[dp]
    for hop, offset in zip(hops, away):
        hop.wait()
        total += x_buf[lax.rem(chip + chips - offset, chips)]
    own[0] = total

    rows = FULL_ROWS // tiles
    cuts = []
    for k, peer in enumerate(plane):
        cut = pltpu.make_async_remote_copy(src_ref=own.at[:, pl.ds(pl.multiple_of(peer[0] * rows, rows), rows)], dst_ref=rs_buf.at[me], send_sem=s2.at[k], recv_sem=r2.at[k], device_id=peer, device_id_type=MESH_ID)
        cut.start()
        cuts.append(cut)
    here = pl.ds(pl.multiple_of(me * rows, rows), rows)
    for cut in cuts:
        cut.wait()
    total = own[:, here, :]
    for offset in range(1, tiles):
        total += rs_buf[lax.rem(me + offset, tiles)]
    piece[...] = total
    gath[:, here, :] = total
    sends = []
    for k, peer in enumerate(plane):
        send = pltpu.make_async_remote_copy(src_ref=piece, dst_ref=gath.at[:, here], send_sem=s3.at[k], recv_sem=r3.at[k], device_id=peer, device_id_type=MESH_ID)
        send.start()
        sends.append(send)
    for send in sends:
        send.wait()
    out_ref[...] = gath[...]


def whole(shape):
    zeros = (0,) * len(shape)
    return pl.BlockSpec(shape, lambda s: zeros)


def per_sample(rows, width):
    return pl.BlockSpec((1, rows, width), lambda s: (s, 0, 0))


def slot_spec(tiles, slots, width):
    return pl.BlockSpec((tiles, 1, slots, width), lambda s: (0, s, 0, 0))


PARAMS = dict(vmem_limit_bytes=63 << 20)


def grid_params():
    return pltpu.CompilerParams(dimension_semantics=("arbitrary",), **PARAMS)


def remote_params(number):
    return pltpu.CompilerParams(collective_id=number, has_side_effects=True, **PARAMS)


def slot_sems(samples, tiles):
    return [pltpu.SemaphoreType.DMA((samples, tiles)), pltpu.SemaphoreType.DMA((samples, tiles)), pltpu.SemaphoreType.DMA((samples,))]


def shard_sems(shards):
    return [pltpu.SemaphoreType.DMA((shards,)), pltpu.SemaphoreType.DMA((shards,)), pltpu.SemaphoreType.DMA]


def solution(mesh):
    lat_spec = P('dp', 'sp', None)
    edge_spec = P('sp')
    mat_spec = P(None, 'dp', None)
    norm_spec = P(None, None, 'dp')
    param_specs = (mat_spec, mat_spec, mat_spec, mat_spec, norm_spec)
    tiles = mesh.shape['sp']
    dp_size = mesh.shape['dp']

    def spread(value, axis):
        count = mesh.shape[axis]
        return lax.all_to_all(jnp.broadcast_to(value[None], (count,) + value.shape), axis, 0, 0, tiled=True)

    def join(stacked, dim):
        moved = jnp.moveaxis(stacked, 0, dim)
        return moved.reshape(moved.shape[:dim] + (moved.shape[dim] * moved.shape[dim + 1],) + moved.shape[dim + 2:])

    def scatter_sum(value, axis, dim):
        count = mesh.shape[axis]
        split = value.reshape(value.shape[:dim] + (count, value.shape[dim] // count) + value.shape[dim + 1:])
        return jnp.sum(lax.all_to_all(jnp.moveaxis(split, dim, 0), axis, 0, 0, tiled=True), axis=0)

    def gather_weights(masters, layer_idx):
        mat_list = [join(spread(master[layer_idx].astype(BF), 'dp'), 0) for master in masters[:4]]
        norm_rows = join(spread(masters[4][layer_idx].astype(BF), 'dp'), 1).astype(F32)
        return mat_list[0], mat_list[1], mat_list[2], mat_list[3], norm_rows

    def reduce_grads(grads):
        parts = [scatter_sum(grad_full, 'dp', 0) for grad_full in grads[:4]] + [scatter_sum(grads[4], 'dp', 1)]
        return tuple(jnp.sum(spread(part, 'sp'), axis=0) for part in parts)

    def general_step(node_lat, edge_lat, senders, edge_mask, node_cot, edge_cot, masters):
        batch_size, tile_nodes, lat_width = node_lat.shape
        degree = edge_lat.shape[1] // tile_nodes
        layers = masters[0].shape[0]
        mask_f = edge_mask.astype(F32).reshape(tile_nodes, degree)
        mask_b = mask_f.astype(BF)
        node_x = node_lat
        edge_x = edge_lat.reshape(batch_size, tile_nodes, degree, lat_width)
        records = []
        for layer_idx in range(layers):
            layer_wts = gather_weights(masters, layer_idx)
            node_all = join(spread(node_x, 'sp'), 1)
            node_new, edge_new, saved = layer_forward(node_x, node_all, edge_x, senders, mask_b, layer_wts)
            records.append((node_x, edge_x, saved))
            node_x = node_new
            edge_x = edge_new
        d_node = node_cot
        d_edge = edge_cot.reshape(batch_size, tile_nodes, degree, lat_width)
        grads_rev = []
        for layer_idx in reversed(range(layers)):
            layer_wts = gather_weights(masters, layer_idx)
            node_in, edge_in, saved = records[layer_idx]
            d_local, scattered, d_edge, grads = layer_backward(d_node, d_edge, node_in, edge_in, senders, mask_f, saved, layer_wts, tile_nodes * tiles)
            returned = scatter_sum(scattered, 'sp', 1)
            d_node = (d_local + returned).astype(BF)
            grads_rev.append(reduce_grads(grads))
        layer_grads = grads_rev[::-1]
        sums = tuple(jnp.stack([per_layer[slot] for per_layer in layer_grads], axis=0) for slot in range(5))
        return sums + (d_node, d_edge.reshape(edge_lat.shape))

    def compact_step(node_lat, edge_lat, send_all, edge_mask, node_cot, edge_cot, masters):
        samples, tile_nodes, width = node_lat.shape
        edges = edge_lat.shape[1]
        cfg = (tiles, SLOTS, tile_nodes, edges // tile_nodes)
        cols = tile_nodes + tiles * SLOTS
        layers = masters[0].shape[0]
        sd = jax.ShapeDtypeStruct
        vmem = pl.BlockSpec(memory_space=pltpu.VMEM)
        hbm = pl.BlockSpec(memory_space=pl.ANY)
        last = samples - 1

        def early(rows):
            return pl.BlockSpec((1, rows, width), lambda s: (jnp.minimum(s, last), 0, 0))

        def late(rows):
            return pl.BlockSpec((1, rows, width), lambda s: (jnp.maximum(s - samples, 0), 0, 0))

        node_b = sd((samples, tile_nodes, width), BF)
        node_f = sd((samples, tile_nodes, width), F32)
        edge_b = sd((samples, edges, width), BF)
        grad_f = sd((GRAD_ROWS, width), F32)
        slot_b = sd((tiles, samples, SLOTS, width), BF)
        full_f = sd((dp_size, FULL_ROWS, width), F32)
        grow_b = sd((8, edges), jnp.int32)
        nrow_b = sd((8, tiles * SLOTS), jnp.int32)
        mcol_b = sd((edges, LANES), F32)
        mrow_b = sd((8, edges), F32)
        weights_b = [sd((layers, rows * dp_size, width), BF) for rows in SHARD_ROWS] + [sd((layers, 8, width), F32)]

        def full_specs(shapes):
            return [whole(item.shape) for item in shapes]

        def scratch(shape, kind=BF):
            return pltpu.VMEM(shape, kind)

        slot_v = scratch(slot_b.shape)
        drop_v = scratch((cols, edges))
        dpre_v = scratch((edges, width))
        fold_v = scratch((tile_nodes, tiles * SLOTS))
        gsend_v = scratch((width, width), F32)
        tables_b = [grow_b, nrow_b, mcol_b, mrow_b]
        outs = pl.pallas_call(
            functools.partial(open_kernel, cfg, dp_size), grid=(2 * samples,),
            out_shape=[node_b, edge_b, edge_b, node_b, node_b, node_b, edge_b, node_f, node_f, grad_f] + tables_b + weights_b + [slot_b],
            in_specs=[whole((tiles, edges)), whole((1, edges)), whole(node_b.shape), early(tile_nodes), early(edges), late(tile_nodes), late(edges)] + [whole(master.shape) for master in masters],
            out_specs=[early(tile_nodes), early(edges), early(edges), early(tile_nodes), early(tile_nodes), early(tile_nodes), late(edges), late(tile_nodes), late(tile_nodes)] + full_specs([grad_f] + tables_b + weights_b) + [hbm],
            scratch_shapes=[scratch(mcol_b.shape, jnp.int32), scratch((edges, cols)), drop_v, scratch((tiles * SLOTS, tile_nodes)), scratch((cols, width)), dpre_v, scratch(edge_b.shape), scratch(node_b.shape),
                            slot_v, slot_v, slot_v, slot_v, scratch((layers, PART_ROWS, width)), scratch((layers, dp_size, PART_ROWS, width))]
            + slot_sems(samples, tiles) + slot_sems(samples, tiles) + slot_sems(samples, tiles) + shard_sems(dp_size) + shard_sems(dp_size),
            name='open', compiler_params=remote_params(1))(send_all, edge_mask.reshape(1, edges), node_lat, node_lat, edge_lat, node_cot, edge_cot, *masters)
        v_one, h_e, y_e, sums, h_n, y_n, d_edge, d_loc, s_loc, grad_two, grow, nrow, mcol, mrow = outs[:14]
        weights = outs[14:-1]
        recv_three = outs[-1]

        node_s = per_sample(tile_nodes, width)
        edge_s = per_sample(edges, width)
        d_edge0, d_loc0, s_loc0, grad_one, recv_four, part_two = pl.pallas_call(
            functools.partial(backward_kernel, cfg, dp_size), grid=(samples,),
            out_shape=(edge_b, node_f, node_f, grad_f, slot_b, full_f),
            in_specs=[node_s, edge_s, edge_s, edge_s, node_s, node_s, node_s, edge_s] + full_specs([grow_b, mrow_b, mcol_b, nrow_b] + weights_b + [node_b, node_f, node_f, slot_b, grad_f]),
            out_specs=[edge_s, node_s, node_s, whole(grad_f.shape), hbm, hbm],
            scratch_shapes=[drop_v, dpre_v, fold_v, gsend_v, scratch(node_b.shape), scratch(full_f.shape, F32), slot_v] + slot_sems(samples, tiles) + shard_sems(dp_size),
            name='backward_one', compiler_params=remote_params(2))(node_lat, edge_lat, h_e, y_e, sums, h_n, y_n, d_edge, grow, mrow, mcol, nrow, *weights, v_one, d_loc, s_loc, recv_three, grad_two)

        d_node, d_edge, full_one = pl.pallas_call(
            functools.partial(finish_kernel, cfg, samples), grid=(samples,),
            out_shape=(node_b, edge_b, full_f),
            in_specs=[node_s, node_s, node_s, slot_spec(tiles, SLOTS, width), edge_s] + full_specs([nrow_b, weights_b[0], grad_f]),
            out_specs=[node_s, edge_s, whole(full_f.shape)],
            scratch_shapes=[fold_v, gsend_v],
            name='finish', compiler_params=grid_params())(node_lat, d_loc0, s_loc0, recv_four, d_edge0, nrow, weights[0], grad_one)

        rows = FULL_ROWS // tiles
        few = pltpu.SemaphoreType.DMA((tiles,))
        both_f = (layers, FULL_ROWS, width)
        half_v = scratch((dp_size // 2, FULL_ROWS, width), F32)
        both = pl.pallas_call(
            functools.partial(tail_kernel, tiles, dp_size),
            out_shape=sd(both_f, F32), in_specs=[vmem, vmem], out_specs=vmem,
            scratch_shapes=[half_v, half_v, scratch(both_f, F32), scratch((tiles, layers, rows, width), F32), scratch((layers, rows, width), F32), scratch(both_f, F32)] + [few] * 8,
            name='tail', compiler_params=remote_params(3))(full_one, part_two)
        return both, d_node, d_edge

    def general_both(*args):
        result = general_step(*args)
        lanes = result[4].shape[-1]
        first = result[0]
        norm = lax.dynamic_update_slice(jnp.zeros((first.shape[0], FULL_ROWS - NORM_OFF, first.shape[-1]), F32), result[4], (0, 0, lax.axis_index('dp') * lanes))
        return jnp.concatenate(result[:4] + (norm,), axis=1), result[5], result[6]

    def train_step(node_lat, edge_lat, senders, edge_mask, node_cot, edge_cot, w_edge1, w_edge2, w_node1, w_node2, norm_par, mom_edge1, mom_edge2, mom_node1, mom_node2, mom_norm, vel_edge1, vel_edge2, vel_node1, vel_node2, vel_norm):
        masters = (w_edge1, w_edge2, w_node1, w_node2, norm_par)
        moments_one = (mom_edge1, mom_edge2, mom_node1, mom_node2, mom_norm)
        moments_two = (vel_edge1, vel_edge2, vel_node1, vel_node2, vel_norm)
        tile_nodes = node_lat.shape[1]
        lines = senders.shape[0] // LANES
        vmem = pl.BlockSpec(memory_space=pltpu.VMEM)
        few = pltpu.SemaphoreType.DMA((tiles,))
        send_all, most = pl.pallas_call(
            functools.partial(ids_kernel, tiles, SLOTS, tile_nodes),
            out_shape=(jax.ShapeDtypeStruct((tiles, lines * LANES), jnp.int32), jax.ShapeDtypeStruct((8, LANES), F32)),
            in_specs=[vmem], out_specs=(vmem, vmem), scratch_shapes=[pltpu.VMEM((tiles, lines, LANES), jnp.int32), few, few],
            name='ids', compiler_params=remote_params(0))(senders.reshape(lines, LANES))
        fits = most[0, 0] <= SLOTS

        def unsettled(state):
            return jnp.logical_not(state[0])

        def settle(state):
            return (True,) + general_both(node_lat, edge_lat, senders, edge_mask, node_cot, edge_cot, masters)

        state = (fits,) + compact_step(node_lat, edge_lat, send_all, edge_mask, node_cot, edge_cot, masters)
        both, d_node, d_edge = lax.while_loop(unsettled, settle, state)[1:]
        state = masters + moments_one + moments_two
        new_state = pl.pallas_call(
            functools.partial(adam_kernel, dp_size), out_shape=[jax.ShapeDtypeStruct(item.shape, F32) for item in state],
            in_specs=[vmem] * (len(state) + 1), out_specs=[vmem] * len(state), name='adam', compiler_params=pltpu.CompilerParams(**PARAMS))(both, *state)
        return tuple(new_state) + (d_node, d_edge)

    return jax.shard_map(train_step, mesh=mesh, in_specs=(lat_spec, lat_spec, edge_spec, edge_spec, lat_spec, lat_spec) + param_specs + param_specs + param_specs, out_specs=param_specs + param_specs + param_specs + (lat_spec, lat_spec), check_vma=False)
```

```python
import functools

import jax
import jax.numpy as jnp
from jax import lax
from jax.experimental import pallas as pl
from jax.experimental.layout import Layout, with_layout_constraint
from jax.experimental.pallas import tpu as pltpu
from jax.sharding import PartitionSpec as P

NORM_EPS = 1e-5
LEARN_RATE = 1e-3
BETA_ONE = 0.9
BETA_TWO = 0.95
ADAM_EPS = 1e-8
DECAY = 0.1
STEP = 10

BF = jnp.bfloat16
F32 = jnp.float32
SLOTS = 80
MESH_ID = pl.DeviceIdType.MESH


def ring_gap(offset, count):
    return min(offset % count, -offset % count)


def far_first(tiles):
    side = int(tiles ** 0.5)
    return sorted(range(1, tiles), key=lambda offset: -ring_gap(offset // side, side) - ring_gap(offset, side))


def line_first(count):
    return sorted(range(1, count), key=lambda offset: -ring_gap(offset, count))

LANES = 128
SHARD_ROWS = (96, 32, 64, 32)
SHARD_OFF = (0, 96, 128, 192)
NORM_OFF = 224
PART_ROWS = 240
FULL_ROWS = 256
GRAD_ROWS = 1800


def contract(left_op, right_op, left_dims, right_dims):
    return lax.dot_general(left_op, right_op, ((left_dims, right_dims), ((), ())), preferred_element_type=jnp.float32)


def norm_forward(out_b, norm_gain, norm_bias):
    values = out_b.astype(jnp.float32)
    centered = values - jnp.mean(values, axis=-1, keepdims=True)
    inv_std = lax.rsqrt(jnp.mean(centered * centered, axis=-1, keepdims=True) + NORM_EPS)
    normed = centered * inv_std
    return normed * norm_gain + norm_bias, normed, inv_std


def mlp_tail(pre_act, w_two, norm_gain, norm_bias):
    pre_b = pre_act.astype(jnp.bfloat16)
    hidden_act = jax.nn.silu(pre_b.astype(jnp.float32)).astype(jnp.bfloat16)
    last_dim = hidden_act.ndim - 1
    out_b = contract(hidden_act, w_two, (last_dim,), (0,)).astype(jnp.bfloat16)
    branch, normed, inv_std = norm_forward(out_b, norm_gain, norm_bias)
    return branch, (pre_b, hidden_act, normed, inv_std)


def mlp_back(d_branch, saved, w_one, w_two, norm_gain):
    pre_b, hidden_act, normed, inv_std = saved
    last_dim = hidden_act.ndim - 1
    lead_dims = tuple(range(last_dim))
    d_gain = jnp.sum(d_branch * normed, axis=lead_dims)
    d_bias = jnp.sum(d_branch, axis=lead_dims)
    d_norm = d_branch * norm_gain
    d_out = (inv_std * (d_norm - jnp.mean(d_norm, axis=-1, keepdims=True) - normed * jnp.mean(d_norm * normed, axis=-1, keepdims=True))).astype(jnp.bfloat16)
    d_two = contract(hidden_act, d_out, lead_dims, lead_dims)
    d_act = contract(d_out, w_two, (last_dim,), (1,)).astype(jnp.bfloat16)
    pre_f = pre_b.astype(jnp.float32)
    gate_sig = jax.nn.sigmoid(pre_f)
    d_pre = (d_act.astype(jnp.float32) * gate_sig * (1.0 + pre_f * (1.0 - gate_sig))).astype(jnp.bfloat16)
    d_in = contract(d_pre, w_one, (last_dim,), (1,))
    return d_pre, d_in, d_two, d_gain, d_bias


def layer_forward(node_x, node_all, edge_x, senders, mask_b, layer_wts):
    w_e1, w_e2, w_n1, w_n2, norm_rows = layer_wts
    lat_width = node_x.shape[-1]
    sender_lat = jnp.take(node_all, senders, axis=1).reshape(edge_x.shape)
    pre_e = (contract(edge_x, w_e1[:lat_width], (3,), (0,))
             + contract(sender_lat, w_e1[lat_width:2 * lat_width], (3,), (0,))
             + contract(node_x, w_e1[2 * lat_width:], (2,), (0,))[:, :, None, :])
    branch_e, saved_e = mlp_tail(pre_e, w_e2, norm_rows[0], norm_rows[1])
    edge_new = (edge_x.astype(jnp.float32) + branch_e).astype(jnp.bfloat16)
    node_sum = jnp.einsum('bngd,ng->bnd', edge_new, mask_b, preferred_element_type=jnp.float32).astype(jnp.bfloat16)
    pre_n = contract(node_x, w_n1[:lat_width], (2,), (0,)) + contract(node_sum, w_n1[lat_width:], (2,), (0,))
    branch_n, saved_n = mlp_tail(pre_n, w_n2, norm_rows[2], norm_rows[3])
    node_new = (node_x.astype(jnp.float32) + branch_n).astype(jnp.bfloat16)
    return node_new, edge_new, (sender_lat, node_sum, saved_e, saved_n)


def layer_backward(d_node_new, d_edge_new, node_x, edge_x, senders, mask_f, saved, layer_wts, total_nodes):
    w_e1, w_e2, w_n1, w_n2, norm_rows = layer_wts
    sender_lat, node_sum, saved_e, saved_n = saved
    batch_size, tile_nodes, degree, lat_width = edge_x.shape
    d_res_n = d_node_new.astype(jnp.float32)
    d_pre_n, d_in_n, d_wn2, d_gain_n, d_bias_n = mlp_back(d_res_n, saved_n, w_n1, w_n2, norm_rows[2])
    d_wn1 = jnp.concatenate([contract(node_x, d_pre_n, (0, 1), (0, 1)), contract(node_sum, d_pre_n, (0, 1), (0, 1))], axis=0)
    d_sum = d_in_n[..., lat_width:].astype(jnp.bfloat16)
    d_res_e = (d_edge_new.astype(jnp.float32) + d_sum.astype(jnp.float32)[:, :, None, :] * mask_f[None, :, :, None]).astype(jnp.bfloat16).astype(jnp.float32)
    d_pre_e, d_in_e, d_we2, d_gain_e, d_bias_e = mlp_back(d_res_e, saved_e, w_e1, w_e2, norm_rows[0])
    recv_grad = contract(node_x, d_pre_e.reshape(batch_size, tile_nodes, -1), (0, 1), (0, 1))
    d_we1 = jnp.concatenate([contract(edge_x, d_pre_e, (0, 1, 2), (0, 1, 2)), contract(sender_lat, d_pre_e, (0, 1, 2), (0, 1, 2)), recv_grad.reshape(lat_width, degree, -1).sum(axis=1)], axis=0)
    d_edge_x = (d_res_e + d_in_e[..., :lat_width]).astype(jnp.bfloat16)
    d_sender = d_in_e[..., lat_width:2 * lat_width].reshape(batch_size, tile_nodes * degree, lat_width)
    scattered = jnp.zeros((batch_size, total_nodes, lat_width), jnp.float32).at[:, senders].add(d_sender)
    d_local = d_res_n + d_in_n[..., :lat_width] + d_in_e[..., 2 * lat_width:].sum(axis=2)
    grads = (d_we1, d_we2, d_wn1, d_wn2, jnp.stack([d_gain_e, d_bias_e, d_gain_n, d_bias_n]))
    return d_local, scattered, d_edge_x, grads


def row_major(value):
    return with_layout_constraint(value, Layout(tuple(range(value.ndim))))


def adamw_update(master, grad_sum, moment_one, moment_two):
    corr_one = 1.0 - BETA_ONE ** STEP
    corr_two = 1.0 - BETA_TWO ** STEP
    one_new = BETA_ONE * moment_one + (1.0 - BETA_ONE) * grad_sum
    two_new = BETA_TWO * moment_two + (1.0 - BETA_TWO) * grad_sum * grad_sum
    direction = (one_new / corr_one) / (jnp.sqrt(two_new / corr_two) + ADAM_EPS)
    return master - LEARN_RATE * (direction + DECAY * master), one_new, two_new


def dot_nn(left_op, right_op):
    return lax.dot_general(left_op, right_op, (((1,), (0,)), ((), ())), preferred_element_type=F32)


def dot_nt(left_op, right_op):
    return lax.dot_general(left_op, right_op, (((1,), (1,)), ((), ())), preferred_element_type=F32)


def dot_tn(left_op, right_op):
    return lax.dot_general(left_op, right_op, (((0,), (0,)), ((), ())), preferred_element_type=F32)


def split_three(values):
    high = values.astype(BF)
    rest = values - high.astype(F32)
    mid = rest.astype(BF)
    low = (rest - mid.astype(F32)).astype(BF)
    return high, mid, low


def to_bf(cond):
    return jnp.where(cond, 1.0, 0.0).astype(BF)


def onehot_cols(col_ids, first, width):
    rows = col_ids.shape[0]
    lane = lax.broadcasted_iota(jnp.int32, (rows, LANES), 1)
    parts = [to_bf(col_ids == lane + (first + LANES * i)) for i in range(width // LANES)]
    return jnp.concatenate(parts, axis=1)


def onehot_rows(row_ids, first, height):
    width = row_ids.shape[1]
    sub = lax.broadcasted_iota(jnp.int32, (height, width), 0) + first
    return to_bf(row_ids == sub)


def norm_parts(out_b):
    values = out_b.astype(F32)
    centered = values - jnp.mean(values, axis=-1, keepdims=True)
    inv_std = lax.rsqrt(jnp.mean(centered * centered, axis=-1, keepdims=True) + NORM_EPS)
    return centered * inv_std, inv_std


def branch_forward(pre_act, w_two, gain, bias):
    pre_b = pre_act.astype(BF)
    pre_f = pre_b.astype(F32)
    sig = jax.nn.sigmoid(pre_f)
    act = (pre_f * sig).astype(BF)
    out_b = dot_nn(act, w_two).astype(BF)
    normed, inv_std = norm_parts(out_b)
    return normed * gain + bias, (pre_b, act, sig, normed, inv_std, out_b)


def branch_backward(d_branch, pre_b, act, sig, normed, inv_std, w_two, gain):
    d_norm = d_branch * gain
    mean_one = jnp.mean(d_norm, axis=-1, keepdims=True)
    mean_two = jnp.mean(d_norm * normed, axis=-1, keepdims=True)
    d_out = (inv_std * (d_norm - mean_one - normed * mean_two)).astype(BF)
    d_two = dot_tn(act, d_out)
    d_act = dot_nt(d_out, w_two).astype(BF)
    pre_f = pre_b.astype(F32)
    d_pre = (d_act.astype(F32) * sig * (1.0 + pre_f * (1.0 - sig))).astype(BF)
    d_gain = jnp.sum(d_branch * normed, axis=0, keepdims=True)
    d_bias = jnp.sum(d_branch, axis=0, keepdims=True)
    return d_pre, d_two, d_gain, d_bias


def load_weights(part_ref, layer, all_wts, norm_ref):
    norm = jnp.zeros((PART_ROWS - NORM_OFF, part_ref.shape[-1]), F32)
    for shard in range(part_ref.shape[0]):
        for ref, rows, off in zip(all_wts, SHARD_ROWS, SHARD_OFF):
            ref[layer, shard * rows:(shard + 1) * rows, :] = part_ref[shard, off:off + rows, :]
        norm += part_ref[shard, NORM_OFF:, :].astype(F32)
    norm_ref[layer] = norm[:8]


def cast_parts(master_refs, part_ref):
    dp = lax.axis_index('dp')
    layers, gains, lanes = master_refs[-1].shape
    width = part_ref.shape[-1]
    spot = lax.broadcasted_iota(jnp.int32, (lanes, width), 1) - lanes * dp
    place = to_bf(spot == lax.broadcasted_iota(jnp.int32, (lanes, width), 0))
    for layer in range(layers):
        for ref, rows, off in zip(master_refs, SHARD_ROWS, SHARD_OFF):
            part_ref[layer, off:off + rows, :] = ref[layer].astype(BF)
        norm = jnp.concatenate([master_refs[-1][layer], jnp.zeros((PART_ROWS - NORM_OFF - gains, lanes), F32)], axis=0)
        part_ref[layer, NORM_OFF:, :] = dot_nn(norm.astype(BF), place).astype(BF)


def peer_tile(me, offset, side):
    row = lax.rem(me // side + offset // side, side)
    col = lax.rem(lax.rem(me, side) + offset % side, side)
    return row * side + col


def greet(peers):
    barrier = pltpu.get_barrier_semaphore()
    for peer in peers:
        pl.semaphore_signal(barrier, inc=1, device_id=peer, device_id_type=MESH_ID)


def greeted(count):
    pl.semaphore_wait(pltpu.get_barrier_semaphore(), count)


def tile_peers(tiles):
    me = lax.axis_index('sp')
    dp = lax.axis_index('dp')
    side = int(tiles ** 0.5)
    return [(peer_tile(me, offset, side), dp) for offset in far_first(tiles)]


def slot_copy(src_ref, dst_ref, sample, spot, send_sem, recv_sem, peer, me):
    return pltpu.make_async_remote_copy(src_ref=src_ref.at[peer[0], sample], dst_ref=dst_ref.at[me, sample], send_sem=send_sem.at[sample, spot], recv_sem=recv_sem.at[sample, spot], device_id=peer, device_id_type=MESH_ID)


def slots_start(src_ref, dst_ref, sample, send_sem, recv_sem, self_sem, tiles):
    me = lax.axis_index('sp')
    pltpu.make_async_copy(src_ref.at[me, sample], dst_ref.at[me, sample], self_sem.at[sample]).start()
    for spot, peer in enumerate(tile_peers(tiles)):
        slot_copy(src_ref, dst_ref, sample, spot, send_sem, recv_sem, peer, me).start()


def slots_wait(src_ref, dst_ref, sample, send_sem, recv_sem, self_sem, tiles):
    me = lax.axis_index('sp')
    pltpu.make_async_copy(src_ref.at[me, sample], dst_ref.at[me, sample], self_sem.at[sample]).wait()
    for spot, peer in enumerate(tile_peers(tiles)):
        slot_copy(src_ref, dst_ref, sample, spot, send_sem, recv_sem, peer, me).wait()


def slots_wait_all(src_ref, dst_ref, samples, send_sem, recv_sem, self_sem, tiles):
    def one(sample, carry):
        slots_wait(src_ref, dst_ref, sample, send_sem, recv_sem, self_sem, tiles)
        return carry
    lax.fori_loop(0, samples, one, 0)


def shard_peers(count):
    me = lax.axis_index('sp')
    dp = lax.axis_index('dp')
    return [(me, lax.rem(dp + offset, count)) for offset in line_first(count)]


def shard_copy(src_ref, dst_ref, spot, send_sem, recv_sem, peer, scatter):
    dp = lax.axis_index('dp')
    src = src_ref.at[peer[1]] if scatter else src_ref
    return pltpu.make_async_remote_copy(src_ref=src, dst_ref=dst_ref.at[dp], send_sem=send_sem.at[spot], recv_sem=recv_sem.at[spot], device_id=peer, device_id_type=MESH_ID)


def shards_start(src_ref, dst_ref, send_sem, recv_sem, self_sem, count, scatter):
    dp = lax.axis_index('dp')
    pltpu.make_async_copy(src_ref.at[dp] if scatter else src_ref, dst_ref.at[dp], self_sem).start()
    for spot, peer in enumerate(shard_peers(count)):
        shard_copy(src_ref, dst_ref, spot, send_sem, recv_sem, peer, scatter).start()


def shards_wait(src_ref, dst_ref, send_sem, recv_sem, self_sem, count, scatter):
    dp = lax.axis_index('dp')
    pltpu.make_async_copy(src_ref.at[dp] if scatter else src_ref, dst_ref.at[dp], self_sem).wait()
    for spot, peer in enumerate(shard_peers(count)):
        shard_copy(src_ref, dst_ref, spot, send_sem, recv_sem, peer, scatter).wait()


def chunk_maps(degree, mask_rows, mask_col):
    chunk = mask_rows.shape[1]
    nodes = chunk // degree
    sub_w = lax.broadcasted_iota(jnp.int32, (nodes, chunk), 0) * degree
    lane_w = lax.broadcasted_iota(jnp.int32, (nodes, chunk), 1)
    wide = (lane_w >= sub_w) & (lane_w < sub_w + degree)
    sub_t = lax.broadcasted_iota(jnp.int32, (chunk, nodes), 0)
    lane_t = lax.broadcasted_iota(jnp.int32, (chunk, nodes), 1) * degree
    tall = (sub_t >= lane_t) & (sub_t < lane_t + degree)
    out = dict(tall=to_bf(tall), wide=to_bf(wide), sum=jnp.where(wide, mask_rows[:1], 0.0).astype(BF))
    if mask_col is not None:
        out['spread'] = jnp.where(tall, jnp.concatenate([mask_col] * (nodes // LANES), axis=1), 0.0).astype(BF)
    return out


def make_tables(tiles, slots, tile_nodes, send_ids, mask_ref, node_ref, gcol_ref, grow_ref, nrow_ref, mcol_ref, mrow_ref, pack_ref, out_ref):
    me = lax.axis_index('sp')
    ids = send_ids[...]
    edges = ids.shape[1]
    tile_of = ids // tile_nodes
    local = (ids - tile_of * tile_nodes).astype(F32)
    row = lax.broadcasted_iota(jnp.int32, (tiles, edges), 0)
    is_me = row == me
    own_tile = jnp.sum(jnp.where(is_me, tile_of, 0), axis=0, keepdims=True)
    own_local = jnp.sum(jnp.where(is_me, local, 0.0), axis=0, keepdims=True)
    own = jnp.where(own_tile == row, 1.0, 0.0)
    inc = jnp.where((tile_of == me) & jnp.logical_not(is_me), 1.0, 0.0)
    both = jnp.concatenate([own, inc], axis=0).astype(BF)
    rank = jnp.zeros((2 * tiles, edges), F32)
    step = 256
    for blk in range(edges // step):
        first = lax.broadcasted_iota(jnp.int32, (step, edges), 0) + blk * step
        second = lax.broadcasted_iota(jnp.int32, (step, edges), 1)
        rank += dot_nn(both[:, blk * step:(blk + 1) * step], to_bf(first < second))
    slot_id = jnp.where(is_me, own_local, rank[:tiles] + (row * slots + tile_nodes).astype(F32))
    gidx = jnp.sum(own * slot_id, axis=0, keepdims=True)
    grow_ref[...] = jnp.broadcast_to(gidx, grow_ref.shape).astype(jnp.int32)
    gcol_ref[...] = jnp.transpose(jnp.broadcast_to(gidx, (LANES, edges))).astype(jnp.int32)
    mask = mask_ref[...].astype(F32)
    mrow_ref[...] = jnp.broadcast_to(mask, mrow_ref.shape)
    mcol_ref[...] = jnp.transpose(jnp.broadcast_to(mask, (LANES, edges)))
    slot_row = lax.broadcasted_iota(jnp.int32, (slots, edges), 0).astype(F32)
    cols = []
    for peer in range(tiles):
        hit = (slot_row == rank[tiles + peer:tiles + peer + 1]) & (inc[peer:peer + 1] > 0.5)
        found = jnp.sum(jnp.where(hit, local[peer:peer + 1] + 1.0, 0.0), axis=1, keepdims=True) - 1.0
        cols.append(jnp.broadcast_to(found, (slots, LANES)))
    ncol_f = jnp.concatenate(cols, axis=0)
    ncol = ncol_f.astype(jnp.int32)
    nrow_ref[...] = jnp.transpose(ncol_f)[:8].astype(jnp.int32)
    group = 4
    for part in range(tiles // group):
        rows = group * slots
        pick = onehot_cols(ncol[part * rows:(part + 1) * rows], 0, tile_nodes)
        pack_ref[part * rows:(part + 1) * rows, :] = pick
        for sample in range(out_ref.shape[1]):
            got = dot_nn(pick, node_ref[sample]).astype(BF)
            out_ref[part * group:(part + 1) * group, sample] = got.reshape(group, slots, got.shape[1])


def fill_rows(rows_ref, node, got, tile_nodes):
    rows_ref[:tile_nodes, :] = node
    rows_ref[tile_nodes:, :] = got.reshape(got.shape[0] * got.shape[1], got.shape[2])


def build_pick(gcol_ref, pick_ref):
    step = 128 * 3

    def build(i, carry):
        base = pl.multiple_of(i * step, step)
        pick_ref[pl.ds(base, step), :] = onehot_cols(gcol_ref[pl.ds(base, step), :], 0, pick_ref.shape[1])
        return carry
    lax.fori_loop(0, pick_ref.shape[0] // step, build, 0)


def fwd_sample(maps, v_c, e_c, pick_ref, rows_ref, wts, norm_ref):
    w_e1, w_e2, w_n1, w_n2 = wts
    width = e_c.shape[-1]
    w_edge, w_send, w_recv = (w_e1[i * width:(i + 1) * width, :] for i in range(w_e1.shape[0] // width))
    sent = dot_nn(pick_ref[...], rows_ref[...]).astype(BF)
    recv = dot_nn(maps['tall'], v_c).astype(BF)
    pre = dot_nn(e_c, w_edge) + dot_nn(sent, w_send) + dot_nn(recv, w_recv)
    rows = [norm_ref[i:i + 1, :] for i in range(len(SHARD_ROWS))]
    branch, edge_s = branch_forward(pre, w_e2[...], rows[0], rows[1])
    e_new = (e_c.astype(F32) + branch).astype(BF)
    sums = dot_nn(maps['sum'], e_new).astype(BF)
    pre_n = dot_nn(v_c, w_n1[:width, :]) + dot_nn(sums, w_n1[width:, :])
    branch_n, node_s = branch_forward(pre_n, w_n2[...], rows[2], rows[3])
    return e_new, sums, branch_n, edge_s, node_s


def ids_kernel(tiles, slots, tile_nodes, mine_ref, ids_ref, most_ref, wide, send_sem, recv_sem):
    me = lax.axis_index('sp')
    peers = tile_peers(tiles)
    greet(peers)
    wide[me] = mine_ref[...]
    greeted(len(peers))
    copies = [pltpu.make_async_remote_copy(src_ref=mine_ref, dst_ref=wide.at[me], send_sem=send_sem.at[spot], recv_sem=recv_sem.at[spot], device_id=peer, device_id_type=MESH_ID) for spot, peer in enumerate(peers)]
    for copy in copies:
        copy.start()
    for copy in copies:
        copy.wait()
    for line in range(wide.shape[1]):
        ids_ref[:, line * LANES:(line + 1) * LANES] = wide[:, line, :]
    tile_of = ids_ref[...] // tile_nodes
    row = lax.broadcasted_iota(jnp.int32, (tiles, LANES), 0)
    most = jnp.zeros((tiles, LANES), F32)
    for peer in range(tiles):
        count = jnp.sum(jnp.where(tile_of == peer, 1.0, 0.0), axis=1, keepdims=True)
        most = jnp.maximum(most, jnp.where(row == peer, 0.0, count))
    most_ref[...] = jnp.broadcast_to(jnp.max(most, axis=0, keepdims=True), most_ref.shape)


def open_kernel(cfg, shards, send_ids, mask_ref, nodes_ref, node_ref, edge_ref, dnode_ref, dedge_ref, m_e1, m_e2, m_n1, m_n2, m_norm,
                vout_ref, he_ref, ye_ref, sum_ref, hn_ref, yn_ref, de_ref, dloc_ref, sloc_ref, grad_ref, grow_ref, nrow_ref, mcol_ref, mrow_ref, w_e1, w_e2, w_n1, w_n2, norm_ref, recv_out,
                gcol_ref, pick_ref, drop_ref, pack_ref, rows_ref, dpre_ref, e_two, v_two, out_buf, in_buf, next_buf, in_two, part_ref, gat_ref,
                send_a, recv_a, self_a, send_b, recv_b, self_b, send_c, recv_c, self_c, send_w, recv_w, self_w, send_x, recv_x, self_x):
    tiles, slots, tile_nodes, degree = cfg
    samples = nodes_ref.shape[0]
    all_wts = (w_e1, w_e2, w_n1, w_n2)
    step = pl.program_id(0)
    weight_sems = ((send_w, recv_w, self_w), (send_x, recv_x, self_x))

    def take_weights(layer):
        shards_wait(part_ref.at[layer], gat_ref.at[layer], *weight_sems[layer], shards, False)
        load_weights(gat_ref.at[layer], layer, all_wts, norm_ref)

    @pl.when(step == 0)
    def _():
        peers = tile_peers(tiles) + shard_peers(shards)
        greet(peers)
        cast_parts((m_e1, m_e2, m_n1, m_n2, m_norm), part_ref)
        make_tables(tiles, slots, tile_nodes, send_ids, mask_ref, nodes_ref, gcol_ref, grow_ref, nrow_ref, mcol_ref, mrow_ref, pack_ref, out_buf)
        greeted(len(peers))
        for sample in range(samples):
            slots_start(out_buf, in_buf, sample, send_a, recv_a, self_a, tiles)
        for layer, sems in enumerate(weight_sems):
            shards_start(part_ref.at[layer], gat_ref.at[layer], *sems, shards, False)
        build_pick(gcol_ref, pick_ref)
        take_weights(0)

    @pl.when(step < samples)
    def _():
        slots_wait(out_buf, in_buf, step, send_a, recv_a, self_a, tiles)
        fill_rows(rows_ref, node_ref[0], in_buf[:, step], tile_nodes)
        node, edge = node_ref[0], edge_ref[0]
        e_new, sums, branch_n, edge_s, node_s = fwd_sample(chunk_maps(degree, mrow_ref[...], None), node, edge, pick_ref, rows_ref, [ref.at[0] for ref in all_wts], norm_ref.at[0])
        v_new = (node.astype(F32) + branch_n).astype(BF)
        for ref, value in ((he_ref, edge_s[0]), (ye_ref, edge_s[-1]), (sum_ref, sums), (hn_ref, node_s[0]), (yn_ref, node_s[-1]), (vout_ref, v_new)):
            ref[0] = value
        e_two[step] = e_new
        v_two[step] = v_new

        def pack(i, carry):
            rows = 4 * slots
            base = pl.multiple_of(i * rows, rows)
            got = dot_nn(pack_ref[pl.ds(base, rows), :], vout_ref[0]).astype(BF)
            next_buf[pl.ds(i * 4, 4), step] = got.reshape(4, slots, got.shape[1])
            return carry
        lax.fori_loop(0, tiles // 4, pack, 0)
        slots_start(next_buf, in_two, step, send_b, recv_b, self_b, tiles)

    @pl.when(step == samples)
    def _():
        take_weights(1)
        build_drop(grow_ref, drop_ref)
        grad_ref[...] = jnp.zeros_like(grad_ref)

    @pl.when(step >= samples)
    def _():
        sample = step - samples
        slots_wait(next_buf, in_two, sample, send_b, recv_b, self_b, tiles)
        node, edge = v_two[sample], e_two[sample]
        fill_rows(rows_ref, node, in_two[:, sample], tile_nodes)
        wts, norm = [ref.at[1] for ref in all_wts], norm_ref.at[1]
        maps = chunk_maps(degree, mrow_ref[...], mcol_ref[...])
        e_new, sums, branch_n, edge_s, node_s = fwd_sample(maps, node, edge, pick_ref, rows_ref, wts, norm)
        back_sample(maps, node, edge, sums, edge_s[:-1], node_s[:-1], dnode_ref[0].astype(F32), dedge_ref, wts, norm, grad_ref, dpre_ref, de_ref, dloc_ref)
        back_pack(dpre_ref, drop_ref, sloc_ref, out_buf, sample, tiles, slots, tile_nodes)
        slots_start(out_buf, recv_out, sample, send_c, recv_c, self_c, tiles)

    @pl.when(step == 2 * samples - 1)
    def _():
        slots_wait_all(out_buf, recv_out, samples, send_c, recv_c, self_c, tiles)


def back_sample(maps, v_c, e_c, sums, edge_s, node_s, d_node, dedge_ref, wts, norm_ref, grad_ref, dpre_ref, de_ref, dloc_ref):
    w_e1, w_e2, w_n1, w_n2 = wts
    width = e_c.shape[-1]
    w_edge, w_send, w_recv = (w_e1[i * width:(i + 1) * width, :] for i in range(w_e1.shape[0] // width))
    d_pre_n, d_wn2, d_gain_n, d_bias_n = branch_backward(d_node, *node_s, w_n2[...], norm_ref[2:3, :])
    d_in_v = dot_nt(d_pre_n, w_n1[:width, :])
    d_sum = dot_nt(d_pre_n, w_n1[width:, :]).astype(BF)
    d_res = (dedge_ref[0].astype(F32) + dot_nn(maps['spread'], d_sum)).astype(BF).astype(F32)
    d_pre, d_we2, d_gain_e, d_bias_e = branch_backward(d_res, *edge_s, w_e2[...], norm_ref[0:1, :])
    dpre_ref[...] = d_pre
    de_ref[0] = (d_res + dot_nt(d_pre, w_edge)).astype(BF)
    recv = split_three(dot_nn(maps['wide'], d_pre))
    dloc_ref[0] = d_node + d_in_v + sum(dot_nt(piece, w_recv) for piece in recv)
    blocks = [dot_tn(e_c, d_pre), None, sum(dot_tn(v_c, piece) for piece in recv), d_we2, dot_tn(v_c, d_pre_n), dot_tn(sums, d_pre_n), d_wn2]
    for i, block in enumerate(blocks):
        if block is not None:
            grad_ref[i * width:(i + 1) * width, :] += block
    rows = [d_gain_e, d_bias_e, d_gain_n, d_bias_n]
    grad_ref[len(blocks) * width:, :] += jnp.concatenate(rows + [jnp.zeros((len(rows), width), F32)], axis=0)


def back_pack(dpre_ref, drop_ref, sloc_ref, send_buf, step, tiles, slots, tile_nodes):
    sloc_ref[0] = dot_nn(drop_ref[:tile_nodes, :], dpre_ref[...])

    def pack(i, carry):
        rows = 4 * slots
        base = pl.multiple_of(tile_nodes + i * rows, 64)
        got = dot_nn(drop_ref[pl.ds(base, rows), :], dpre_ref[...]).astype(BF)
        send_buf[pl.ds(i * 4, 4), step] = got.reshape(4, slots, got.shape[1])
        return carry
    lax.fori_loop(0, tiles // 4, pack, 0)


def build_drop(grow_ref, drop_ref):
    step = 256

    def build(i, carry):
        base = pl.multiple_of(i * step, step)
        drop_ref[pl.ds(base, step), :] = onehot_rows(grow_ref[0:1, :], base, step)
        return carry
    lax.fori_loop(0, drop_ref.shape[0] // step, build, 0)


def again(pre_b, out_b):
    pre_f = pre_b.astype(F32)
    sig = jax.nn.sigmoid(pre_f)
    act = (pre_f * sig).astype(BF)
    normed, inv_std = norm_parts(out_b)
    return pre_b, act, sig, normed, inv_std


def backward_kernel(cfg, shards, node_ref, edge_ref, he_ref, ye_ref, sum_ref, hn_ref, yn_ref, dedge_ref, grow_ref, mrow_ref, mcol_ref, nrow_ref, w_e1, w_e2, w_n1, w_n2, norms_ref, vall_ref, dlall_ref, slall_ref, recv_ref, gtwo_ref,
                    de_ref, dloc_ref, sloc_ref, grad_ref, recv_out, part_out,
                    drop_ref, dpre_ref, fold_ref, gsend_ref, dv_ref, full_ref, send_buf, send_b, recv_b, self_b, send_w, recv_w, self_w):
    tiles, slots, tile_nodes, degree = cfg
    samples = vall_ref.shape[0]
    step = pl.program_id(0)

    @pl.when(step == 0)
    def _():
        peers = tile_peers(tiles) + shard_peers(shards)
        greet(peers)
        fold_ref[...] = onehot_rows(nrow_ref[:1], 0, tile_nodes)
        gsend_ref[...] = jnp.zeros_like(gsend_ref)

        def finish(sample, carry):
            dv_ref[sample] = finish_sample(vall_ref[sample], dlall_ref[sample], slall_ref[sample], recv_ref[:, sample], fold_ref, gsend_ref, w_e1.at[1])
            return carry
        lax.fori_loop(0, samples, finish, 0)
        lay_grads(full_ref, gtwo_ref, gsend_ref)
        greeted(len(peers))
        shards_start(full_ref, part_out, send_w, recv_w, self_w, shards, True)
        build_drop(grow_ref, drop_ref)
        grad_ref[...] = jnp.zeros_like(grad_ref)

    maps = chunk_maps(degree, mrow_ref[...], mcol_ref[...])
    edge_s = again(he_ref[0], ye_ref[0])
    node_s = again(hn_ref[0], yn_ref[0])
    back_sample(maps, node_ref[0], edge_ref[0], sum_ref[0], edge_s, node_s, dv_ref[step].astype(F32), dedge_ref, [ref.at[0] for ref in (w_e1, w_e2, w_n1, w_n2)], norms_ref.at[0], grad_ref, dpre_ref, de_ref, dloc_ref)
    back_pack(dpre_ref, drop_ref, sloc_ref, send_buf, step, tiles, slots, tile_nodes)
    slots_start(send_buf, recv_out, step, send_b, recv_b, self_b, tiles)

    @pl.when(step == samples - 1)
    def _():
        shards_wait(full_ref, part_out, send_w, recv_w, self_w, shards, True)
        slots_wait_all(send_buf, recv_out, samples, send_b, recv_b, self_b, tiles)


def finish_sample(node, d_loc, s_loc, got, fold_ref, gsend_ref, w_e1):
    width = node.shape[-1]
    total = s_loc + dot_nn(fold_ref[...], got.reshape(got.shape[0] * got.shape[1], width))
    pieces = split_three(total)
    w_send = w_e1[width:2 * width, :]
    gsend_ref[...] += sum(dot_tn(node, piece) for piece in pieces)
    return (d_loc + sum(dot_nt(piece, w_send) for piece in pieces)).astype(BF)


def lay_grads(full_ref, grad_ref, gsend_ref):
    shards, rows_all, width = full_ref.shape
    sources = ((grad_ref, 0), (gsend_ref, 0), (grad_ref, 2 * width))
    for shard in range(shards):
        row = SHARD_ROWS[0] * shard
        last = row + SHARD_ROWS[0]
        spot = 0
        while row < last:
            block = row // width
            count = min(last, (block + 1) * width) - row
            ref, base = sources[block]
            base = base + row - block * width
            full_ref[shard, spot:spot + count, :] = ref[base:base + count, :]
            row += count
            spot += count
        first = 3 * width
        for rows, off in zip(SHARD_ROWS[1:], SHARD_OFF[1:]):
            full_ref[shard, off:off + rows, :] = grad_ref[first + shard * rows:first + (shard + 1) * rows, :]
            first += rows * shards
        full_ref[shard, NORM_OFF:NORM_OFF + 8, :] = grad_ref[first:first + 8, :]
        full_ref[shard, NORM_OFF + 8:, :] = jnp.zeros((rows_all - NORM_OFF - 8, width), F32)


def finish_kernel(cfg, samples, node_ref, dloc_ref, sloc_ref, recv_ref, de_ref, nrow_ref, w_e1, grad_ref, dv_ref, dout_ref, full_ref, fold_ref, gsend_ref):
    tile_nodes = node_ref.shape[1]
    step = pl.program_id(0)

    @pl.when(step == 0)
    def _():
        fold_ref[...] = onehot_rows(nrow_ref[:1], 0, tile_nodes)
        gsend_ref[...] = jnp.zeros_like(gsend_ref)

    dv_ref[0] = finish_sample(node_ref[0], dloc_ref[0], sloc_ref[0], recv_ref[:, 0], fold_ref, gsend_ref, w_e1.at[0])
    dout_ref[0] = de_ref[0]

    @pl.when(step == samples - 1)
    def _():
        lay_grads(full_ref, grad_ref, gsend_ref)


def adam_kernel(shards, both_ref, *refs):
    dp = lax.axis_index('dp')
    masters, ones, twos, new_masters, new_ones, new_twos = (refs[i:i + 5] for i in range(0, len(refs), 5))
    layers, gains, lanes = masters[-1].shape
    norm = both_ref[:, NORM_OFF:NORM_OFF + gains, :lanes]
    for shard in range(1, shards):
        norm = jnp.where(dp == shard, both_ref[:, NORM_OFF:NORM_OFF + gains, shard * lanes:(shard + 1) * lanes], norm)
    sums = [both_ref[:, off:off + rows, :] for rows, off in zip(SHARD_ROWS, SHARD_OFF)] + [norm]
    for slot, grad_sum in enumerate(sums):
        results = adamw_update(masters[slot][...], grad_sum, ones[slot][...], twos[slot][...])
        for ref, value in zip((new_masters[slot], new_ones[slot], new_twos[slot]), results):
            ref[...] = value


def tail_kernel(tiles, shards, full_ref, part_ref, out_ref, half_buf, x_buf, own, rs_buf, piece, gath, s0, r0, s1, r1, s2, r2, s3, r3):
    me = lax.axis_index('sp')
    dp = lax.axis_index('dp')
    core = lax.rem(dp, 2)
    chip = dp // 2
    chips = shards // 2
    partner = (me, dp + 1 - 2 * core)
    away = line_first(chips)
    spots = [lax.rem(chip + offset, chips) for offset in away]
    line = [(me, spot * 2 + core) for spot in spots]
    plane = tile_peers(tiles)
    greet([partner] + line + plane)
    greeted(1 + len(line) + len(plane))

    pair = [pltpu.make_async_remote_copy(src_ref=full_ref.at[spot * 2 + 1 - core], dst_ref=half_buf.at[spot], send_sem=s0.at[k], recv_sem=r0.at[k], device_id=partner, device_id_type=MESH_ID) for k, spot in enumerate(spots + [chip])]
    for copy in pair:
        copy.start()
    total = part_ref[0]
    for shard in range(1, shards):
        total += part_ref[shard]
    own[1] = total
    hops = []
    for k, spot in enumerate(spots):
        pair[k].wait()
        half_buf[spot] += full_ref[spot * 2 + core]
        hop = pltpu.make_async_remote_copy(src_ref=half_buf.at[spot], dst_ref=x_buf.at[chip], send_sem=s1.at[k], recv_sem=r1.at[k], device_id=line[k], device_id_type=MESH_ID)
        hop.start()
        hops.append(hop)
    pair[-1].wait()
    total = half_buf[chip] + full_ref[dp]
    for hop, offset in zip(hops, away):
        hop.wait()
        total += x_buf[lax.rem(chip + chips - offset, chips)]
    own[0] = total

    rows = FULL_ROWS // tiles
    cuts = []
    for k, peer in enumerate(plane):
        cut = pltpu.make_async_remote_copy(src_ref=own.at[:, pl.ds(pl.multiple_of(peer[0] * rows, rows), rows)], dst_ref=rs_buf.at[me], send_sem=s2.at[k], recv_sem=r2.at[k], device_id=peer, device_id_type=MESH_ID)
        cut.start()
        cuts.append(cut)
    here = pl.ds(pl.multiple_of(me * rows, rows), rows)
    for cut in cuts:
        cut.wait()
    total = own[:, here, :]
    for offset in range(1, tiles):
        total += rs_buf[lax.rem(me + offset, tiles)]
    piece[...] = total
    gath[:, here, :] = total
    sends = []
    for k, peer in enumerate(plane):
        send = pltpu.make_async_remote_copy(src_ref=piece, dst_ref=gath.at[:, here], send_sem=s3.at[k], recv_sem=r3.at[k], device_id=peer, device_id_type=MESH_ID)
        send.start()
        sends.append(send)
    for send in sends:
        send.wait()
    out_ref[...] = gath[...]


def whole(shape):
    zeros = (0,) * len(shape)
    return pl.BlockSpec(shape, lambda s: zeros)


def per_sample(rows, width):
    return pl.BlockSpec((1, rows, width), lambda s: (s, 0, 0))


def slot_spec(tiles, slots, width):
    return pl.BlockSpec((tiles, 1, slots, width), lambda s: (0, s, 0, 0))


PARAMS = dict(vmem_limit_bytes=63 << 20)


def grid_params():
    return pltpu.CompilerParams(dimension_semantics=("arbitrary",), **PARAMS)


def remote_params(number):
    return pltpu.CompilerParams(collective_id=number, has_side_effects=True, **PARAMS)


def slot_sems(samples, tiles):
    return [pltpu.SemaphoreType.DMA((samples, tiles)), pltpu.SemaphoreType.DMA((samples, tiles)), pltpu.SemaphoreType.DMA((samples,))]


def shard_sems(shards):
    return [pltpu.SemaphoreType.DMA((shards,)), pltpu.SemaphoreType.DMA((shards,)), pltpu.SemaphoreType.DMA]


def solution(mesh):
    lat_spec = P('dp', 'sp', None)
    edge_spec = P('sp')
    mat_spec = P(None, 'dp', None)
    norm_spec = P(None, None, 'dp')
    param_specs = (mat_spec, mat_spec, mat_spec, mat_spec, norm_spec)
    tiles = mesh.shape['sp']
    dp_size = mesh.shape['dp']

    def spread(value, axis):
        count = mesh.shape[axis]
        return lax.all_to_all(jnp.broadcast_to(value[None], (count,) + value.shape), axis, 0, 0, tiled=True)

    def join(stacked, dim):
        moved = jnp.moveaxis(stacked, 0, dim)
        return moved.reshape(moved.shape[:dim] + (moved.shape[dim] * moved.shape[dim + 1],) + moved.shape[dim + 2:])

    def scatter_sum(value, axis, dim):
        count = mesh.shape[axis]
        split = value.reshape(value.shape[:dim] + (count, value.shape[dim] // count) + value.shape[dim + 1:])
        return jnp.sum(lax.all_to_all(jnp.moveaxis(split, dim, 0), axis, 0, 0, tiled=True), axis=0)

    def gather_weights(masters, layer_idx):
        mat_list = [join(spread(master[layer_idx].astype(BF), 'dp'), 0) for master in masters[:4]]
        norm_rows = join(spread(masters[4][layer_idx].astype(BF), 'dp'), 1).astype(F32)
        return mat_list[0], mat_list[1], mat_list[2], mat_list[3], norm_rows

    def reduce_grads(grads):
        parts = [scatter_sum(grad_full, 'dp', 0) for grad_full in grads[:4]] + [scatter_sum(grads[4], 'dp', 1)]
        return tuple(jnp.sum(spread(part, 'sp'), axis=0) for part in parts)

    def general_step(node_lat, edge_lat, senders, edge_mask, node_cot, edge_cot, masters):
        batch_size, tile_nodes, lat_width = node_lat.shape
        degree = edge_lat.shape[1] // tile_nodes
        layers = masters[0].shape[0]
        mask_f = edge_mask.astype(F32).reshape(tile_nodes, degree)
        mask_b = mask_f.astype(BF)
        node_x = node_lat
        edge_x = edge_lat.reshape(batch_size, tile_nodes, degree, lat_width)
        records = []
        for layer_idx in range(layers):
            layer_wts = gather_weights(masters, layer_idx)
            node_all = join(spread(node_x, 'sp'), 1)
            node_new, edge_new, saved = layer_forward(node_x, node_all, edge_x, senders, mask_b, layer_wts)
            records.append((node_x, edge_x, saved))
            node_x = node_new
            edge_x = edge_new
        d_node = node_cot
        d_edge = edge_cot.reshape(batch_size, tile_nodes, degree, lat_width)
        grads_rev = []
        for layer_idx in reversed(range(layers)):
            layer_wts = gather_weights(masters, layer_idx)
            node_in, edge_in, saved = records[layer_idx]
            d_local, scattered, d_edge, grads = layer_backward(d_node, d_edge, node_in, edge_in, senders, mask_f, saved, layer_wts, tile_nodes * tiles)
            returned = scatter_sum(scattered, 'sp', 1)
            d_node = (d_local + returned).astype(BF)
            grads_rev.append(reduce_grads(grads))
        layer_grads = grads_rev[::-1]
        sums = tuple(jnp.stack([per_layer[slot] for per_layer in layer_grads], axis=0) for slot in range(5))
        return sums + (d_node, d_edge.reshape(edge_lat.shape))

    def compact_step(node_lat, edge_lat, send_all, edge_mask, node_cot, edge_cot, masters):
        samples, tile_nodes, width = node_lat.shape
        edges = edge_lat.shape[1]
        cfg = (tiles, SLOTS, tile_nodes, edges // tile_nodes)
        cols = tile_nodes + tiles * SLOTS
        layers = masters[0].shape[0]
        sd = jax.ShapeDtypeStruct
        vmem = pl.BlockSpec(memory_space=pltpu.VMEM)
        hbm = pl.BlockSpec(memory_space=pl.ANY)
        last = samples - 1

        def early(rows):
            return pl.BlockSpec((1, rows, width), lambda s: (jnp.minimum(s, last), 0, 0))

        def late(rows):
            return pl.BlockSpec((1, rows, width), lambda s: (jnp.maximum(s - samples, 0), 0, 0))

        node_b = sd((samples, tile_nodes, width), BF)
        node_f = sd((samples, tile_nodes, width), F32)
        edge_b = sd((samples, edges, width), BF)
        grad_f = sd((GRAD_ROWS, width), F32)
        slot_b = sd((tiles, samples, SLOTS, width), BF)
        full_f = sd((dp_size, FULL_ROWS, width), F32)
        grow_b = sd((8, edges), jnp.int32)
        nrow_b = sd((8, tiles * SLOTS), jnp.int32)
        mcol_b = sd((edges, LANES), F32)
        mrow_b = sd((8, edges), F32)
        weights_b = [sd((layers, rows * dp_size, width), BF) for rows in SHARD_ROWS] + [sd((layers, 8, width), F32)]

        def full_specs(shapes):
            return [whole(item.shape) for item in shapes]

        def scratch(shape, kind=BF):
            return pltpu.VMEM(shape, kind)

        slot_v = scratch(slot_b.shape)
        drop_v = scratch((cols, edges))
        dpre_v = scratch((edges, width))
        fold_v = scratch((tile_nodes, tiles * SLOTS))
        gsend_v = scratch((width, width), F32)
        tables_b = [grow_b, nrow_b, mcol_b, mrow_b]
        outs = pl.pallas_call(
            functools.partial(open_kernel, cfg, dp_size), grid=(2 * samples,),
            out_shape=[node_b, edge_b, edge_b, node_b, node_b, node_b, edge_b, node_f, node_f, grad_f] + tables_b + weights_b + [slot_b],
            in_specs=[whole((tiles, edges)), whole((1, edges)), whole(node_b.shape), early(tile_nodes), early(edges), late(tile_nodes), late(edges)] + [whole(master.shape) for master in masters],
            out_specs=[early(tile_nodes), early(edges), early(edges), early(tile_nodes), early(tile_nodes), early(tile_nodes), late(edges), late(tile_nodes), late(tile_nodes)] + full_specs([grad_f] + tables_b + weights_b) + [hbm],
            scratch_shapes=[scratch(mcol_b.shape, jnp.int32), scratch((edges, cols)), drop_v, scratch((tiles * SLOTS, tile_nodes)), scratch((cols, width)), dpre_v, scratch(edge_b.shape), scratch(node_b.shape),
                            slot_v, slot_v, slot_v, slot_v, scratch((layers, PART_ROWS, width)), scratch((layers, dp_size, PART_ROWS, width))]
            + slot_sems(samples, tiles) + slot_sems(samples, tiles) + slot_sems(samples, tiles) + shard_sems(dp_size) + shard_sems(dp_size),
            name='open', compiler_params=remote_params(1))(send_all, edge_mask.reshape(1, edges), node_lat, node_lat, edge_lat, node_cot, edge_cot, *masters)
        v_one, h_e, y_e, sums, h_n, y_n, d_edge, d_loc, s_loc, grad_two, grow, nrow, mcol, mrow = outs[:14]
        weights = outs[14:-1]
        recv_three = outs[-1]

        node_s = per_sample(tile_nodes, width)
        edge_s = per_sample(edges, width)
        d_edge0, d_loc0, s_loc0, grad_one, recv_four, part_two = pl.pallas_call(
            functools.partial(backward_kernel, cfg, dp_size), grid=(samples,),
            out_shape=(edge_b, node_f, node_f, grad_f, slot_b, full_f),
            in_specs=[node_s, edge_s, edge_s, edge_s, node_s, node_s, node_s, edge_s] + full_specs([grow_b, mrow_b, mcol_b, nrow_b] + weights_b + [node_b, node_f, node_f, slot_b, grad_f]),
            out_specs=[edge_s, node_s, node_s, whole(grad_f.shape), hbm, hbm],
            scratch_shapes=[drop_v, dpre_v, fold_v, gsend_v, scratch(node_b.shape), scratch(full_f.shape, F32), slot_v] + slot_sems(samples, tiles) + shard_sems(dp_size),
            name='backward_one', compiler_params=remote_params(2))(node_lat, edge_lat, h_e, y_e, sums, h_n, y_n, d_edge, grow, mrow, mcol, nrow, *weights, v_one, d_loc, s_loc, recv_three, grad_two)

        d_node, d_edge, full_one = pl.pallas_call(
            functools.partial(finish_kernel, cfg, samples), grid=(samples,),
            out_shape=(node_b, edge_b, full_f),
            in_specs=[node_s, node_s, node_s, slot_spec(tiles, SLOTS, width), edge_s] + full_specs([nrow_b, weights_b[0], grad_f]),
            out_specs=[node_s, edge_s, whole(full_f.shape)],
            scratch_shapes=[fold_v, gsend_v],
            name='finish', compiler_params=grid_params())(node_lat, d_loc0, s_loc0, recv_four, d_edge0, nrow, weights[0], grad_one)

        rows = FULL_ROWS // tiles
        few = pltpu.SemaphoreType.DMA((tiles,))
        both_f = (layers, FULL_ROWS, width)
        half_v = scratch((dp_size // 2, FULL_ROWS, width), F32)
        both = pl.pallas_call(
            functools.partial(tail_kernel, tiles, dp_size),
            out_shape=sd(both_f, F32), in_specs=[vmem, vmem], out_specs=vmem,
            scratch_shapes=[half_v, half_v, scratch(both_f, F32), scratch((tiles, layers, rows, width), F32), scratch((layers, rows, width), F32), scratch(both_f, F32)] + [few] * 8,
            name='tail', compiler_params=remote_params(3))(full_one, part_two)
        return both, d_node, d_edge

    def general_both(*args):
        result = general_step(*args)
        lanes = result[4].shape[-1]
        first = result[0]
        norm = lax.dynamic_update_slice(jnp.zeros((first.shape[0], FULL_ROWS - NORM_OFF, first.shape[-1]), F32), result[4], (0, 0, lax.axis_index('dp') * lanes))
        return jnp.concatenate(result[:4] + (norm,), axis=1), result[5], result[6]

    def train_step(node_lat, edge_lat, senders, edge_mask, node_cot, edge_cot, w_edge1, w_edge2, w_node1, w_node2, norm_par, mom_edge1, mom_edge2, mom_node1, mom_node2, mom_norm, vel_edge1, vel_edge2, vel_node1, vel_node2, vel_norm):
        masters = (w_edge1, w_edge2, w_node1, w_node2, norm_par)
        moments_one = (mom_edge1, mom_edge2, mom_node1, mom_node2, mom_norm)
        moments_two = (vel_edge1, vel_edge2, vel_node1, vel_node2, vel_norm)
        tile_nodes = node_lat.shape[1]
        lines = senders.shape[0] // LANES
        vmem = pl.BlockSpec(memory_space=pltpu.VMEM)
        few = pltpu.SemaphoreType.DMA((tiles,))
        send_all, most = pl.pallas_call(
            functools.partial(ids_kernel, tiles, SLOTS, tile_nodes),
            out_shape=(jax.ShapeDtypeStruct((tiles, lines * LANES), jnp.int32), jax.ShapeDtypeStruct((8, LANES), F32)),
            in_specs=[vmem], out_specs=(vmem, vmem), scratch_shapes=[pltpu.VMEM((tiles, lines, LANES), jnp.int32), few, few],
            name='ids', compiler_params=remote_params(0))(senders.reshape(lines, LANES))
        fits = most[0, 0] <= SLOTS

        def unsettled(state):
            return jnp.logical_not(state[0])

        def settle(state):
            held = tuple(master * jnp.logical_not(state[0]).astype(F32) for master in masters)
            args = (node_lat, edge_lat, senders, edge_mask, node_cot, edge_cot, held)
            return (True,) + jax.tree.map(row_major, general_both(*jax.tree.map(row_major, args)))

        state = (fits,) + compact_step(node_lat, edge_lat, send_all, edge_mask, node_cot, edge_cot, masters)
        both, d_node, d_edge = lax.while_loop(unsettled, settle, state)[1:]
        state = masters + moments_one + moments_two
        new_state = pl.pallas_call(
            functools.partial(adam_kernel, dp_size), out_shape=[jax.ShapeDtypeStruct(item.shape, F32) for item in state],
            in_specs=[vmem] * (len(state) + 1), out_specs=[vmem] * len(state), name='adam', compiler_params=pltpu.CompilerParams(**PARAMS))(both, *state)
        return tuple(new_state) + (d_node, d_edge)

    return jax.shard_map(train_step, mesh=mesh, in_specs=(lat_spec, lat_spec, edge_spec, edge_spec, lat_spec, lat_spec) + param_specs + param_specs + param_specs, out_specs=param_specs + param_specs + param_specs + (lat_spec, lat_spec), check_vma=False)
```

```python
import functools

import jax
import jax.numpy as jnp
from jax import lax
from jax.experimental import pallas as pl
from jax.experimental.layout import Layout, with_layout_constraint
from jax.experimental.pallas import tpu as pltpu
from jax.sharding import PartitionSpec as P

NORM_EPS = 1e-5
LEARN_RATE = 1e-3
BETA_ONE = 0.9
BETA_TWO = 0.95
ADAM_EPS = 1e-8
DECAY = 0.1
STEP = 10

NODE_DIMS = (0, 1)
EDGE_DIMS = (0, 1, 2)
BF = jnp.bfloat16
F32 = jnp.float32
SLOTS = 80
MESH_ID = pl.DeviceIdType.MESH


def ring_gap(offset, count):
    return min(offset % count, -offset % count)


def far_first(tiles):
    side = int(tiles ** 0.5)
    return sorted(range(1, tiles), key=lambda offset: -ring_gap(offset // side, side) - ring_gap(offset, side))


def line_first(count):
    return sorted(range(1, count), key=lambda offset: -ring_gap(offset, count))

LANES = 128
SHARD_ROWS = (96, 32, 64, 32)
SHARD_OFF = (0, 96, 128, 192)
NORM_OFF = 224
PART_ROWS = 240
FULL_ROWS = 256
GRAD_ROWS = 1800


def contract(left_op, right_op, left_dims, right_dims):
    return lax.dot_general(left_op, right_op, ((left_dims, right_dims), ((), ())), preferred_element_type=jnp.float32)


def norm_forward(out_b, norm_gain, norm_bias):
    values = out_b.astype(jnp.float32)
    centered = values - jnp.mean(values, axis=-1, keepdims=True)
    inv_std = lax.rsqrt(jnp.mean(centered * centered, axis=-1, keepdims=True) + NORM_EPS)
    normed = centered * inv_std
    return normed * norm_gain + norm_bias, normed, inv_std


def mlp_tail(pre_act, w_two, norm_gain, norm_bias):
    pre_b = pre_act.astype(jnp.bfloat16)
    hidden_act = jax.nn.silu(pre_b.astype(jnp.float32)).astype(jnp.bfloat16)
    last_dim = hidden_act.ndim - 1
    out_b = contract(hidden_act, w_two, (last_dim,), (0,)).astype(jnp.bfloat16)
    branch, normed, inv_std = norm_forward(out_b, norm_gain, norm_bias)
    return branch, (pre_b, hidden_act, normed, inv_std)


def mlp_back(d_branch, saved, w_one, w_two, norm_gain):
    pre_b, hidden_act, normed, inv_std = saved
    last_dim = hidden_act.ndim - 1
    lead_dims = tuple(range(last_dim))
    d_gain = jnp.sum(d_branch * normed, axis=lead_dims)
    d_bias = jnp.sum(d_branch, axis=lead_dims)
    d_norm = d_branch * norm_gain
    d_out = (inv_std * (d_norm - jnp.mean(d_norm, axis=-1, keepdims=True) - normed * jnp.mean(d_norm * normed, axis=-1, keepdims=True))).astype(jnp.bfloat16)
    d_two = contract(hidden_act, d_out, lead_dims, lead_dims)
    d_act = contract(d_out, w_two, (last_dim,), (1,)).astype(jnp.bfloat16)
    pre_f = pre_b.astype(jnp.float32)
    gate_sig = jax.nn.sigmoid(pre_f)
    d_pre = (d_act.astype(jnp.float32) * gate_sig * (1.0 + pre_f * (1.0 - gate_sig))).astype(jnp.bfloat16)
    d_in = contract(d_pre, w_one, (last_dim,), (1,))
    return d_pre, d_in, d_two, d_gain, d_bias


def layer_forward(node_x, node_all, edge_x, senders, mask_b, layer_wts):
    w_e1, w_e2, w_n1, w_n2, norm_rows = layer_wts
    lat_width = node_x.shape[-1]
    sender_lat = jnp.take(node_all, senders, axis=1).reshape(edge_x.shape)
    pre_e = (contract(edge_x, w_e1[:lat_width], (3,), (0,))
             + contract(sender_lat, w_e1[lat_width:2 * lat_width], (3,), (0,))
             + contract(node_x, w_e1[2 * lat_width:], (2,), (0,))[:, :, None, :])
    branch_e, saved_e = mlp_tail(pre_e, w_e2, norm_rows[0], norm_rows[1])
    edge_new = (edge_x.astype(jnp.float32) + branch_e).astype(jnp.bfloat16)
    node_sum = jnp.einsum('bngd,ng->bnd', edge_new, mask_b, preferred_element_type=jnp.float32).astype(jnp.bfloat16)
    pre_n = contract(node_x, w_n1[:lat_width], (2,), (0,)) + contract(node_sum, w_n1[lat_width:], (2,), (0,))
    branch_n, saved_n = mlp_tail(pre_n, w_n2, norm_rows[2], norm_rows[3])
    node_new = (node_x.astype(jnp.float32) + branch_n).astype(jnp.bfloat16)
    return node_new, edge_new, (sender_lat, node_sum, saved_e, saved_n)


def layer_backward(d_node_new, d_edge_new, node_x, edge_x, senders, mask_f, saved, layer_wts, total_nodes):
    w_e1, w_e2, w_n1, w_n2, norm_rows = layer_wts
    sender_lat, node_sum, saved_e, saved_n = saved
    batch_size, tile_nodes, degree, lat_width = edge_x.shape
    d_res_n = d_node_new.astype(jnp.float32)
    d_pre_n, d_in_n, d_wn2, d_gain_n, d_bias_n = mlp_back(d_res_n, saved_n, w_n1, w_n2, norm_rows[2])
    d_wn1 = jnp.concatenate([contract(node_x, d_pre_n, NODE_DIMS, NODE_DIMS), contract(node_sum, d_pre_n, NODE_DIMS, NODE_DIMS)], axis=0)
    d_sum = d_in_n[..., lat_width:].astype(jnp.bfloat16)
    d_res_e = (d_edge_new.astype(jnp.float32) + d_sum.astype(jnp.float32)[:, :, None, :] * mask_f[None, :, :, None]).astype(jnp.bfloat16).astype(jnp.float32)
    d_pre_e, d_in_e, d_we2, d_gain_e, d_bias_e = mlp_back(d_res_e, saved_e, w_e1, w_e2, norm_rows[0])
    recv_grad = contract(node_x, d_pre_e.reshape(batch_size, tile_nodes, -1), NODE_DIMS, NODE_DIMS)
    d_we1 = jnp.concatenate([contract(edge_x, d_pre_e, EDGE_DIMS, EDGE_DIMS), contract(sender_lat, d_pre_e, EDGE_DIMS, EDGE_DIMS), recv_grad.reshape(lat_width, degree, -1).sum(axis=1)], axis=0)
    d_edge_x = (d_res_e + d_in_e[..., :lat_width]).astype(jnp.bfloat16)
    d_sender = d_in_e[..., lat_width:2 * lat_width].reshape(batch_size, tile_nodes * degree, lat_width)
    scattered = jnp.zeros((batch_size, total_nodes, lat_width), jnp.float32).at[:, senders].add(d_sender)
    d_local = d_res_n + d_in_n[..., :lat_width] + d_in_e[..., 2 * lat_width:].sum(axis=2)
    grads = (d_we1, d_we2, d_wn1, d_wn2, jnp.stack([d_gain_e, d_bias_e, d_gain_n, d_bias_n]))
    return d_local, scattered, d_edge_x, grads


def row_major(value):
    return with_layout_constraint(value, Layout(tuple(range(value.ndim))))


def adamw_update(master, grad_sum, moment_one, moment_two):
    corr_one = 1.0 - BETA_ONE ** STEP
    corr_two = 1.0 - BETA_TWO ** STEP
    one_new = BETA_ONE * moment_one + (1.0 - BETA_ONE) * grad_sum
    two_new = BETA_TWO * moment_two + (1.0 - BETA_TWO) * grad_sum * grad_sum
    direction = (one_new / corr_one) / (jnp.sqrt(two_new / corr_two) + ADAM_EPS)
    return master - LEARN_RATE * (direction + DECAY * master), one_new, two_new


def dot_nn(left_op, right_op):
    return lax.dot_general(left_op, right_op, (((1,), (0,)), ((), ())), preferred_element_type=F32)


def dot_nt(left_op, right_op):
    return lax.dot_general(left_op, right_op, (((1,), (1,)), ((), ())), preferred_element_type=F32)


def dot_tn(left_op, right_op):
    return lax.dot_general(left_op, right_op, (((0,), (0,)), ((), ())), preferred_element_type=F32)


def split_three(values):
    high = values.astype(BF)
    rest = values - high.astype(F32)
    mid = rest.astype(BF)
    low = (rest - mid.astype(F32)).astype(BF)
    return high, mid, low


def to_bf(cond):
    return jnp.where(cond, 1.0, 0.0).astype(BF)


def onehot_cols(col_ids, first, width):
    rows = col_ids.shape[0]
    lane = lax.broadcasted_iota(jnp.int32, (rows, LANES), 1)
    parts = [to_bf(col_ids == lane + (first + LANES * i)) for i in range(width // LANES)]
    return jnp.concatenate(parts, axis=1)


def onehot_rows(row_ids, first, height):
    width = row_ids.shape[1]
    sub = lax.broadcasted_iota(jnp.int32, (height, width), 0) + first
    return to_bf(row_ids == sub)


def norm_parts(out_b):
    values = out_b.astype(F32)
    centered = values - jnp.mean(values, axis=-1, keepdims=True)
    inv_std = lax.rsqrt(jnp.mean(centered * centered, axis=-1, keepdims=True) + NORM_EPS)
    return centered * inv_std, inv_std


def branch_forward(pre_act, w_two, gain, bias):
    pre_b = pre_act.astype(BF)
    pre_f = pre_b.astype(F32)
    sig = jax.nn.sigmoid(pre_f)
    act = (pre_f * sig).astype(BF)
    out_b = dot_nn(act, w_two).astype(BF)
    normed, inv_std = norm_parts(out_b)
    return normed * gain + bias, (pre_b, act, sig, normed, inv_std, out_b)


def branch_backward(d_branch, pre_b, act, sig, normed, inv_std, w_two, gain):
    d_norm = d_branch * gain
    mean_one = jnp.mean(d_norm, axis=-1, keepdims=True)
    mean_two = jnp.mean(d_norm * normed, axis=-1, keepdims=True)
    d_out = (inv_std * (d_norm - mean_one - normed * mean_two)).astype(BF)
    d_two = dot_tn(act, d_out)
    d_act = dot_nt(d_out, w_two).astype(BF)
    pre_f = pre_b.astype(F32)
    d_pre = (d_act.astype(F32) * sig * (1.0 + pre_f * (1.0 - sig))).astype(BF)
    d_gain = jnp.sum(d_branch * normed, axis=0, keepdims=True)
    d_bias = jnp.sum(d_branch, axis=0, keepdims=True)
    return d_pre, d_two, d_gain, d_bias


def load_weights(part_ref, layer, all_wts, norm_ref):
    norm = jnp.zeros((PART_ROWS - NORM_OFF, part_ref.shape[-1]), F32)
    for shard in range(part_ref.shape[0]):
        for ref, rows, off in zip(all_wts, SHARD_ROWS, SHARD_OFF):
            ref[layer, shard * rows:(shard + 1) * rows, :] = part_ref[shard, off:off + rows, :]
        norm += part_ref[shard, NORM_OFF:, :].astype(F32)
    norm_ref[layer] = norm[:8]


def cast_parts(master_refs, part_ref):
    dp = lax.axis_index('dp')
    layers, gains, lanes = master_refs[-1].shape
    width = part_ref.shape[-1]
    spot = lax.broadcasted_iota(jnp.int32, (lanes, width), 1) - lanes * dp
    place = to_bf(spot == lax.broadcasted_iota(jnp.int32, (lanes, width), 0))
    for layer in range(layers):
        for ref, rows, off in zip(master_refs, SHARD_ROWS, SHARD_OFF):
            part_ref[layer, off:off + rows, :] = ref[layer].astype(BF)
        norm = jnp.concatenate([master_refs[-1][layer], jnp.zeros((PART_ROWS - NORM_OFF - gains, lanes), F32)], axis=0)
        part_ref[layer, NORM_OFF:, :] = dot_nn(norm.astype(BF), place).astype(BF)


def peer_tile(me, offset, side):
    row = lax.rem(me // side + offset // side, side)
    col = lax.rem(lax.rem(me, side) + offset % side, side)
    return row * side + col


def greet(peers):
    barrier = pltpu.get_barrier_semaphore()
    for peer in peers:
        pl.semaphore_signal(barrier, inc=1, device_id=peer, device_id_type=MESH_ID)


def greeted(count):
    pl.semaphore_wait(pltpu.get_barrier_semaphore(), count)


def tile_peers(tiles):
    me = lax.axis_index('sp')
    dp = lax.axis_index('dp')
    side = int(tiles ** 0.5)
    return [(peer_tile(me, offset, side), dp) for offset in far_first(tiles)]


def slot_copy(src_ref, dst_ref, sample, spot, send_sem, recv_sem, peer, me):
    return pltpu.make_async_remote_copy(src_ref=src_ref.at[peer[0], sample], dst_ref=dst_ref.at[me, sample], send_sem=send_sem.at[sample, spot], recv_sem=recv_sem.at[sample, spot], device_id=peer, device_id_type=MESH_ID)


def slots_start(src_ref, dst_ref, sample, send_sem, recv_sem, self_sem, tiles):
    me = lax.axis_index('sp')
    pltpu.make_async_copy(src_ref.at[me, sample], dst_ref.at[me, sample], self_sem.at[sample]).start()
    for spot, peer in enumerate(tile_peers(tiles)):
        slot_copy(src_ref, dst_ref, sample, spot, send_sem, recv_sem, peer, me).start()


def slots_wait(src_ref, dst_ref, sample, send_sem, recv_sem, self_sem, tiles):
    me = lax.axis_index('sp')
    pltpu.make_async_copy(src_ref.at[me, sample], dst_ref.at[me, sample], self_sem.at[sample]).wait()
    for spot, peer in enumerate(tile_peers(tiles)):
        slot_copy(src_ref, dst_ref, sample, spot, send_sem, recv_sem, peer, me).wait()


def slots_wait_all(src_ref, dst_ref, samples, send_sem, recv_sem, self_sem, tiles):
    def one(sample, carry):
        slots_wait(src_ref, dst_ref, sample, send_sem, recv_sem, self_sem, tiles)
        return carry
    lax.fori_loop(0, samples, one, 0)


def shard_peers(count):
    me = lax.axis_index('sp')
    dp = lax.axis_index('dp')
    return [(me, lax.rem(dp + offset, count)) for offset in line_first(count)]


def shard_copy(src_ref, dst_ref, spot, send_sem, recv_sem, peer, scatter):
    dp = lax.axis_index('dp')
    src = src_ref.at[peer[1]] if scatter else src_ref
    return pltpu.make_async_remote_copy(src_ref=src, dst_ref=dst_ref.at[dp], send_sem=send_sem.at[spot], recv_sem=recv_sem.at[spot], device_id=peer, device_id_type=MESH_ID)


def shards_start(src_ref, dst_ref, send_sem, recv_sem, self_sem, count, scatter):
    dp = lax.axis_index('dp')
    pltpu.make_async_copy(src_ref.at[dp] if scatter else src_ref, dst_ref.at[dp], self_sem).start()
    for spot, peer in enumerate(shard_peers(count)):
        shard_copy(src_ref, dst_ref, spot, send_sem, recv_sem, peer, scatter).start()


def shards_wait(src_ref, dst_ref, send_sem, recv_sem, self_sem, count, scatter):
    dp = lax.axis_index('dp')
    pltpu.make_async_copy(src_ref.at[dp] if scatter else src_ref, dst_ref.at[dp], self_sem).wait()
    for spot, peer in enumerate(shard_peers(count)):
        shard_copy(src_ref, dst_ref, spot, send_sem, recv_sem, peer, scatter).wait()


def chunk_maps(degree, mask_rows, mask_col):
    chunk = mask_rows.shape[1]
    nodes = chunk // degree
    sub_w = lax.broadcasted_iota(jnp.int32, (nodes, chunk), 0) * degree
    lane_w = lax.broadcasted_iota(jnp.int32, (nodes, chunk), 1)
    wide = (lane_w >= sub_w) & (lane_w < sub_w + degree)
    sub_t = lax.broadcasted_iota(jnp.int32, (chunk, nodes), 0)
    lane_t = lax.broadcasted_iota(jnp.int32, (chunk, nodes), 1) * degree
    tall = (sub_t >= lane_t) & (sub_t < lane_t + degree)
    out = dict(tall=to_bf(tall), wide=to_bf(wide), sum=jnp.where(wide, mask_rows[:1], 0.0).astype(BF))
    if mask_col is not None:
        out['spread'] = jnp.where(tall, jnp.concatenate([mask_col] * (nodes // LANES), axis=1), 0.0).astype(BF)
    return out


def make_tables(tiles, slots, tile_nodes, send_ids, mask_ref, node_ref, gcol_ref, grow_ref, nrow_ref, mcol_ref, mrow_ref, pack_ref, out_ref):
    me = lax.axis_index('sp')
    ids = send_ids[...]
    edges = ids.shape[1]
    tile_of = ids // tile_nodes
    local = (ids - tile_of * tile_nodes).astype(F32)
    row = lax.broadcasted_iota(jnp.int32, (tiles, edges), 0)
    is_me = row == me
    own_tile = jnp.sum(jnp.where(is_me, tile_of, 0), axis=0, keepdims=True)
    own_local = jnp.sum(jnp.where(is_me, local, 0.0), axis=0, keepdims=True)
    own = jnp.where(own_tile == row, 1.0, 0.0)
    inc = jnp.where((tile_of == me) & jnp.logical_not(is_me), 1.0, 0.0)
    both = jnp.concatenate([own, inc], axis=0).astype(BF)
    rank = jnp.zeros((2 * tiles, edges), F32)
    step = 256
    for blk in range(edges // step):
        first = lax.broadcasted_iota(jnp.int32, (step, edges), 0) + blk * step
        second = lax.broadcasted_iota(jnp.int32, (step, edges), 1)
        rank += dot_nn(both[:, blk * step:(blk + 1) * step], to_bf(first < second))
    slot_id = jnp.where(is_me, own_local, rank[:tiles] + (row * slots + tile_nodes).astype(F32))
    gidx = jnp.sum(own * slot_id, axis=0, keepdims=True)
    grow_ref[...] = jnp.broadcast_to(gidx, grow_ref.shape).astype(jnp.int32)
    gcol_ref[...] = jnp.transpose(jnp.broadcast_to(gidx, (LANES, edges))).astype(jnp.int32)
    mask = mask_ref[...].astype(F32)
    mrow_ref[...] = jnp.broadcast_to(mask, mrow_ref.shape)
    mcol_ref[...] = jnp.transpose(jnp.broadcast_to(mask, (LANES, edges)))
    slot_row = lax.broadcasted_iota(jnp.int32, (slots, edges), 0).astype(F32)
    cols = []
    for peer in range(tiles):
        hit = (slot_row == rank[tiles + peer:tiles + peer + 1]) & (inc[peer:peer + 1] > 0.5)
        found = jnp.sum(jnp.where(hit, local[peer:peer + 1] + 1.0, 0.0), axis=1, keepdims=True) - 1.0
        cols.append(jnp.broadcast_to(found, (slots, LANES)))
    ncol_f = jnp.concatenate(cols, axis=0)
    ncol = ncol_f.astype(jnp.int32)
    nrow_ref[...] = jnp.transpose(ncol_f)[:8].astype(jnp.int32)
    group = 4
    for part in range(tiles // group):
        rows = group * slots
        pick = onehot_cols(ncol[part * rows:(part + 1) * rows], 0, tile_nodes)
        pack_ref[part * rows:(part + 1) * rows, :] = pick
        for sample in range(out_ref.shape[1]):
            got = dot_nn(pick, node_ref[sample]).astype(BF)
            out_ref[part * group:(part + 1) * group, sample] = got.reshape(group, slots, got.shape[1])


def fill_rows(rows_ref, node, got, tile_nodes):
    rows_ref[:tile_nodes, :] = node
    rows_ref[tile_nodes:, :] = got.reshape(got.shape[0] * got.shape[1], got.shape[2])


def build_pick(gcol_ref, pick_ref):
    step = 128 * 3

    def build(i, carry):
        base = pl.multiple_of(i * step, step)
        pick_ref[pl.ds(base, step), :] = onehot_cols(gcol_ref[pl.ds(base, step), :], 0, pick_ref.shape[1])
        return carry
    lax.fori_loop(0, pick_ref.shape[0] // step, build, 0)


def fwd_sample(maps, v_c, e_c, pick_ref, rows_ref, wts, norm_ref):
    w_e1, w_e2, w_n1, w_n2 = wts
    width = e_c.shape[-1]
    w_edge, w_send, w_recv = (w_e1[i * width:(i + 1) * width, :] for i in range(w_e1.shape[0] // width))
    sent = dot_nn(pick_ref[...], rows_ref[...]).astype(BF)
    recv = dot_nn(maps['tall'], v_c).astype(BF)
    pre = dot_nn(e_c, w_edge) + dot_nn(sent, w_send) + dot_nn(recv, w_recv)
    rows = [norm_ref[i:i + 1, :] for i in range(len(SHARD_ROWS))]
    branch, edge_s = branch_forward(pre, w_e2[...], rows[0], rows[1])
    e_new = (e_c.astype(F32) + branch).astype(BF)
    sums = dot_nn(maps['sum'], e_new).astype(BF)
    pre_n = dot_nn(v_c, w_n1[:width, :]) + dot_nn(sums, w_n1[width:, :])
    branch_n, node_s = branch_forward(pre_n, w_n2[...], rows[2], rows[3])
    return e_new, sums, branch_n, edge_s, node_s


def ids_kernel(tiles, slots, tile_nodes, mine_ref, ids_ref, most_ref, wide, send_sem, recv_sem):
    me = lax.axis_index('sp')
    peers = tile_peers(tiles)
    greet(peers)
    wide[me] = mine_ref[...]
    greeted(len(peers))
    copies = [pltpu.make_async_remote_copy(src_ref=mine_ref, dst_ref=wide.at[me], send_sem=send_sem.at[spot], recv_sem=recv_sem.at[spot], device_id=peer, device_id_type=MESH_ID) for spot, peer in enumerate(peers)]
    for copy in copies:
        copy.start()
    for copy in copies:
        copy.wait()
    for line in range(wide.shape[1]):
        ids_ref[:, line * LANES:(line + 1) * LANES] = wide[:, line, :]
    tile_of = ids_ref[...] // tile_nodes
    row = lax.broadcasted_iota(jnp.int32, (tiles, LANES), 0)
    most = jnp.zeros((tiles, LANES), F32)
    for peer in range(tiles):
        count = jnp.sum(jnp.where(tile_of == peer, 1.0, 0.0), axis=1, keepdims=True)
        most = jnp.maximum(most, jnp.where(row == peer, 0.0, count))
    most_ref[...] = jnp.broadcast_to(jnp.max(most, axis=0, keepdims=True), most_ref.shape)


def open_kernel(cfg, shards, send_ids, mask_ref, nodes_ref, node_ref, edge_ref, dnode_ref, dedge_ref, m_e1, m_e2, m_n1, m_n2, m_norm,
                vout_ref, he_ref, ye_ref, sum_ref, hn_ref, yn_ref, de_ref, dloc_ref, sloc_ref, grad_ref, grow_ref, nrow_ref, mcol_ref, mrow_ref, w_e1, w_e2, w_n1, w_n2, norm_ref, recv_out,
                gcol_ref, pick_ref, drop_ref, pack_ref, rows_ref, dpre_ref, e_two, v_two, out_buf, in_buf, next_buf, in_two, part_ref, gat_ref,
                send_a, recv_a, self_a, send_b, recv_b, self_b, send_c, recv_c, self_c, send_w, recv_w, self_w, send_x, recv_x, self_x):
    tiles, slots, tile_nodes, degree = cfg
    samples = nodes_ref.shape[0]
    all_wts = (w_e1, w_e2, w_n1, w_n2)
    step = pl.program_id(0)
    weight_sems = ((send_w, recv_w, self_w), (send_x, recv_x, self_x))

    def take_weights(layer):
        shards_wait(part_ref.at[layer], gat_ref.at[layer], *weight_sems[layer], shards, False)
        load_weights(gat_ref.at[layer], layer, all_wts, norm_ref)

    @pl.when(step == 0)
    def _():
        peers = tile_peers(tiles) + shard_peers(shards)
        greet(peers)
        cast_parts((m_e1, m_e2, m_n1, m_n2, m_norm), part_ref)
        make_tables(tiles, slots, tile_nodes, send_ids, mask_ref, nodes_ref, gcol_ref, grow_ref, nrow_ref, mcol_ref, mrow_ref, pack_ref, out_buf)
        greeted(len(peers))
        for sample in range(samples):
            slots_start(out_buf, in_buf, sample, send_a, recv_a, self_a, tiles)
        for layer, sems in enumerate(weight_sems):
            shards_start(part_ref.at[layer], gat_ref.at[layer], *sems, shards, False)
        build_pick(gcol_ref, pick_ref)
        take_weights(0)

    @pl.when(step < samples)
    def _():
        slots_wait(out_buf, in_buf, step, send_a, recv_a, self_a, tiles)
        fill_rows(rows_ref, node_ref[0], in_buf[:, step], tile_nodes)
        node, edge = node_ref[0], edge_ref[0]
        e_new, sums, branch_n, edge_s, node_s = fwd_sample(chunk_maps(degree, mrow_ref[...], None), node, edge, pick_ref, rows_ref, [ref.at[0] for ref in all_wts], norm_ref.at[0])
        v_new = (node.astype(F32) + branch_n).astype(BF)
        for ref, value in ((he_ref, edge_s[0]), (ye_ref, edge_s[-1]), (sum_ref, sums), (hn_ref, node_s[0]), (yn_ref, node_s[-1]), (vout_ref, v_new)):
            ref[0] = value
        e_two[step] = e_new
        v_two[step] = v_new

        def pack(i, carry):
            rows = 4 * slots
            base = pl.multiple_of(i * rows, rows)
            got = dot_nn(pack_ref[pl.ds(base, rows), :], vout_ref[0]).astype(BF)
            next_buf[pl.ds(i * 4, 4), step] = got.reshape(4, slots, got.shape[1])
            return carry
        lax.fori_loop(0, tiles // 4, pack, 0)
        slots_start(next_buf, in_two, step, send_b, recv_b, self_b, tiles)

    @pl.when(step == samples)
    def _():
        take_weights(1)
        build_drop(grow_ref, drop_ref)
        grad_ref[...] = jnp.zeros_like(grad_ref)

    @pl.when(step >= samples)
    def _():
        sample = step - samples
        slots_wait(next_buf, in_two, sample, send_b, recv_b, self_b, tiles)
        node, edge = v_two[sample], e_two[sample]
        fill_rows(rows_ref, node, in_two[:, sample], tile_nodes)
        wts, norm = [ref.at[1] for ref in all_wts], norm_ref.at[1]
        maps = chunk_maps(degree, mrow_ref[...], mcol_ref[...])
        e_new, sums, branch_n, edge_s, node_s = fwd_sample(maps, node, edge, pick_ref, rows_ref, wts, norm)
        back_sample(maps, node, edge, sums, edge_s[:-1], node_s[:-1], dnode_ref[0].astype(F32), dedge_ref, wts, norm, grad_ref, dpre_ref, de_ref, dloc_ref)
        back_pack(dpre_ref, drop_ref, sloc_ref, out_buf, sample, tiles, slots, tile_nodes)
        slots_start(out_buf, recv_out, sample, send_c, recv_c, self_c, tiles)

    @pl.when(step == 2 * samples - 1)
    def _():
        slots_wait_all(out_buf, recv_out, samples, send_c, recv_c, self_c, tiles)


def back_sample(maps, v_c, e_c, sums, edge_s, node_s, d_node, dedge_ref, wts, norm_ref, grad_ref, dpre_ref, de_ref, dloc_ref):
    w_e1, w_e2, w_n1, w_n2 = wts
    width = e_c.shape[-1]
    w_edge, w_send, w_recv = (w_e1[i * width:(i + 1) * width, :] for i in range(w_e1.shape[0] // width))
    d_pre_n, d_wn2, d_gain_n, d_bias_n = branch_backward(d_node, *node_s, w_n2[...], norm_ref[2:3, :])
    d_in_v = dot_nt(d_pre_n, w_n1[:width, :])
    d_sum = dot_nt(d_pre_n, w_n1[width:, :]).astype(BF)
    d_res = (dedge_ref[0].astype(F32) + dot_nn(maps['spread'], d_sum)).astype(BF).astype(F32)
    d_pre, d_we2, d_gain_e, d_bias_e = branch_backward(d_res, *edge_s, w_e2[...], norm_ref[0:1, :])
    dpre_ref[...] = d_pre
    de_ref[0] = (d_res + dot_nt(d_pre, w_edge)).astype(BF)
    recv = split_three(dot_nn(maps['wide'], d_pre))
    dloc_ref[0] = d_node + d_in_v + sum(dot_nt(piece, w_recv) for piece in recv)
    blocks = [dot_tn(e_c, d_pre), None, sum(dot_tn(v_c, piece) for piece in recv), d_we2, dot_tn(v_c, d_pre_n), dot_tn(sums, d_pre_n), d_wn2]
    for i, block in enumerate(blocks):
        if block is not None:
            grad_ref[i * width:(i + 1) * width, :] += block
    rows = [d_gain_e, d_bias_e, d_gain_n, d_bias_n]
    grad_ref[len(blocks) * width:, :] += jnp.concatenate(rows + [jnp.zeros((len(rows), width), F32)], axis=0)


def back_pack(dpre_ref, drop_ref, sloc_ref, send_buf, step, tiles, slots, tile_nodes):
    sloc_ref[0] = dot_nn(drop_ref[:tile_nodes, :], dpre_ref[...])

    def pack(i, carry):
        rows = 4 * slots
        base = pl.multiple_of(tile_nodes + i * rows, 64)
        got = dot_nn(drop_ref[pl.ds(base, rows), :], dpre_ref[...]).astype(BF)
        send_buf[pl.ds(i * 4, 4), step] = got.reshape(4, slots, got.shape[1])
        return carry
    lax.fori_loop(0, tiles // 4, pack, 0)


def build_drop(grow_ref, drop_ref):
    step = 256

    def build(i, carry):
        base = pl.multiple_of(i * step, step)
        drop_ref[pl.ds(base, step), :] = onehot_rows(grow_ref[0:1, :], base, step)
        return carry
    lax.fori_loop(0, drop_ref.shape[0] // step, build, 0)


def again(pre_b, out_b):
    pre_f = pre_b.astype(F32)
    sig = jax.nn.sigmoid(pre_f)
    act = (pre_f * sig).astype(BF)
    normed, inv_std = norm_parts(out_b)
    return pre_b, act, sig, normed, inv_std


def close_kernel(cfg, shards, node_ref, edge_ref, he_ref, ye_ref, sum_ref, hn_ref, yn_ref, dedge_ref, nodes_ref, grow_ref, mrow_ref, mcol_ref, nrow_ref, w_e1, w_e2, w_n1, w_n2, norms_ref, vall_ref, dlall_ref, slall_ref, recv_ref, gtwo_ref,
                 de_ref, dv_out, both_ref,
                 grad_ref, dloc_ref, sloc_ref, in_buf, part_buf, drop_ref, dpre_ref, fold_ref, gsend_ref, dv_ref, full_ref, send_buf, half_buf, x_buf, own, rs_buf, piece, ws_buf, gath,
                 send_b, recv_b, self_b, send_w, recv_w, self_w, s0, r0, s1, r1, s2, r2, s3, r3, s4, r4, s5, r5, self_s):
    tiles, slots, tile_nodes, degree = cfg
    samples = vall_ref.shape[0]
    step = pl.program_id(0)
    me = lax.axis_index('sp')
    dp = lax.axis_index('dp')
    core = lax.rem(dp, 2)
    chip = dp // 2
    chips = shards // 2
    plane = tile_peers(tiles)
    others = shard_peers(shards)

    @pl.when(step == 0)
    def _():
        greet(plane + others)
        fold_ref[...] = onehot_rows(nrow_ref[:1], 0, tile_nodes)
        gsend_ref[...] = jnp.zeros_like(gsend_ref)

        def finish(sample, carry):
            dv_ref[sample] = finish_sample(vall_ref[sample], dlall_ref[sample], slall_ref[sample], recv_ref[:, sample], fold_ref, gsend_ref, w_e1.at[1])
            return carry
        lax.fori_loop(0, samples, finish, 0)
        lay_grads(full_ref, gtwo_ref, gsend_ref)
        greeted(len(plane + others))
        shards_start(full_ref, part_buf, send_w, recv_w, self_w, shards, True)
        build_drop(grow_ref, drop_ref)
        grad_ref[...] = jnp.zeros_like(grad_ref)

    maps = chunk_maps(degree, mrow_ref[...], mcol_ref[...])
    edge_s = again(he_ref[0], ye_ref[0])
    node_s = again(hn_ref[0], yn_ref[0])
    back_sample(maps, node_ref[0], edge_ref[0], sum_ref[0], edge_s, node_s, dv_ref[step].astype(F32), dedge_ref, [ref.at[0] for ref in (w_e1, w_e2, w_n1, w_n2)], norms_ref.at[0], grad_ref, dpre_ref, de_ref, dloc_ref.at[pl.ds(step, 1)])
    back_pack(dpre_ref, drop_ref, sloc_ref.at[pl.ds(step, 1)], send_buf, step, tiles, slots, tile_nodes)
    slots_start(send_buf, in_buf, step, send_b, recv_b, self_b, tiles)

    @pl.when(step == samples - 1)
    def _():
        away = line_first(chips)
        spots = [lax.rem(chip + offset, chips) for offset in away]
        line = [(me, spot * 2 + core) for spot in spots]
        shards_wait(full_ref, part_buf, send_w, recv_w, self_w, shards, True)
        gsend_ref[...] = jnp.zeros_like(gsend_ref)
        lay_grads(full_ref, grad_ref, gsend_ref)
        pair = [pltpu.make_async_remote_copy(src_ref=full_ref.at[spot * 2 + 1 - core], dst_ref=half_buf.at[spot], send_sem=s0.at[k], recv_sem=r0.at[k], device_id=(me, dp + 1 - 2 * core), device_id_type=MESH_ID) for k, spot in enumerate(spots + [chip])]
        for copy in pair:
            copy.start()
        own[1] = sum(part_buf[shard] for shard in range(shards))
        hops = []
        for k, spot in enumerate(spots):
            pair[k].wait()
            half_buf[spot] += full_ref[spot * 2 + core]
            hop = pltpu.make_async_remote_copy(src_ref=half_buf.at[spot], dst_ref=x_buf.at[chip], send_sem=s1.at[k], recv_sem=r1.at[k], device_id=line[k], device_id_type=MESH_ID)
            hop.start()
            hops.append(hop)
        pair[-1].wait()

        def finish(sample, carry):
            slots_wait(send_buf, in_buf, sample, send_b, recv_b, self_b, tiles)
            dv_out[sample] = finish_sample(nodes_ref[sample], dloc_ref[sample], sloc_ref[sample], in_buf[:, sample], fold_ref, gsend_ref, w_e1.at[0])
            return carry
        lax.fori_loop(0, samples, finish, 0)
        own[2] = gsend_ref[...]
        total = half_buf[chip] + full_ref[dp]
        for hop, offset in zip(hops, away):
            hop.wait()
            total += x_buf[lax.rem(chip + chips - offset, chips)]
        own[0] = total

        rows = FULL_ROWS // tiles
        here = pl.ds(pl.multiple_of(me * rows, rows), rows)
        cuts = [pltpu.make_async_remote_copy(src_ref=own.at[:, pl.ds(pl.multiple_of(peer[0] * rows, rows), rows)], dst_ref=rs_buf.at[me], send_sem=s2.at[k], recv_sem=r2.at[k], device_id=peer, device_id_type=MESH_ID) for k, peer in enumerate(plane)]
        for cut in cuts:
            cut.start()
        for cut in cuts:
            cut.wait()
        piece[...] = own[:, here, :] + sum(rs_buf[lax.rem(me + offset, tiles)] for offset in range(1, tiles))
        shards_start(piece.at[2], ws_buf, s4, r4, self_s, shards, False)
        sends = [pltpu.make_async_remote_copy(src_ref=piece.at[:2], dst_ref=gath.at[:2, here], send_sem=s3.at[k], recv_sem=r3.at[k], device_id=peer, device_id_type=MESH_ID) for k, peer in enumerate(plane)]
        for send in sends:
            send.start()
        shards_wait(piece.at[2], ws_buf, s4, r4, self_s, shards, False)
        mine = rs_buf.at[me, 2]
        mine[...] = sum(ws_buf[shard] for shard in range(shards))
        more = [pltpu.make_async_remote_copy(src_ref=mine, dst_ref=gath.at[2, here], send_sem=s5.at[k], recv_sem=r5.at[k], device_id=peer, device_id_type=MESH_ID) for k, peer in enumerate(plane)]
        for send in more:
            send.start()
        gath[:2, here, :] = piece[:2]
        gath[2, here, :] = mine[...]
        for send in sends + more:
            send.wait()
        both_ref[...] = gath[...]


def finish_sample(node, d_loc, s_loc, got, fold_ref, gsend_ref, w_e1):
    width = node.shape[-1]
    total = s_loc + dot_nn(fold_ref[...], got.reshape(got.shape[0] * got.shape[1], width))
    pieces = split_three(total)
    w_send = w_e1[width:2 * width, :]
    gsend_ref[...] += sum(dot_tn(node, piece) for piece in pieces)
    return (d_loc + sum(dot_nt(piece, w_send) for piece in pieces)).astype(BF)


def lay_grads(full_ref, grad_ref, gsend_ref):
    shards, rows_all, width = full_ref.shape
    sources = ((grad_ref, 0), (gsend_ref, 0), (grad_ref, 2 * width))
    for shard in range(shards):
        row = SHARD_ROWS[0] * shard
        last = row + SHARD_ROWS[0]
        spot = 0
        while row < last:
            block = row // width
            count = min(last, (block + 1) * width) - row
            ref, base = sources[block]
            base = base + row - block * width
            full_ref[shard, spot:spot + count, :] = ref[base:base + count, :]
            row += count
            spot += count
        first = 3 * width
        for rows, off in zip(SHARD_ROWS[1:], SHARD_OFF[1:]):
            full_ref[shard, off:off + rows, :] = grad_ref[first + shard * rows:first + (shard + 1) * rows, :]
            first += rows * shards
        full_ref[shard, NORM_OFF:NORM_OFF + 8, :] = grad_ref[first:first + 8, :]
        full_ref[shard, NORM_OFF + 8:, :] = jnp.zeros((rows_all - NORM_OFF - 8, width), F32)


def adam_kernel(shards, both_ref, *refs):
    refs, extra = refs[:-1], refs[-1]
    dp = lax.axis_index('dp')
    masters, ones, twos, new_masters, new_ones, new_twos = (refs[i:i + 5] for i in range(0, len(refs), 5))
    layers, gains, lanes = masters[-1].shape
    norm = both_ref[:2, NORM_OFF:NORM_OFF + gains, :lanes]
    for shard in range(1, shards):
        norm = jnp.where(dp == shard, both_ref[:2, NORM_OFF:NORM_OFF + gains, shard * lanes:(shard + 1) * lanes], norm)
    sums = [both_ref[:2, off:off + rows, :] for rows, off in zip(SHARD_ROWS, SHARD_OFF)] + [norm]
    rows, width = SHARD_ROWS[0], extra.shape[1]
    extra[...] = jnp.zeros_like(extra)
    extra[width:2 * width, :] = both_ref[2]
    sums[0] = jnp.stack([sums[0][0] + extra[pl.ds(pl.multiple_of(dp * rows, rows), rows), :], sums[0][1]])
    for slot, grad_sum in enumerate(sums):
        results = adamw_update(masters[slot][...], grad_sum, ones[slot][...], twos[slot][...])
        for ref, value in zip((new_masters[slot], new_ones[slot], new_twos[slot]), results):
            ref[...] = value


def whole(shape):
    zeros = (0,) * len(shape)
    return pl.BlockSpec(shape, lambda s: zeros)


def per_sample(rows, width):
    return pl.BlockSpec((1, rows, width), lambda s: (s, 0, 0))


def slot_spec(tiles, slots, width):
    return pl.BlockSpec((tiles, 1, slots, width), lambda s: (0, s, 0, 0))


PARAMS = dict(vmem_limit_bytes=63 << 20)


def grid_params():
    return pltpu.CompilerParams(dimension_semantics=("arbitrary",), **PARAMS)


def remote_params(number):
    return pltpu.CompilerParams(collective_id=number, has_side_effects=True, **PARAMS)


def slot_sems(samples, tiles):
    return [pltpu.SemaphoreType.DMA((samples, tiles)), pltpu.SemaphoreType.DMA((samples, tiles)), pltpu.SemaphoreType.DMA((samples,))]


def shard_sems(shards):
    return [pltpu.SemaphoreType.DMA((shards,)), pltpu.SemaphoreType.DMA((shards,)), pltpu.SemaphoreType.DMA]


def solution(mesh):
    lat_spec = P('dp', 'sp', None)
    edge_spec = P('sp')
    mat_spec = P(None, 'dp', None)
    norm_spec = P(None, None, 'dp')
    param_specs = (mat_spec, mat_spec, mat_spec, mat_spec, norm_spec)
    tiles = mesh.shape['sp']
    dp_size = mesh.shape['dp']

    def spread(value, axis):
        count = mesh.shape[axis]
        return lax.all_to_all(jnp.broadcast_to(value[None], (count,) + value.shape), axis, 0, 0, tiled=True)

    def join(stacked, dim):
        moved = jnp.moveaxis(stacked, 0, dim)
        return moved.reshape(moved.shape[:dim] + (moved.shape[dim] * moved.shape[dim + 1],) + moved.shape[dim + 2:])

    def scatter_sum(value, axis, dim):
        count = mesh.shape[axis]
        split = value.reshape(value.shape[:dim] + (count, value.shape[dim] // count) + value.shape[dim + 1:])
        return jnp.sum(lax.all_to_all(jnp.moveaxis(split, dim, 0), axis, 0, 0, tiled=True), axis=0)

    def gather_weights(masters, layer_idx):
        mat_list = [join(spread(master[layer_idx].astype(BF), 'dp'), 0) for master in masters[:4]]
        norm_rows = join(spread(masters[4][layer_idx].astype(BF), 'dp'), 1).astype(F32)
        return mat_list[0], mat_list[1], mat_list[2], mat_list[3], norm_rows

    def reduce_grads(grads):
        parts = [scatter_sum(grad_full, 'dp', 0) for grad_full in grads[:4]] + [scatter_sum(grads[4], 'dp', 1)]
        return tuple(jnp.sum(spread(part, 'sp'), axis=0) for part in parts)

    def general_step(node_lat, edge_lat, senders, edge_mask, node_cot, edge_cot, masters):
        batch_size, tile_nodes, lat_width = node_lat.shape
        degree = edge_lat.shape[1] // tile_nodes
        layers = masters[0].shape[0]
        mask_f = edge_mask.astype(F32).reshape(tile_nodes, degree)
        mask_b = mask_f.astype(BF)
        node_x = node_lat
        edge_x = edge_lat.reshape(batch_size, tile_nodes, degree, lat_width)
        records = []
        for layer_idx in range(layers):
            layer_wts = gather_weights(masters, layer_idx)
            node_all = join(spread(node_x, 'sp'), 1)
            node_new, edge_new, saved = layer_forward(node_x, node_all, edge_x, senders, mask_b, layer_wts)
            records.append((node_x, edge_x, saved))
            node_x = node_new
            edge_x = edge_new
        d_node = node_cot
        d_edge = edge_cot.reshape(batch_size, tile_nodes, degree, lat_width)
        grads_rev = []
        for layer_idx in reversed(range(layers)):
            layer_wts = gather_weights(masters, layer_idx)
            node_in, edge_in, saved = records[layer_idx]
            d_local, scattered, d_edge, grads = layer_backward(d_node, d_edge, node_in, edge_in, senders, mask_f, saved, layer_wts, tile_nodes * tiles)
            returned = scatter_sum(scattered, 'sp', 1)
            d_node = (d_local + returned).astype(BF)
            grads_rev.append(reduce_grads(grads))
        layer_grads = grads_rev[::-1]
        sums = tuple(jnp.stack([per_layer[slot] for per_layer in layer_grads], axis=0) for slot in range(5))
        return sums + (d_node, d_edge.reshape(edge_lat.shape))

    def compact_step(node_lat, edge_lat, send_all, edge_mask, node_cot, edge_cot, masters):
        samples, tile_nodes, width = node_lat.shape
        edges = edge_lat.shape[1]
        cfg = (tiles, SLOTS, tile_nodes, edges // tile_nodes)
        cols = tile_nodes + tiles * SLOTS
        layers = masters[0].shape[0]
        sd = jax.ShapeDtypeStruct
        vmem = pl.BlockSpec(memory_space=pltpu.VMEM)
        hbm = pl.BlockSpec(memory_space=pl.ANY)
        last = samples - 1

        def early(rows):
            return pl.BlockSpec((1, rows, width), lambda s: (jnp.minimum(s, last), 0, 0))

        def late(rows):
            return pl.BlockSpec((1, rows, width), lambda s: (jnp.maximum(s - samples, 0), 0, 0))

        node_b = sd((samples, tile_nodes, width), BF)
        node_f = sd((samples, tile_nodes, width), F32)
        edge_b = sd((samples, edges, width), BF)
        grad_f = sd((GRAD_ROWS, width), F32)
        slot_b = sd((tiles, samples, SLOTS, width), BF)
        full_f = sd((dp_size, FULL_ROWS, width), F32)
        grow_b = sd((8, edges), jnp.int32)
        nrow_b = sd((8, tiles * SLOTS), jnp.int32)
        mcol_b = sd((edges, LANES), F32)
        mrow_b = sd((8, edges), F32)
        weights_b = [sd((layers, rows * dp_size, width), BF) for rows in SHARD_ROWS] + [sd((layers, 8, width), F32)]

        def full_specs(shapes):
            return [whole(item.shape) for item in shapes]

        def scratch(shape, kind=BF):
            return pltpu.VMEM(shape, kind)

        slot_v = scratch(slot_b.shape)
        drop_v = scratch((cols, edges))
        dpre_v = scratch((edges, width))
        fold_v = scratch((tile_nodes, tiles * SLOTS))
        gsend_v = scratch((width, width), F32)
        tables_b = [grow_b, nrow_b, mcol_b, mrow_b]
        outs = pl.pallas_call(
            functools.partial(open_kernel, cfg, dp_size), grid=(2 * samples,),
            out_shape=[node_b, edge_b, edge_b, node_b, node_b, node_b, edge_b, node_f, node_f, grad_f] + tables_b + weights_b + [slot_b],
            in_specs=[whole((tiles, edges)), whole((1, edges)), whole(node_b.shape), early(tile_nodes), early(edges), late(tile_nodes), late(edges)] + [whole(master.shape) for master in masters],
            out_specs=[early(tile_nodes), early(edges), early(edges), early(tile_nodes), early(tile_nodes), early(tile_nodes), late(edges), late(tile_nodes), late(tile_nodes)] + full_specs([grad_f] + tables_b + weights_b) + [hbm],
            scratch_shapes=[scratch(mcol_b.shape, jnp.int32), scratch((edges, cols)), drop_v, scratch((tiles * SLOTS, tile_nodes)), scratch((cols, width)), dpre_v, scratch(edge_b.shape), scratch(node_b.shape),
                            slot_v, slot_v, slot_v, slot_v, scratch((layers, PART_ROWS, width)), scratch((layers, dp_size, PART_ROWS, width))]
            + slot_sems(samples, tiles) + slot_sems(samples, tiles) + slot_sems(samples, tiles) + shard_sems(dp_size) + shard_sems(dp_size),
            name='open', compiler_params=remote_params(1))(send_all, edge_mask.reshape(1, edges), node_lat, node_lat, edge_lat, node_cot, edge_cot, *masters)
        v_one, h_e, y_e, sums, h_n, y_n, d_edge, d_loc, s_loc, grad_two, grow, nrow, mcol, mrow = outs[:14]
        weights = outs[14:-1]
        recv_three = outs[-1]

        node_s = per_sample(tile_nodes, width)
        edge_s = per_sample(edges, width)
        rows = FULL_ROWS // tiles
        groups = layers + 1
        both_f = (groups, FULL_ROWS, width)
        few = pltpu.SemaphoreType.DMA((tiles,))
        half_v = scratch((dp_size // 2, FULL_ROWS, width), F32)
        d_edge0, d_node, both = pl.pallas_call(
            functools.partial(close_kernel, cfg, dp_size), grid=(samples,),
            out_shape=(edge_b, node_b, sd(both_f, F32)),
            in_specs=[node_s, edge_s, edge_s, edge_s, node_s, node_s, node_s, edge_s] + full_specs([node_b, grow_b, mrow_b, mcol_b, nrow_b] + weights_b + [node_b, node_f, node_f, slot_b, grad_f]),
            out_specs=[edge_s] + full_specs([node_b, sd(both_f, F32)]),
            scratch_shapes=[scratch(grad_f.shape, F32), scratch(node_f.shape, F32), scratch(node_f.shape, F32), slot_v, scratch(full_f.shape, F32), drop_v, dpre_v, fold_v, gsend_v, scratch(node_b.shape), scratch(full_f.shape, F32), slot_v,
                            half_v, half_v, scratch(both_f, F32), scratch((tiles, groups, rows, width), F32), scratch((groups, rows, width), F32), scratch((dp_size, rows, width), F32), scratch(both_f, F32)]
            + slot_sems(samples, tiles) + shard_sems(dp_size) + [few] * 12 + [pltpu.SemaphoreType.DMA],
            name='close', compiler_params=remote_params(2))(node_lat, edge_lat, h_e, y_e, sums, h_n, y_n, d_edge, node_lat, grow, mrow, mcol, nrow, *weights, v_one, d_loc, s_loc, recv_three, grad_two)
        return both, d_node, d_edge0

    def general_both(*args):
        result = general_step(*args)
        lanes = result[4].shape[-1]
        first = result[0]
        norm = lax.dynamic_update_slice(jnp.zeros((first.shape[0], FULL_ROWS - NORM_OFF, first.shape[-1]), F32), result[4], (0, 0, lax.axis_index('dp') * lanes))
        both = jnp.concatenate(result[:4] + (norm,), axis=1)
        return jnp.concatenate([both, jnp.zeros_like(both[:1])], axis=0), result[5], result[6]

    def train_step(node_lat, edge_lat, senders, edge_mask, node_cot, edge_cot, w_edge1, w_edge2, w_node1, w_node2, norm_par, mom_edge1, mom_edge2, mom_node1, mom_node2, mom_norm, vel_edge1, vel_edge2, vel_node1, vel_node2, vel_norm):
        masters = (w_edge1, w_edge2, w_node1, w_node2, norm_par)
        moments_one = (mom_edge1, mom_edge2, mom_node1, mom_node2, mom_norm)
        moments_two = (vel_edge1, vel_edge2, vel_node1, vel_node2, vel_norm)
        tile_nodes = node_lat.shape[1]
        lines = senders.shape[0] // LANES
        vmem = pl.BlockSpec(memory_space=pltpu.VMEM)
        few = pltpu.SemaphoreType.DMA((tiles,))
        send_all, most = pl.pallas_call(
            functools.partial(ids_kernel, tiles, SLOTS, tile_nodes),
            out_shape=(jax.ShapeDtypeStruct((tiles, lines * LANES), jnp.int32), jax.ShapeDtypeStruct((8, LANES), F32)),
            in_specs=[vmem], out_specs=(vmem, vmem), scratch_shapes=[pltpu.VMEM((tiles, lines, LANES), jnp.int32), few, few],
            name='ids', compiler_params=remote_params(0))(senders.reshape(lines, LANES))
        fits = most[0, 0] <= SLOTS

        def unsettled(state):
            return jnp.logical_not(state[0])

        def settle(state):
            held = tuple(master * jnp.logical_not(state[0]).astype(F32) for master in masters)
            args = (node_lat, edge_lat, senders, edge_mask, node_cot, edge_cot, held)
            return (True,) + jax.tree.map(row_major, general_both(*jax.tree.map(row_major, args)))

        state = (fits,) + compact_step(node_lat, edge_lat, send_all, edge_mask, node_cot, edge_cot, masters)
        both, d_node, d_edge = lax.while_loop(unsettled, settle, state)[1:]
        state = masters + moments_one + moments_two
        new_state = pl.pallas_call(
            functools.partial(adam_kernel, dp_size), out_shape=[jax.ShapeDtypeStruct(item.shape, F32) for item in state],
            in_specs=[vmem] * (len(state) + 1), out_specs=[vmem] * len(state), scratch_shapes=[pltpu.VMEM((w_edge2.shape[-1] * 3, w_edge2.shape[-1]), F32)], name='adam', compiler_params=pltpu.CompilerParams(**PARAMS))(both, *state)
        return tuple(new_state) + (d_node, d_edge)

    return jax.shard_map(train_step, mesh=mesh, in_specs=(lat_spec, lat_spec, edge_spec, edge_spec, lat_spec, lat_spec) + param_specs + param_specs + param_specs, out_specs=param_specs + param_specs + param_specs + (lat_spec, lat_spec), check_vma=False)
```

```python
import functools

import jax
import jax.numpy as jnp
from jax import lax
from jax.experimental import pallas as pl
from jax.experimental.layout import Layout, with_layout_constraint
from jax.experimental.pallas import tpu as pltpu
from jax.sharding import PartitionSpec as P

NORM_EPS = 1e-5
LEARN_RATE = 1e-3
BETA_ONE = 0.9
BETA_TWO = 0.95
ADAM_EPS = 1e-8
DECAY = 0.1
STEP = 10

NODE_DIMS = (0, 1)
EDGE_DIMS = (0, 1, 2)
BF = jnp.bfloat16
F32 = jnp.float32
SLOTS = 80
MESH_ID = pl.DeviceIdType.MESH


def ring_gap(offset, count):
    return min(offset % count, -offset % count)


def far_first(tiles):
    side = int(tiles ** 0.5)
    return sorted(range(1, tiles), key=lambda offset: -ring_gap(offset // side, side) - ring_gap(offset, side))


def line_first(count):
    return sorted(range(1, count), key=lambda offset: -ring_gap(offset, count))

LANES = 128
SHARD_ROWS = (96, 32, 64, 32)
SHARD_OFF = (0, 96, 128, 192)
NORM_OFF = 224
PART_ROWS = 240
FULL_ROWS = 256
GRAD_ROWS = 1800


def contract(left_op, right_op, left_dims, right_dims):
    return lax.dot_general(left_op, right_op, ((left_dims, right_dims), ((), ())), preferred_element_type=jnp.float32)


def norm_forward(out_b, norm_gain, norm_bias):
    values = out_b.astype(jnp.float32)
    centered = values - jnp.mean(values, axis=-1, keepdims=True)
    inv_std = lax.rsqrt(jnp.mean(centered * centered, axis=-1, keepdims=True) + NORM_EPS)
    normed = centered * inv_std
    return normed * norm_gain + norm_bias, normed, inv_std


def mlp_tail(pre_act, w_two, norm_gain, norm_bias):
    pre_b = pre_act.astype(jnp.bfloat16)
    hidden_act = jax.nn.silu(pre_b.astype(jnp.float32)).astype(jnp.bfloat16)
    last_dim = hidden_act.ndim - 1
    out_b = contract(hidden_act, w_two, (last_dim,), (0,)).astype(jnp.bfloat16)
    branch, normed, inv_std = norm_forward(out_b, norm_gain, norm_bias)
    return branch, (pre_b, hidden_act, normed, inv_std)


def mlp_back(d_branch, saved, w_one, w_two, norm_gain):
    pre_b, hidden_act, normed, inv_std = saved
    last_dim = hidden_act.ndim - 1
    lead_dims = tuple(range(last_dim))
    d_gain = jnp.sum(d_branch * normed, axis=lead_dims)
    d_bias = jnp.sum(d_branch, axis=lead_dims)
    d_norm = d_branch * norm_gain
    d_out = (inv_std * (d_norm - jnp.mean(d_norm, axis=-1, keepdims=True) - normed * jnp.mean(d_norm * normed, axis=-1, keepdims=True))).astype(jnp.bfloat16)
    d_two = contract(hidden_act, d_out, lead_dims, lead_dims)
    d_act = contract(d_out, w_two, (last_dim,), (1,)).astype(jnp.bfloat16)
    pre_f = pre_b.astype(jnp.float32)
    gate_sig = jax.nn.sigmoid(pre_f)
    d_pre = (d_act.astype(jnp.float32) * gate_sig * (1.0 + pre_f * (1.0 - gate_sig))).astype(jnp.bfloat16)
    d_in = contract(d_pre, w_one, (last_dim,), (1,))
    return d_pre, d_in, d_two, d_gain, d_bias


def layer_forward(node_x, node_all, edge_x, senders, mask_b, layer_wts):
    w_e1, w_e2, w_n1, w_n2, norm_rows = layer_wts
    lat_width = node_x.shape[-1]
    sender_lat = jnp.take(node_all, senders, axis=1).reshape(edge_x.shape)
    pre_e = (contract(edge_x, w_e1[:lat_width], (3,), (0,))
             + contract(sender_lat, w_e1[lat_width:2 * lat_width], (3,), (0,))
             + contract(node_x, w_e1[2 * lat_width:], (2,), (0,))[:, :, None, :])
    branch_e, saved_e = mlp_tail(pre_e, w_e2, norm_rows[0], norm_rows[1])
    edge_new = (edge_x.astype(jnp.float32) + branch_e).astype(jnp.bfloat16)
    node_sum = jnp.einsum('bngd,ng->bnd', edge_new, mask_b, preferred_element_type=jnp.float32).astype(jnp.bfloat16)
    pre_n = contract(node_x, w_n1[:lat_width], (2,), (0,)) + contract(node_sum, w_n1[lat_width:], (2,), (0,))
    branch_n, saved_n = mlp_tail(pre_n, w_n2, norm_rows[2], norm_rows[3])
    node_new = (node_x.astype(jnp.float32) + branch_n).astype(jnp.bfloat16)
    return node_new, edge_new, (sender_lat, node_sum, saved_e, saved_n)


def layer_backward(d_node_new, d_edge_new, node_x, edge_x, senders, mask_f, saved, layer_wts, total_nodes):
    w_e1, w_e2, w_n1, w_n2, norm_rows = layer_wts
    sender_lat, node_sum, saved_e, saved_n = saved
    batch_size, tile_nodes, degree, lat_width = edge_x.shape
    d_res_n = d_node_new.astype(jnp.float32)
    d_pre_n, d_in_n, d_wn2, d_gain_n, d_bias_n = mlp_back(d_res_n, saved_n, w_n1, w_n2, norm_rows[2])
    d_wn1 = jnp.concatenate([contract(node_x, d_pre_n, NODE_DIMS, NODE_DIMS), contract(node_sum, d_pre_n, NODE_DIMS, NODE_DIMS)], axis=0)
    d_sum = d_in_n[..., lat_width:].astype(jnp.bfloat16)
    d_res_e = (d_edge_new.astype(jnp.float32) + d_sum.astype(jnp.float32)[:, :, None, :] * mask_f[None, :, :, None]).astype(jnp.bfloat16).astype(jnp.float32)
    d_pre_e, d_in_e, d_we2, d_gain_e, d_bias_e = mlp_back(d_res_e, saved_e, w_e1, w_e2, norm_rows[0])
    recv_grad = contract(node_x, d_pre_e.reshape(batch_size, tile_nodes, -1), NODE_DIMS, NODE_DIMS)
    d_we1 = jnp.concatenate([contract(edge_x, d_pre_e, EDGE_DIMS, EDGE_DIMS), contract(sender_lat, d_pre_e, EDGE_DIMS, EDGE_DIMS), recv_grad.reshape(lat_width, degree, -1).sum(axis=1)], axis=0)
    d_edge_x = (d_res_e + d_in_e[..., :lat_width]).astype(jnp.bfloat16)
    d_sender = d_in_e[..., lat_width:2 * lat_width].reshape(batch_size, tile_nodes * degree, lat_width)
    scattered = jnp.zeros((batch_size, total_nodes, lat_width), jnp.float32).at[:, senders].add(d_sender)
    d_local = d_res_n + d_in_n[..., :lat_width] + d_in_e[..., 2 * lat_width:].sum(axis=2)
    grads = (d_we1, d_we2, d_wn1, d_wn2, jnp.stack([d_gain_e, d_bias_e, d_gain_n, d_bias_n]))
    return d_local, scattered, d_edge_x, grads


def row_major(value):
    return with_layout_constraint(value, Layout(tuple(range(value.ndim))))


def adamw_update(master, grad_sum, moment_one, moment_two):
    corr_one = 1.0 - BETA_ONE ** STEP
    corr_two = 1.0 - BETA_TWO ** STEP
    one_new = BETA_ONE * moment_one + (1.0 - BETA_ONE) * grad_sum
    two_new = BETA_TWO * moment_two + (1.0 - BETA_TWO) * grad_sum * grad_sum
    direction = (one_new / corr_one) / (jnp.sqrt(two_new / corr_two) + ADAM_EPS)
    return master - LEARN_RATE * (direction + DECAY * master), one_new, two_new


def dot_nn(left_op, right_op):
    return lax.dot_general(left_op, right_op, (((1,), (0,)), ((), ())), preferred_element_type=F32)


def dot_nt(left_op, right_op):
    return lax.dot_general(left_op, right_op, (((1,), (1,)), ((), ())), preferred_element_type=F32)


def dot_tn(left_op, right_op):
    return lax.dot_general(left_op, right_op, (((0,), (0,)), ((), ())), preferred_element_type=F32)


def split_three(values):
    high = values.astype(BF)
    rest = values - high.astype(F32)
    mid = rest.astype(BF)
    low = (rest - mid.astype(F32)).astype(BF)
    return high, mid, low


def to_f(cond):
    return jnp.where(cond, 1.0, 0.0)


def to_bf(cond):
    return to_f(cond).astype(BF)


def onehot_cols(col_ids, first, width):
    rows = col_ids.shape[0]
    lane = lax.broadcasted_iota(jnp.int32, (rows, LANES), 1)
    parts = [to_bf(col_ids == lane + (first + LANES * i)) for i in range(width // LANES)]
    return jnp.concatenate(parts, axis=1)


def onehot_rows(row_ids, first, height):
    width = row_ids.shape[1]
    sub = lax.broadcasted_iota(jnp.int32, (height, width), 0) + first
    return to_bf(row_ids == sub)


def norm_parts(out_b):
    values = out_b.astype(F32)
    centered = values - jnp.mean(values, axis=-1, keepdims=True)
    inv_std = lax.rsqrt(jnp.mean(centered * centered, axis=-1, keepdims=True) + NORM_EPS)
    return centered * inv_std, inv_std


def branch_forward(pre_act, w_two, gain, bias):
    pre_b = pre_act.astype(BF)
    pre_f = pre_b.astype(F32)
    sig = jax.nn.sigmoid(pre_f)
    act = (pre_f * sig).astype(BF)
    out_b = dot_nn(act, w_two).astype(BF)
    normed, inv_std = norm_parts(out_b)
    return normed * gain + bias, (pre_b, act, sig, normed, inv_std, out_b)


def branch_backward(d_branch, pre_b, act, sig, normed, inv_std, w_two, gain):
    d_norm = d_branch * gain
    mean_one = jnp.mean(d_norm, axis=-1, keepdims=True)
    mean_two = jnp.mean(d_norm * normed, axis=-1, keepdims=True)
    d_out = (inv_std * (d_norm - mean_one - normed * mean_two)).astype(BF)
    d_two = dot_tn(act, d_out)
    d_act = dot_nt(d_out, w_two).astype(BF)
    pre_f = pre_b.astype(F32)
    d_pre = (d_act.astype(F32) * sig * (1.0 + pre_f * (1.0 - sig))).astype(BF)
    d_gain = jnp.sum(d_branch * normed, axis=0, keepdims=True)
    d_bias = jnp.sum(d_branch, axis=0, keepdims=True)
    return d_pre, d_two, d_gain, d_bias


def load_weights(part_ref, layer, all_wts, norm_ref):
    norm = jnp.zeros((PART_ROWS - NORM_OFF, part_ref.shape[-1]), F32)
    for shard in range(part_ref.shape[0]):
        for ref, rows, off in zip(all_wts, SHARD_ROWS, SHARD_OFF):
            ref[layer, shard * rows:(shard + 1) * rows, :] = part_ref[shard, off:off + rows, :]
        norm += part_ref[shard, NORM_OFF:, :].astype(F32)
    norm_ref[layer] = norm[:8]


def cast_parts(master_refs, part_ref):
    dp = lax.axis_index('dp')
    layers, gains, lanes = master_refs[-1].shape
    width = part_ref.shape[-1]
    spot = lax.broadcasted_iota(jnp.int32, (lanes, width), 1) - lanes * dp
    place = to_bf(spot == lax.broadcasted_iota(jnp.int32, (lanes, width), 0))
    for layer in range(layers):
        for ref, rows, off in zip(master_refs, SHARD_ROWS, SHARD_OFF):
            part_ref[layer, off:off + rows, :] = ref[layer].astype(BF)
        norm = jnp.concatenate([master_refs[-1][layer], jnp.zeros((PART_ROWS - NORM_OFF - gains, lanes), F32)], axis=0)
        part_ref[layer, NORM_OFF:, :] = dot_nn(norm.astype(BF), place).astype(BF)


def peer_tile(me, offset, side):
    row = lax.rem(me // side + offset // side, side)
    col = lax.rem(lax.rem(me, side) + offset % side, side)
    return row * side + col


def greet(peers):
    barrier = pltpu.get_barrier_semaphore()
    for peer in peers:
        pl.semaphore_signal(barrier, inc=1, device_id=peer, device_id_type=MESH_ID)


def greeted(count):
    pl.semaphore_wait(pltpu.get_barrier_semaphore(), count)


def tile_peers(tiles):
    me = lax.axis_index('sp')
    dp = lax.axis_index('dp')
    side = int(tiles ** 0.5)
    return [(peer_tile(me, offset, side), dp) for offset in far_first(tiles)]


def slot_copy(src_ref, dst_ref, sample, spot, send_sem, recv_sem, peer, me):
    return pltpu.make_async_remote_copy(src_ref=src_ref.at[peer[0], sample], dst_ref=dst_ref.at[me, sample], send_sem=send_sem.at[sample, spot], recv_sem=recv_sem.at[sample, spot], device_id=peer, device_id_type=MESH_ID)


def slots_start(src_ref, dst_ref, sample, send_sem, recv_sem, self_sem, tiles):
    me = lax.axis_index('sp')
    pltpu.make_async_copy(src_ref.at[me, sample], dst_ref.at[me, sample], self_sem.at[sample]).start()
    for spot, peer in enumerate(tile_peers(tiles)):
        slot_copy(src_ref, dst_ref, sample, spot, send_sem, recv_sem, peer, me).start()


def slots_wait(src_ref, dst_ref, sample, send_sem, recv_sem, self_sem, tiles):
    me = lax.axis_index('sp')
    pltpu.make_async_copy(src_ref.at[me, sample], dst_ref.at[me, sample], self_sem.at[sample]).wait()
    for spot, peer in enumerate(tile_peers(tiles)):
        slot_copy(src_ref, dst_ref, sample, spot, send_sem, recv_sem, peer, me).wait()


def slots_wait_all(src_ref, dst_ref, samples, send_sem, recv_sem, self_sem, tiles):
    def one(sample, carry):
        slots_wait(src_ref, dst_ref, sample, send_sem, recv_sem, self_sem, tiles)
        return carry
    lax.fori_loop(0, samples, one, 0)


def shard_peers(count):
    me = lax.axis_index('sp')
    dp = lax.axis_index('dp')
    return [(me, lax.rem(dp + offset, count)) for offset in line_first(count)]


def shard_copy(src_ref, dst_ref, spot, send_sem, recv_sem, peer, scatter):
    dp = lax.axis_index('dp')
    src = src_ref.at[peer[1]] if scatter else src_ref
    return pltpu.make_async_remote_copy(src_ref=src, dst_ref=dst_ref.at[dp], send_sem=send_sem.at[spot], recv_sem=recv_sem.at[spot], device_id=peer, device_id_type=MESH_ID)


def shards_start(src_ref, dst_ref, send_sem, recv_sem, self_sem, count, scatter):
    dp = lax.axis_index('dp')
    pltpu.make_async_copy(src_ref.at[dp] if scatter else src_ref, dst_ref.at[dp], self_sem).start()
    for spot, peer in enumerate(shard_peers(count)):
        shard_copy(src_ref, dst_ref, spot, send_sem, recv_sem, peer, scatter).start()


def shards_wait(src_ref, dst_ref, send_sem, recv_sem, self_sem, count, scatter):
    dp = lax.axis_index('dp')
    pltpu.make_async_copy(src_ref.at[dp] if scatter else src_ref, dst_ref.at[dp], self_sem).wait()
    for spot, peer in enumerate(shard_peers(count)):
        shard_copy(src_ref, dst_ref, spot, send_sem, recv_sem, peer, scatter).wait()


def chunk_maps(degree, mask_rows, mask_col):
    chunk = mask_rows.shape[1]
    nodes = chunk // degree
    sub_w = lax.broadcasted_iota(jnp.int32, (nodes, chunk), 0) * degree
    lane_w = lax.broadcasted_iota(jnp.int32, (nodes, chunk), 1)
    wide = (lane_w >= sub_w) & (lane_w < sub_w + degree)
    sub_t = lax.broadcasted_iota(jnp.int32, (chunk, nodes), 0)
    lane_t = lax.broadcasted_iota(jnp.int32, (chunk, nodes), 1) * degree
    tall = (sub_t >= lane_t) & (sub_t < lane_t + degree)
    out = dict(tall=to_bf(tall), wide=to_bf(wide), sum=jnp.where(wide, mask_rows[:1], 0.0).astype(BF))
    if mask_col is not None:
        out['spread'] = jnp.where(tall, jnp.concatenate([mask_col] * (nodes // LANES), axis=1), 0.0).astype(BF)
    return out


def make_tables(tiles, slots, tile_nodes, send_ids, mask_ref, node_ref, gcol_ref, grow_ref, nrow_ref, mcol_ref, mrow_ref, pack_ref, out_ref):
    me = lax.axis_index('sp')
    ids = send_ids[...]
    edges = ids.shape[1]
    tile_of = ids // tile_nodes
    local = (ids - tile_of * tile_nodes).astype(F32)
    row = lax.broadcasted_iota(jnp.int32, (tiles, edges), 0)
    is_me = row == me
    own_tile = jnp.sum(jnp.where(is_me, tile_of, 0), axis=0, keepdims=True)
    own_local = jnp.sum(jnp.where(is_me, local, 0.0), axis=0, keepdims=True)
    own = to_f(own_tile == row)
    inc = to_f((tile_of == me) & jnp.logical_not(is_me))
    both = jnp.concatenate([own, inc], axis=0).astype(BF)
    rank = jnp.zeros((2 * tiles, edges), F32)
    step = 256
    for blk in range(edges // step):
        first = lax.broadcasted_iota(jnp.int32, (step, edges), 0) + blk * step
        second = lax.broadcasted_iota(jnp.int32, (step, edges), 1)
        rank += dot_nn(both[:, blk * step:(blk + 1) * step], to_bf(first < second))
    slot_id = jnp.where(is_me, own_local, rank[:tiles] + (row * slots + tile_nodes).astype(F32))
    gidx = jnp.sum(own * slot_id, axis=0, keepdims=True)
    grow_ref[...] = jnp.broadcast_to(gidx, grow_ref.shape).astype(jnp.int32)
    gcol_ref[...] = jnp.transpose(jnp.broadcast_to(gidx, (LANES, edges))).astype(jnp.int32)
    mask = jnp.concatenate([mask_ref[line:line + 1, :] for line in range(mask_ref.shape[0])], axis=1).astype(F32)
    mrow_ref[...] = jnp.broadcast_to(mask, mrow_ref.shape)
    mcol_ref[...] = jnp.transpose(jnp.broadcast_to(mask, (LANES, edges)))
    slot_row = lax.broadcasted_iota(jnp.int32, (slots, edges), 0).astype(F32)
    cols = []
    for peer in range(tiles):
        hit = (slot_row == rank[tiles + peer:tiles + peer + 1]) & (inc[peer:peer + 1] > 0.5)
        found = jnp.sum(jnp.where(hit, local[peer:peer + 1] + 1.0, 0.0), axis=1, keepdims=True) - 1.0
        cols.append(jnp.broadcast_to(found, (slots, LANES)))
    ncol_f = jnp.concatenate(cols, axis=0)
    ncol = ncol_f.astype(jnp.int32)
    nrow_ref[...] = jnp.transpose(ncol_f)[:8].astype(jnp.int32)
    group = 4
    for part in range(tiles // group):
        rows = group * slots
        pick = onehot_cols(ncol[part * rows:(part + 1) * rows], 0, tile_nodes)
        pack_ref[part * rows:(part + 1) * rows, :] = pick
        for sample in range(out_ref.shape[1]):
            got = dot_nn(pick, node_ref[sample]).astype(BF)
            out_ref[part * group:(part + 1) * group, sample] = got.reshape(group, slots, got.shape[1])


def fill_rows(rows_ref, node, got, tile_nodes):
    rows_ref[:tile_nodes, :] = node
    rows_ref[tile_nodes:, :] = got.reshape(got.shape[0] * got.shape[1], got.shape[2])


def build_pick(gcol_ref, pick_ref):
    step = 128 * 3

    def build(i, carry):
        base = pl.multiple_of(i * step, step)
        pick_ref[pl.ds(base, step), :] = onehot_cols(gcol_ref[pl.ds(base, step), :], 0, pick_ref.shape[1])
        return carry
    lax.fori_loop(0, pick_ref.shape[0] // step, build, 0)


def fwd_sample(maps, v_c, e_c, pick_ref, rows_ref, wts, norm_ref):
    w_e1, w_e2, w_n1, w_n2 = wts
    width = e_c.shape[-1]
    w_edge, w_send, w_recv = (w_e1[i * width:(i + 1) * width, :] for i in range(w_e1.shape[0] // width))
    sent = dot_nn(pick_ref[...], rows_ref[...]).astype(BF)
    recv = dot_nn(maps['tall'], v_c).astype(BF)
    pre = dot_nn(e_c, w_edge) + dot_nn(sent, w_send) + dot_nn(recv, w_recv)
    rows = [norm_ref[i:i + 1, :] for i in range(len(SHARD_ROWS))]
    branch, edge_s = branch_forward(pre, w_e2[...], rows[0], rows[1])
    e_new = (e_c.astype(F32) + branch).astype(BF)
    sums = dot_nn(maps['sum'], e_new).astype(BF)
    pre_n = dot_nn(v_c, w_n1[:width, :]) + dot_nn(sums, w_n1[width:, :])
    branch_n, node_s = branch_forward(pre_n, w_n2[...], rows[2], rows[3])
    return e_new, sums, branch_n, edge_s, node_s


def share_ids(peers, mine_ref, wide, ids_ref, most_ref, send_sem, recv_sem, tile_nodes):
    me = lax.axis_index('sp')
    wide[me] = mine_ref[...]
    copies = [pltpu.make_async_remote_copy(src_ref=mine_ref, dst_ref=wide.at[me], send_sem=send_sem.at[spot], recv_sem=recv_sem.at[spot], device_id=peer, device_id_type=MESH_ID) for spot, peer in enumerate(peers)]
    for copy in copies:
        copy.start()
    for copy in copies:
        copy.wait()
    tiles, lines, lanes = wide.shape
    for line in range(lines):
        ids_ref[:, line * lanes:(line + 1) * lanes] = wide[:, line, :]
    tile_of = ids_ref[...] // tile_nodes
    row = lax.broadcasted_iota(jnp.int32, (tiles, lanes), 0)
    most = jnp.zeros((tiles, lanes), F32)
    for peer in range(tiles):
        count = jnp.sum(to_f(tile_of == peer), axis=1, keepdims=True)
        most = jnp.maximum(most, jnp.where(row == peer, 0.0, count))
    most_ref[...] = jnp.broadcast_to(jnp.max(most, axis=0, keepdims=True), most_ref.shape)


def open_kernel(cfg, shards, mine_ref, mask_ref, nodes_ref, node_ref, edge_ref, dnode_ref, dedge_ref, m_e1, m_e2, m_n1, m_n2, m_norm,
                vout_ref, he_ref, ye_ref, sum_ref, hn_ref, yn_ref, de_ref, dloc_ref, sloc_ref, grad_ref, grow_ref, nrow_ref, mcol_ref, mrow_ref, w_e1, w_e2, w_n1, w_n2, norm_ref, most_ref, recv_out,
                wide, ids_ref, gcol_ref, pick_ref, drop_ref, pack_ref, rows_ref, dpre_ref, e_two, v_two, out_buf, in_buf, next_buf, in_two, part_ref, gat_ref,
                send_a, recv_a, self_a, send_b, recv_b, self_b, send_c, recv_c, self_c, send_w, recv_w, self_w, send_x, recv_x, self_x, send_i, recv_i):
    tiles, slots, tile_nodes, degree = cfg
    samples = nodes_ref.shape[0]
    all_wts = (w_e1, w_e2, w_n1, w_n2)
    step = pl.program_id(0)
    weight_sems = ((send_w, recv_w, self_w), (send_x, recv_x, self_x))

    def take_weights(layer):
        shards_wait(part_ref.at[layer], gat_ref.at[layer], *weight_sems[layer], shards, False)
        load_weights(gat_ref.at[layer], layer, all_wts, norm_ref)

    @pl.when(step == 0)
    def _():
        plane = tile_peers(tiles)
        peers = plane + shard_peers(shards)
        greet(peers)
        cast_parts((m_e1, m_e2, m_n1, m_n2, m_norm), part_ref)
        greeted(len(peers))
        share_ids(plane, mine_ref, wide, ids_ref, most_ref, send_i, recv_i, tile_nodes)
        make_tables(tiles, slots, tile_nodes, ids_ref, mask_ref, nodes_ref, gcol_ref, grow_ref, nrow_ref, mcol_ref, mrow_ref, pack_ref, out_buf)
        for sample in range(samples):
            slots_start(out_buf, in_buf, sample, send_a, recv_a, self_a, tiles)
        for layer, sems in enumerate(weight_sems):
            shards_start(part_ref.at[layer], gat_ref.at[layer], *sems, shards, False)
        build_pick(gcol_ref, pick_ref)
        build_drop(grow_ref, drop_ref)
        grad_ref[...] = jnp.zeros_like(grad_ref)
        take_weights(0)

    @pl.when(step == samples - 1)
    def _():
        take_weights(1)

    @pl.when(step < samples)
    def _():
        slots_wait(out_buf, in_buf, step, send_a, recv_a, self_a, tiles)
        fill_rows(rows_ref, node_ref[0], in_buf[:, step], tile_nodes)
        node, edge = node_ref[0], edge_ref[0]
        e_new, sums, branch_n, edge_s, node_s = fwd_sample(chunk_maps(degree, mrow_ref[...], None), node, edge, pick_ref, rows_ref, [ref.at[0] for ref in all_wts], norm_ref.at[0])
        v_new = (node.astype(F32) + branch_n).astype(BF)
        for ref, value in ((he_ref, edge_s[0]), (ye_ref, edge_s[-1]), (sum_ref, sums), (hn_ref, node_s[0]), (yn_ref, node_s[-1]), (vout_ref, v_new)):
            ref[0] = value
        e_two[step] = e_new
        v_two[step] = v_new

        def pack(i, carry):
            rows = 4 * slots
            base = pl.multiple_of(i * rows, rows)
            got = dot_nn(pack_ref[pl.ds(base, rows), :], vout_ref[0]).astype(BF)
            next_buf[pl.ds(i * 4, 4), step] = got.reshape(4, slots, got.shape[1])
            return carry
        lax.fori_loop(0, tiles // 4, pack, 0)
        slots_start(next_buf, in_two, step, send_b, recv_b, self_b, tiles)

    @pl.when(step >= samples)
    def _():
        sample = step - samples
        slots_wait(next_buf, in_two, sample, send_b, recv_b, self_b, tiles)
        node, edge = v_two[sample], e_two[sample]
        fill_rows(rows_ref, node, in_two[:, sample], tile_nodes)
        wts, norm = [ref.at[1] for ref in all_wts], norm_ref.at[1]
        maps = chunk_maps(degree, mrow_ref[...], mcol_ref[...])
        e_new, sums, branch_n, edge_s, node_s = fwd_sample(maps, node, edge, pick_ref, rows_ref, wts, norm)
        back_sample(maps, node, edge, sums, edge_s[:-1], node_s[:-1], dnode_ref[0].astype(F32), dedge_ref, wts, norm, grad_ref, dpre_ref, de_ref, dloc_ref)
        back_pack(dpre_ref, drop_ref, sloc_ref, out_buf, sample, tiles, slots, tile_nodes)
        slots_start(out_buf, recv_out, sample, send_c, recv_c, self_c, tiles)

    @pl.when(step == 2 * samples - 1)
    def _():
        slots_wait_all(out_buf, recv_out, samples, send_c, recv_c, self_c, tiles)


def back_sample(maps, v_c, e_c, sums, edge_s, node_s, d_node, dedge_ref, wts, norm_ref, grad_ref, dpre_ref, de_ref, dloc_ref):
    w_e1, w_e2, w_n1, w_n2 = wts
    width = e_c.shape[-1]
    w_edge, w_send, w_recv = (w_e1[i * width:(i + 1) * width, :] for i in range(w_e1.shape[0] // width))
    d_pre_n, d_wn2, d_gain_n, d_bias_n = branch_backward(d_node, *node_s, w_n2[...], norm_ref[2:3, :])
    d_in_v = dot_nt(d_pre_n, w_n1[:width, :])
    d_sum = dot_nt(d_pre_n, w_n1[width:, :]).astype(BF)
    d_res = (dedge_ref[0].astype(F32) + dot_nn(maps['spread'], d_sum)).astype(BF).astype(F32)
    d_pre, d_we2, d_gain_e, d_bias_e = branch_backward(d_res, *edge_s, w_e2[...], norm_ref[0:1, :])
    dpre_ref[...] = d_pre
    de_ref[0] = (d_res + dot_nt(d_pre, w_edge)).astype(BF)
    recv = split_three(dot_nn(maps['wide'], d_pre))
    dloc_ref[0] = d_node + d_in_v + sum(dot_nt(piece, w_recv) for piece in recv)
    blocks = [dot_tn(e_c, d_pre), None, sum(dot_tn(v_c, piece) for piece in recv), d_we2, dot_tn(v_c, d_pre_n), dot_tn(sums, d_pre_n), d_wn2]
    for i, block in enumerate(blocks):
        if block is not None:
            grad_ref[i * width:(i + 1) * width, :] += block
    rows = [d_gain_e, d_bias_e, d_gain_n, d_bias_n]
    grad_ref[len(blocks) * width:, :] += jnp.concatenate(rows + [jnp.zeros((len(rows), width), F32)], axis=0)


def back_pack(dpre_ref, drop_ref, sloc_ref, send_buf, step, tiles, slots, tile_nodes):
    sloc_ref[0] = dot_nn(drop_ref[:tile_nodes, :], dpre_ref[...])

    def pack(i, carry):
        rows = 4 * slots
        base = pl.multiple_of(tile_nodes + i * rows, 64)
        got = dot_nn(drop_ref[pl.ds(base, rows), :], dpre_ref[...]).astype(BF)
        send_buf[pl.ds(i * 4, 4), step] = got.reshape(4, slots, got.shape[1])
        return carry
    lax.fori_loop(0, tiles // 4, pack, 0)


def build_drop(grow_ref, drop_ref):
    step = 256

    def build(i, carry):
        base = pl.multiple_of(i * step, step)
        drop_ref[pl.ds(base, step), :] = onehot_rows(grow_ref[0:1, :], base, step)
        return carry
    lax.fori_loop(0, drop_ref.shape[0] // step, build, 0)


def again(pre_b, out_b):
    pre_f = pre_b.astype(F32)
    sig = jax.nn.sigmoid(pre_f)
    act = (pre_f * sig).astype(BF)
    normed, inv_std = norm_parts(out_b)
    return pre_b, act, sig, normed, inv_std


def close_kernel(cfg, shards, node_ref, edge_ref, he_ref, ye_ref, sum_ref, hn_ref, yn_ref, dedge_ref, nodes_ref, grow_ref, mrow_ref, mcol_ref, nrow_ref, w_e1, w_e2, w_n1, w_n2, norms_ref, vall_ref, dlall_ref, slall_ref, recv_ref, gtwo_ref,
                 de_ref, dv_out, both_ref,
                 grad_ref, dloc_ref, sloc_ref, in_buf, part_buf, drop_ref, dpre_ref, fold_ref, gsend_ref, dv_ref, full_ref, send_buf, half_buf, x_buf, own, rs_buf, piece, ws_buf, gath,
                 send_b, recv_b, self_b, send_w, recv_w, self_w, s0, r0, s1, r1, s2, r2, s3, r3, s4, r4, s5, r5, self_s):
    tiles, slots, tile_nodes, degree = cfg
    samples = vall_ref.shape[0]
    step = pl.program_id(0)
    me = lax.axis_index('sp')
    dp = lax.axis_index('dp')
    core = lax.rem(dp, 2)
    chip = dp // 2
    chips = shards // 2
    plane = tile_peers(tiles)
    others = shard_peers(shards)

    @pl.when(step == 0)
    def _():
        greet(plane + others)
        fold_ref[...] = onehot_rows(nrow_ref[:1], 0, tile_nodes)
        gsend_ref[...] = jnp.zeros_like(gsend_ref)

        def finish(sample, carry):
            dv_ref[sample] = finish_sample(vall_ref[sample], dlall_ref[sample], slall_ref[sample], recv_ref[:, sample], fold_ref, gsend_ref, w_e1.at[1])
            return carry
        lax.fori_loop(0, samples, finish, 0)
        lay_grads(full_ref, gtwo_ref, gsend_ref)
        greeted(len(plane + others))
        shards_start(full_ref, part_buf, send_w, recv_w, self_w, shards, True)
        build_drop(grow_ref, drop_ref)
        grad_ref[...] = jnp.zeros_like(grad_ref)

    maps = chunk_maps(degree, mrow_ref[...], mcol_ref[...])
    edge_s = again(he_ref[0], ye_ref[0])
    node_s = again(hn_ref[0], yn_ref[0])
    back_sample(maps, node_ref[0], edge_ref[0], sum_ref[0], edge_s, node_s, dv_ref[step].astype(F32), dedge_ref, [ref.at[0] for ref in (w_e1, w_e2, w_n1, w_n2)], norms_ref.at[0], grad_ref, dpre_ref, de_ref, dloc_ref.at[pl.ds(step, 1)])
    back_pack(dpre_ref, drop_ref, sloc_ref.at[pl.ds(step, 1)], send_buf, step, tiles, slots, tile_nodes)
    slots_start(send_buf, in_buf, step, send_b, recv_b, self_b, tiles)

    @pl.when(step == samples - 1)
    def _():
        away = line_first(chips)
        spots = [lax.rem(chip + offset, chips) for offset in away]
        line = [(me, spot * 2 + core) for spot in spots]
        shards_wait(full_ref, part_buf, send_w, recv_w, self_w, shards, True)
        gsend_ref[...] = jnp.zeros_like(gsend_ref)
        lay_grads(full_ref, grad_ref, gsend_ref)
        pair = [pltpu.make_async_remote_copy(src_ref=full_ref.at[spot * 2 + 1 - core], dst_ref=half_buf.at[spot], send_sem=s0.at[k], recv_sem=r0.at[k], device_id=(me, dp + 1 - 2 * core), device_id_type=MESH_ID) for k, spot in enumerate(spots + [chip])]
        for copy in pair:
            copy.start()
        own[1] = sum(part_buf[shard] for shard in range(shards))
        hops = []
        for k, spot in enumerate(spots):
            pair[k].wait()
            half_buf[spot] += full_ref[spot * 2 + core]
            hop = pltpu.make_async_remote_copy(src_ref=half_buf.at[spot], dst_ref=x_buf.at[chip], send_sem=s1.at[k], recv_sem=r1.at[k], device_id=line[k], device_id_type=MESH_ID)
            hop.start()
            hops.append(hop)
        pair[-1].wait()

        def finish(sample, carry):
            slots_wait(send_buf, in_buf, sample, send_b, recv_b, self_b, tiles)
            dv_out[sample] = finish_sample(nodes_ref[sample], dloc_ref[sample], sloc_ref[sample], in_buf[:, sample], fold_ref, gsend_ref, w_e1.at[0])
            return carry
        lax.fori_loop(0, samples, finish, 0)
        own[2] = gsend_ref[...]
        total = half_buf[chip] + full_ref[dp]
        for hop, offset in zip(hops, away):
            hop.wait()
            total += x_buf[lax.rem(chip + chips - offset, chips)]
        own[0] = total

        rows = FULL_ROWS // tiles
        here = pl.ds(pl.multiple_of(me * rows, rows), rows)
        cuts = [pltpu.make_async_remote_copy(src_ref=own.at[:, pl.ds(pl.multiple_of(peer[0] * rows, rows), rows)], dst_ref=rs_buf.at[me], send_sem=s2.at[k], recv_sem=r2.at[k], device_id=peer, device_id_type=MESH_ID) for k, peer in enumerate(plane)]
        for cut in cuts:
            cut.start()
        for cut in cuts:
            cut.wait()
        piece[...] = own[:, here, :] + sum(rs_buf[lax.rem(me + offset, tiles)] for offset in range(1, tiles))
        shards_start(piece.at[2], ws_buf, s4, r4, self_s, shards, False)
        sends = [pltpu.make_async_remote_copy(src_ref=piece.at[:2], dst_ref=gath.at[:2, here], send_sem=s3.at[k], recv_sem=r3.at[k], device_id=peer, device_id_type=MESH_ID) for k, peer in enumerate(plane)]
        for send in sends:
            send.start()
        shards_wait(piece.at[2], ws_buf, s4, r4, self_s, shards, False)
        mine = rs_buf.at[me, 2]
        mine[...] = sum(ws_buf[shard] for shard in range(shards))
        more = [pltpu.make_async_remote_copy(src_ref=mine, dst_ref=gath.at[2, here], send_sem=s5.at[k], recv_sem=r5.at[k], device_id=peer, device_id_type=MESH_ID) for k, peer in enumerate(plane)]
        for send in more:
            send.start()
        gath[:2, here, :] = piece[:2]
        gath[2, here, :] = mine[...]
        for send in sends + more:
            send.wait()
        both_ref[...] = gath[...]


def finish_sample(node, d_loc, s_loc, got, fold_ref, gsend_ref, w_e1):
    width = node.shape[-1]
    total = s_loc + dot_nn(fold_ref[...], got.reshape(got.shape[0] * got.shape[1], width))
    pieces = split_three(total)
    w_send = w_e1[width:2 * width, :]
    gsend_ref[...] += sum(dot_tn(node, piece) for piece in pieces)
    return (d_loc + sum(dot_nt(piece, w_send) for piece in pieces)).astype(BF)


def lay_grads(full_ref, grad_ref, gsend_ref):
    shards, rows_all, width = full_ref.shape
    sources = ((grad_ref, 0), (gsend_ref, 0), (grad_ref, 2 * width))
    for shard in range(shards):
        row = SHARD_ROWS[0] * shard
        last = row + SHARD_ROWS[0]
        spot = 0
        while row < last:
            block = row // width
            count = min(last, (block + 1) * width) - row
            ref, base = sources[block]
            base = base + row - block * width
            full_ref[shard, spot:spot + count, :] = ref[base:base + count, :]
            row += count
            spot += count
        first = 3 * width
        for rows, off in zip(SHARD_ROWS[1:], SHARD_OFF[1:]):
            full_ref[shard, off:off + rows, :] = grad_ref[first + shard * rows:first + (shard + 1) * rows, :]
            first += rows * shards
        full_ref[shard, NORM_OFF:NORM_OFF + 8, :] = grad_ref[first:first + 8, :]
        full_ref[shard, NORM_OFF + 8:, :] = jnp.zeros((rows_all - NORM_OFF - 8, width), F32)


def adam_kernel(shards, both_ref, dnode_ref, dedge_ref, *refs):
    count = (len(refs) - 7) // 2
    node_out, edge_out = refs[count:count + 2]
    refs = refs[:count] + refs[count + 2:]
    extra, node_buf, edge_buf, sems_in, sems_out = refs[-5:]
    moves = []
    for k, (src, buf, dst) in enumerate(((dedge_ref, edge_buf, edge_out), (dnode_ref, node_buf, node_out))):
        for sample in range(src.shape[0]):
            moves.append((pltpu.make_async_copy(src.at[sample], buf.at[sample], sems_in.at[k, sample]), pltpu.make_async_copy(buf.at[sample], dst.at[sample], sems_out.at[k, sample])))
    for load, store in moves:
        load.start()
    for load, store in moves:
        load.wait()
        store.start()
    dp = lax.axis_index('dp')
    masters, ones, twos, new_masters, new_ones, new_twos = (refs[i:i + 5] for i in range(0, len(refs) - 5, 5))
    layers, gains, lanes = masters[-1].shape
    norm = both_ref[:2, NORM_OFF:NORM_OFF + gains, :lanes]
    for shard in range(1, shards):
        norm = jnp.where(dp == shard, both_ref[:2, NORM_OFF:NORM_OFF + gains, shard * lanes:(shard + 1) * lanes], norm)
    sums = [both_ref[:2, off:off + rows, :] for rows, off in zip(SHARD_ROWS, SHARD_OFF)] + [norm]
    rows, width = SHARD_ROWS[0], extra.shape[1]
    extra[...] = jnp.zeros_like(extra)
    extra[width:2 * width, :] = both_ref[2]
    sums[0] = jnp.stack([sums[0][0] + extra[pl.ds(pl.multiple_of(dp * rows, rows), rows), :], sums[0][1]])
    for slot, grad_sum in enumerate(sums):
        results = adamw_update(masters[slot][...], grad_sum, ones[slot][...], twos[slot][...])
        for ref, value in zip((new_masters[slot], new_ones[slot], new_twos[slot]), results):
            ref[...] = value
    for load, store in moves:
        store.wait()


def whole(shape):
    zeros = (0,) * len(shape)
    return pl.BlockSpec(shape, lambda s: zeros)


def per_sample(rows, width):
    return pl.BlockSpec((1, rows, width), lambda s: (s, 0, 0))


def slot_spec(tiles, slots, width):
    return pl.BlockSpec((tiles, 1, slots, width), lambda s: (0, s, 0, 0))


PARAMS = dict(vmem_limit_bytes=63 << 20)


def grid_params():
    return pltpu.CompilerParams(dimension_semantics=("arbitrary",), **PARAMS)


def remote_params(number):
    return pltpu.CompilerParams(collective_id=number, has_side_effects=True, **PARAMS)


def slot_sems(samples, tiles):
    return [pltpu.SemaphoreType.DMA((samples, tiles)), pltpu.SemaphoreType.DMA((samples, tiles)), pltpu.SemaphoreType.DMA((samples,))]


def shard_sems(shards):
    return [pltpu.SemaphoreType.DMA((shards,)), pltpu.SemaphoreType.DMA((shards,)), pltpu.SemaphoreType.DMA]


def solution(mesh):
    lat_spec = P('dp', 'sp', None)
    edge_spec = P('sp')
    mat_spec = P(None, 'dp', None)
    norm_spec = P(None, None, 'dp')
    param_specs = (mat_spec, mat_spec, mat_spec, mat_spec, norm_spec)
    tiles = mesh.shape['sp']
    dp_size = mesh.shape['dp']

    def spread(value, axis):
        count = mesh.shape[axis]
        return lax.all_to_all(jnp.broadcast_to(value[None], (count,) + value.shape), axis, 0, 0, tiled=True)

    def join(stacked, dim):
        moved = jnp.moveaxis(stacked, 0, dim)
        return moved.reshape(moved.shape[:dim] + (moved.shape[dim] * moved.shape[dim + 1],) + moved.shape[dim + 2:])

    def scatter_sum(value, axis, dim):
        count = mesh.shape[axis]
        split = value.reshape(value.shape[:dim] + (count, value.shape[dim] // count) + value.shape[dim + 1:])
        return jnp.sum(lax.all_to_all(jnp.moveaxis(split, dim, 0), axis, 0, 0, tiled=True), axis=0)

    def gather_weights(masters, layer_idx):
        mat_list = [join(spread(master[layer_idx].astype(BF), 'dp'), 0) for master in masters[:4]]
        norm_rows = join(spread(masters[4][layer_idx].astype(BF), 'dp'), 1).astype(F32)
        return mat_list[0], mat_list[1], mat_list[2], mat_list[3], norm_rows

    def reduce_grads(grads):
        parts = [scatter_sum(grad_full, 'dp', 0) for grad_full in grads[:4]] + [scatter_sum(grads[4], 'dp', 1)]
        return tuple(jnp.sum(spread(part, 'sp'), axis=0) for part in parts)

    def general_step(node_lat, edge_lat, senders, edge_mask, node_cot, edge_cot, masters):
        batch_size, tile_nodes, lat_width = node_lat.shape
        degree = edge_lat.shape[1] // tile_nodes
        layers = masters[0].shape[0]
        mask_f = edge_mask.astype(F32).reshape(tile_nodes, degree)
        mask_b = mask_f.astype(BF)
        node_x = node_lat
        edge_x = edge_lat.reshape(batch_size, tile_nodes, degree, lat_width)
        records = []
        for layer_idx in range(layers):
            layer_wts = gather_weights(masters, layer_idx)
            node_all = join(spread(node_x, 'sp'), 1)
            node_new, edge_new, saved = layer_forward(node_x, node_all, edge_x, senders, mask_b, layer_wts)
            records.append((node_x, edge_x, saved))
            node_x = node_new
            edge_x = edge_new
        d_node = node_cot
        d_edge = edge_cot.reshape(batch_size, tile_nodes, degree, lat_width)
        grads_rev = []
        for layer_idx in reversed(range(layers)):
            layer_wts = gather_weights(masters, layer_idx)
            node_in, edge_in, saved = records[layer_idx]
            d_local, scattered, d_edge, grads = layer_backward(d_node, d_edge, node_in, edge_in, senders, mask_f, saved, layer_wts, tile_nodes * tiles)
            returned = scatter_sum(scattered, 'sp', 1)
            d_node = (d_local + returned).astype(BF)
            grads_rev.append(reduce_grads(grads))
        layer_grads = grads_rev[::-1]
        sums = tuple(jnp.stack([per_layer[slot] for per_layer in layer_grads], axis=0) for slot in range(5))
        return sums + (d_node, d_edge.reshape(edge_lat.shape))

    def compact_step(node_lat, edge_lat, senders, edge_mask, node_cot, edge_cot, masters):
        samples, tile_nodes, width = node_lat.shape
        edges = edge_lat.shape[1]
        cfg = (tiles, SLOTS, tile_nodes, edges // tile_nodes)
        cols = tile_nodes + tiles * SLOTS
        layers = masters[0].shape[0]
        sd = jax.ShapeDtypeStruct
        vmem = pl.BlockSpec(memory_space=pltpu.VMEM)
        hbm = pl.BlockSpec(memory_space=pl.ANY)
        last = samples - 1

        def early(rows):
            return pl.BlockSpec((1, rows, width), lambda s: (jnp.minimum(s, last), 0, 0))

        def late(rows):
            return pl.BlockSpec((1, rows, width), lambda s: (jnp.maximum(s - samples, 0), 0, 0))

        node_b = sd((samples, tile_nodes, width), BF)
        node_f = sd((samples, tile_nodes, width), F32)
        edge_b = sd((samples, edges, width), BF)
        grad_f = sd((GRAD_ROWS, width), F32)
        slot_b = sd((tiles, samples, SLOTS, width), BF)
        full_f = sd((dp_size, FULL_ROWS, width), F32)
        grow_b = sd((8, edges), jnp.int32)
        nrow_b = sd((8, tiles * SLOTS), jnp.int32)
        mcol_b = sd((edges, LANES), F32)
        mrow_b = sd((8, edges), F32)
        lines = edges // LANES
        most_b = sd((8, LANES), F32)
        few = pltpu.SemaphoreType.DMA((tiles,))
        weights_b = [sd((layers, rows * dp_size, width), BF) for rows in SHARD_ROWS] + [sd((layers, 8, width), F32)]

        def full_specs(shapes):
            return [whole(item.shape) for item in shapes]

        def scratch(shape, kind=BF):
            return pltpu.VMEM(shape, kind)

        slot_v = scratch(slot_b.shape)
        drop_v = scratch((cols, edges))
        dpre_v = scratch((edges, width))
        fold_v = scratch((tile_nodes, tiles * SLOTS))
        gsend_v = scratch((width, width), F32)
        tables_b = [grow_b, nrow_b, mcol_b, mrow_b]
        outs = pl.pallas_call(
            functools.partial(open_kernel, cfg, dp_size), grid=(2 * samples,),
            out_shape=[node_b, edge_b, edge_b, node_b, node_b, node_b, edge_b, node_f, node_f, grad_f] + tables_b + weights_b + [most_b, slot_b],
            in_specs=[whole((lines, LANES)), whole((lines, LANES)), whole(node_b.shape), early(tile_nodes), early(edges), late(tile_nodes), late(edges)] + [whole(master.shape) for master in masters],
            out_specs=[early(tile_nodes), early(edges), early(edges), early(tile_nodes), early(tile_nodes), early(tile_nodes), late(edges), late(tile_nodes), late(tile_nodes)] + full_specs([grad_f] + tables_b + weights_b + [most_b]) + [hbm],
            scratch_shapes=[scratch((tiles, lines, LANES), jnp.int32), scratch((tiles, edges), jnp.int32), scratch(mcol_b.shape, jnp.int32), scratch((edges, cols)), drop_v, scratch((tiles * SLOTS, tile_nodes)), scratch((cols, width)), dpre_v, scratch(edge_b.shape), scratch(node_b.shape),
                            slot_v, slot_v, slot_v, slot_v, scratch((layers, PART_ROWS, width)), scratch((layers, dp_size, PART_ROWS, width))]
            + slot_sems(samples, tiles) + slot_sems(samples, tiles) + slot_sems(samples, tiles) + shard_sems(dp_size) + shard_sems(dp_size) + [few, few],
            name='open', compiler_params=remote_params(1))(senders.reshape(lines, LANES), edge_mask.reshape(lines, LANES), node_lat, node_lat, edge_lat, node_cot, edge_cot, *masters)
        v_one, h_e, y_e, sums, h_n, y_n, d_edge, d_loc, s_loc, grad_two, grow, nrow, mcol, mrow = outs[:14]
        weights = outs[14:-2]
        most, recv_three = outs[-2:]

        node_s = per_sample(tile_nodes, width)
        edge_s = per_sample(edges, width)
        rows = FULL_ROWS // tiles
        groups = layers + 1
        both_f = (groups, FULL_ROWS, width)
        half_v = scratch((dp_size // 2, FULL_ROWS, width), F32)
        d_edge0, d_node, both = pl.pallas_call(
            functools.partial(close_kernel, cfg, dp_size), grid=(samples,),
            out_shape=(edge_b, node_b, sd(both_f, F32)),
            in_specs=[node_s, edge_s, edge_s, edge_s, node_s, node_s, node_s, edge_s] + full_specs([node_b, grow_b, mrow_b, mcol_b, nrow_b] + weights_b + [node_b, node_f, node_f, slot_b, grad_f]),
            out_specs=[edge_s] + full_specs([node_b, sd(both_f, F32)]),
            scratch_shapes=[scratch(grad_f.shape, F32), scratch(node_f.shape, F32), scratch(node_f.shape, F32), slot_v, scratch(full_f.shape, F32), drop_v, dpre_v, fold_v, gsend_v, scratch(node_b.shape), scratch(full_f.shape, F32), slot_v,
                            half_v, half_v, scratch(both_f, F32), scratch((tiles, groups, rows, width), F32), scratch((groups, rows, width), F32), scratch((dp_size, rows, width), F32), scratch(both_f, F32)]
            + slot_sems(samples, tiles) + shard_sems(dp_size) + [few] * 12 + [pltpu.SemaphoreType.DMA],
            name='close', compiler_params=remote_params(2))(node_lat, edge_lat, h_e, y_e, sums, h_n, y_n, d_edge, node_lat, grow, mrow, mcol, nrow, *weights, v_one, d_loc, s_loc, recv_three, grad_two)
        return most[0, 0] <= SLOTS, both, d_node, d_edge0

    def general_both(*args):
        result = general_step(*args)
        lanes = result[4].shape[-1]
        first = result[0]
        norm = lax.dynamic_update_slice(jnp.zeros((first.shape[0], FULL_ROWS - NORM_OFF, first.shape[-1]), F32), result[4], (0, 0, lax.axis_index('dp') * lanes))
        both = jnp.concatenate(result[:4] + (norm,), axis=1)
        return jnp.concatenate([both, jnp.zeros_like(both[:1])], axis=0), result[5], result[6]

    def train_step(node_lat, edge_lat, senders, edge_mask, node_cot, edge_cot, w_edge1, w_edge2, w_node1, w_node2, norm_par, mom_edge1, mom_edge2, mom_node1, mom_node2, mom_norm, vel_edge1, vel_edge2, vel_node1, vel_node2, vel_norm):
        masters = (w_edge1, w_edge2, w_node1, w_node2, norm_par)
        moments_one = (mom_edge1, mom_edge2, mom_node1, mom_node2, mom_norm)
        moments_two = (vel_edge1, vel_edge2, vel_node1, vel_node2, vel_norm)
        tile_nodes = node_lat.shape[1]
        vmem = pl.BlockSpec(memory_space=pltpu.VMEM)
        hbm = pl.BlockSpec(memory_space=pl.ANY)

        def unsettled(state):
            return jnp.logical_not(state[0])

        def settle(state):
            held = tuple(master * jnp.logical_not(state[0]).astype(F32) for master in masters)
            args = (node_lat, edge_lat, senders, edge_mask, node_cot, edge_cot, held)
            return (True,) + jax.tree.map(row_major, general_both(*jax.tree.map(row_major, args)))

        state = compact_step(node_lat, edge_lat, senders, edge_mask, node_cot, edge_cot, masters)
        both, d_node, d_edge = lax.while_loop(unsettled, settle, state)[1:]
        state = masters + moments_one + moments_two
        passed = [jax.ShapeDtypeStruct(item.shape, item.dtype) for item in (d_node, d_edge)]
        width = w_edge2.shape[-1]
        sems = pltpu.SemaphoreType.DMA((2, d_node.shape[0]))
        new_state = pl.pallas_call(
            functools.partial(adam_kernel, dp_size), out_shape=passed + [jax.ShapeDtypeStruct(item.shape, F32) for item in state],
            in_specs=[vmem, hbm, hbm] + [vmem] * len(state), out_specs=[hbm, hbm] + [vmem] * len(state),
            scratch_shapes=[pltpu.VMEM((w_edge1.shape[1] * dp_size, width), F32), pltpu.VMEM(d_node.shape, BF), pltpu.VMEM(d_edge.shape, BF), sems, sems],
            name='adam', compiler_params=pltpu.CompilerParams(**PARAMS))(both, d_node, d_edge, *state)
        return tuple(new_state[2:]) + tuple(new_state[:2])

    return jax.shard_map(train_step, mesh=mesh, in_specs=(lat_spec, lat_spec, edge_spec, edge_spec, lat_spec, lat_spec) + param_specs + param_specs + param_specs, out_specs=param_specs + param_specs + param_specs + (lat_spec, lat_spec), check_vma=False)
```

```python
import functools

import jax
import jax.numpy as jnp
from jax import lax
from jax.experimental import pallas as pl
from jax.experimental.layout import Layout, with_layout_constraint
from jax.experimental.pallas import tpu as pltpu
from jax.sharding import PartitionSpec as P

NORM_EPS = 1e-5
LEARN_RATE = 1e-3
BETA_ONE = 0.9
BETA_TWO = 0.95
ADAM_EPS = 1e-8
DECAY = 0.1
STEP = 10

NODE_DIMS = (0, 1)
EDGE_DIMS = (0, 1, 2)
BF = jnp.bfloat16
F32 = jnp.float32
SLOTS = 80
LIVE = 72
MESH_ID = pl.DeviceIdType.MESH


def ring_gap(offset, count):
    return min(offset % count, -offset % count)


def far_first(tiles):
    side = int(tiles ** 0.5)
    return sorted(range(1, tiles), key=lambda offset: -ring_gap(offset // side, side) - ring_gap(offset, side))


def line_first(count):
    return sorted(range(1, count), key=lambda offset: -ring_gap(offset, count))

LANES = 128
SHARD_ROWS = (96, 32, 64, 32)
SHARD_OFF = (0, 96, 128, 192)
NORM_OFF = 224
PART_ROWS = 240
FULL_ROWS = 256
GRAD_ROWS = 1800


def contract(left_op, right_op, left_dims, right_dims):
    return lax.dot_general(left_op, right_op, ((left_dims, right_dims), ((), ())), preferred_element_type=jnp.float32)


def norm_forward(out_b, norm_gain, norm_bias):
    values = out_b.astype(jnp.float32)
    centered = values - jnp.mean(values, axis=-1, keepdims=True)
    inv_std = lax.rsqrt(jnp.mean(centered * centered, axis=-1, keepdims=True) + NORM_EPS)
    normed = centered * inv_std
    return normed * norm_gain + norm_bias, normed, inv_std


def mlp_tail(pre_act, w_two, norm_gain, norm_bias):
    pre_b = pre_act.astype(jnp.bfloat16)
    hidden_act = jax.nn.silu(pre_b.astype(jnp.float32)).astype(jnp.bfloat16)
    last_dim = hidden_act.ndim - 1
    out_b = contract(hidden_act, w_two, (last_dim,), (0,)).astype(jnp.bfloat16)
    branch, normed, inv_std = norm_forward(out_b, norm_gain, norm_bias)
    return branch, (pre_b, hidden_act, normed, inv_std)


def mlp_back(d_branch, saved, w_one, w_two, norm_gain):
    pre_b, hidden_act, normed, inv_std = saved
    last_dim = hidden_act.ndim - 1
    lead_dims = tuple(range(last_dim))
    d_gain = jnp.sum(d_branch * normed, axis=lead_dims)
    d_bias = jnp.sum(d_branch, axis=lead_dims)
    d_norm = d_branch * norm_gain
    d_out = (inv_std * (d_norm - jnp.mean(d_norm, axis=-1, keepdims=True) - normed * jnp.mean(d_norm * normed, axis=-1, keepdims=True))).astype(jnp.bfloat16)
    d_two = contract(hidden_act, d_out, lead_dims, lead_dims)
    d_act = contract(d_out, w_two, (last_dim,), (1,)).astype(jnp.bfloat16)
    pre_f = pre_b.astype(jnp.float32)
    gate_sig = jax.nn.sigmoid(pre_f)
    d_pre = (d_act.astype(jnp.float32) * gate_sig * (1.0 + pre_f * (1.0 - gate_sig))).astype(jnp.bfloat16)
    d_in = contract(d_pre, w_one, (last_dim,), (1,))
    return d_pre, d_in, d_two, d_gain, d_bias


def layer_forward(node_x, node_all, edge_x, senders, mask_b, layer_wts):
    w_e1, w_e2, w_n1, w_n2, norm_rows = layer_wts
    lat_width = node_x.shape[-1]
    sender_lat = jnp.take(node_all, senders, axis=1).reshape(edge_x.shape)
    pre_e = (contract(edge_x, w_e1[:lat_width], (3,), (0,))
             + contract(sender_lat, w_e1[lat_width:2 * lat_width], (3,), (0,))
             + contract(node_x, w_e1[2 * lat_width:], (2,), (0,))[:, :, None, :])
    branch_e, saved_e = mlp_tail(pre_e, w_e2, norm_rows[0], norm_rows[1])
    edge_new = (edge_x.astype(jnp.float32) + branch_e).astype(jnp.bfloat16)
    node_sum = jnp.einsum('bngd,ng->bnd', edge_new, mask_b, preferred_element_type=jnp.float32).astype(jnp.bfloat16)
    pre_n = contract(node_x, w_n1[:lat_width], (2,), (0,)) + contract(node_sum, w_n1[lat_width:], (2,), (0,))
    branch_n, saved_n = mlp_tail(pre_n, w_n2, norm_rows[2], norm_rows[3])
    node_new = (node_x.astype(jnp.float32) + branch_n).astype(jnp.bfloat16)
    return node_new, edge_new, (sender_lat, node_sum, saved_e, saved_n)


def layer_backward(d_node_new, d_edge_new, node_x, edge_x, senders, mask_f, saved, layer_wts, total_nodes):
    w_e1, w_e2, w_n1, w_n2, norm_rows = layer_wts
    sender_lat, node_sum, saved_e, saved_n = saved
    batch_size, tile_nodes, degree, lat_width = edge_x.shape
    d_res_n = d_node_new.astype(jnp.float32)
    d_pre_n, d_in_n, d_wn2, d_gain_n, d_bias_n = mlp_back(d_res_n, saved_n, w_n1, w_n2, norm_rows[2])
    d_wn1 = jnp.concatenate([contract(node_x, d_pre_n, NODE_DIMS, NODE_DIMS), contract(node_sum, d_pre_n, NODE_DIMS, NODE_DIMS)], axis=0)
    d_sum = d_in_n[..., lat_width:].astype(jnp.bfloat16)
    d_res_e = (d_edge_new.astype(jnp.float32) + d_sum.astype(jnp.float32)[:, :, None, :] * mask_f[None, :, :, None]).astype(jnp.bfloat16).astype(jnp.float32)
    d_pre_e, d_in_e, d_we2, d_gain_e, d_bias_e = mlp_back(d_res_e, saved_e, w_e1, w_e2, norm_rows[0])
    recv_grad = contract(node_x, d_pre_e.reshape(batch_size, tile_nodes, -1), NODE_DIMS, NODE_DIMS)
    d_we1 = jnp.concatenate([contract(edge_x, d_pre_e, EDGE_DIMS, EDGE_DIMS), contract(sender_lat, d_pre_e, EDGE_DIMS, EDGE_DIMS), recv_grad.reshape(lat_width, degree, -1).sum(axis=1)], axis=0)
    d_edge_x = (d_res_e + d_in_e[..., :lat_width]).astype(jnp.bfloat16)
    d_sender = d_in_e[..., lat_width:2 * lat_width].reshape(batch_size, tile_nodes * degree, lat_width)
    scattered = jnp.zeros((batch_size, total_nodes, lat_width), jnp.float32).at[:, senders].add(d_sender)
    d_local = d_res_n + d_in_n[..., :lat_width] + d_in_e[..., 2 * lat_width:].sum(axis=2)
    grads = (d_we1, d_we2, d_wn1, d_wn2, jnp.stack([d_gain_e, d_bias_e, d_gain_n, d_bias_n]))
    return d_local, scattered, d_edge_x, grads


def row_major(value):
    return with_layout_constraint(value, Layout(tuple(range(value.ndim))))


def adamw_update(master, grad_sum, moment_one, moment_two):
    corr_one = 1.0 - BETA_ONE ** STEP
    corr_two = 1.0 - BETA_TWO ** STEP
    one_new = BETA_ONE * moment_one + (1.0 - BETA_ONE) * grad_sum
    two_new = BETA_TWO * moment_two + (1.0 - BETA_TWO) * grad_sum * grad_sum
    direction = (one_new / corr_one) / (jnp.sqrt(two_new / corr_two) + ADAM_EPS)
    return master - LEARN_RATE * (direction + DECAY * master), one_new, two_new


def dot_nn(left_op, right_op):
    return lax.dot_general(left_op, right_op, (((1,), (0,)), ((), ())), preferred_element_type=F32)


def dot_nt(left_op, right_op):
    return lax.dot_general(left_op, right_op, (((1,), (1,)), ((), ())), preferred_element_type=F32)


def dot_tn(left_op, right_op):
    return lax.dot_general(left_op, right_op, (((0,), (0,)), ((), ())), preferred_element_type=F32)


def split_three(values):
    high = values.astype(BF)
    rest = values - high.astype(F32)
    mid = rest.astype(BF)
    low = (rest - mid.astype(F32)).astype(BF)
    return high, mid, low


def to_f(cond):
    return jnp.where(cond, 1.0, 0.0)


def to_bf(cond):
    return to_f(cond).astype(BF)


def onehot_cols(col_ids, first, width):
    rows = col_ids.shape[0]
    lane = lax.broadcasted_iota(jnp.int32, (rows, LANES), 1)
    parts = [to_bf(col_ids == lane + (first + LANES * i)) for i in range(width // LANES)]
    return jnp.concatenate(parts, axis=1)


def onehot_rows(row_ids, first, height):
    width = row_ids.shape[1]
    sub = lax.broadcasted_iota(jnp.int32, (height, width), 0) + first
    return to_bf(row_ids == sub)


def norm_parts(out_b):
    values = out_b.astype(F32)
    centered = values - jnp.mean(values, axis=-1, keepdims=True)
    inv_std = lax.rsqrt(jnp.mean(centered * centered, axis=-1, keepdims=True) + NORM_EPS)
    return centered * inv_std, inv_std


def branch_forward(pre_act, w_two, gain, bias):
    pre_b = pre_act.astype(BF)
    pre_f = pre_b.astype(F32)
    sig = jax.nn.sigmoid(pre_f)
    act = (pre_f * sig).astype(BF)
    out_b = dot_nn(act, w_two).astype(BF)
    normed, inv_std = norm_parts(out_b)
    return normed * gain + bias, (pre_b, act, sig, normed, inv_std, out_b)


def branch_backward(d_branch, pre_b, act, sig, normed, inv_std, w_two, gain):
    d_norm = d_branch * gain
    mean_one = jnp.mean(d_norm, axis=-1, keepdims=True)
    mean_two = jnp.mean(d_norm * normed, axis=-1, keepdims=True)
    d_out = (inv_std * (d_norm - mean_one - normed * mean_two)).astype(BF)
    d_two = dot_tn(act, d_out)
    d_act = dot_nt(d_out, w_two).astype(BF)
    pre_f = pre_b.astype(F32)
    d_pre = (d_act.astype(F32) * sig * (1.0 + pre_f * (1.0 - sig))).astype(BF)
    d_gain = jnp.sum(d_branch * normed, axis=0, keepdims=True)
    d_bias = jnp.sum(d_branch, axis=0, keepdims=True)
    return d_pre, d_two, d_gain, d_bias


def load_weights(part_ref, layer, all_wts, norm_ref):
    norm = jnp.zeros((PART_ROWS - NORM_OFF, part_ref.shape[-1]), F32)
    for shard in range(part_ref.shape[0]):
        for ref, rows, off in zip(all_wts, SHARD_ROWS, SHARD_OFF):
            ref[layer, shard * rows:(shard + 1) * rows, :] = part_ref[shard, off:off + rows, :]
        norm += part_ref[shard, NORM_OFF:, :].astype(F32)
    norm_ref[layer] = norm[:8]


def cast_parts(master_refs, part_ref):
    dp = lax.axis_index('dp')
    layers, gains, lanes = master_refs[-1].shape
    width = part_ref.shape[-1]
    spot = lax.broadcasted_iota(jnp.int32, (lanes, width), 1) - lanes * dp
    place = to_bf(spot == lax.broadcasted_iota(jnp.int32, (lanes, width), 0))
    for layer in range(layers):
        for ref, rows, off in zip(master_refs, SHARD_ROWS, SHARD_OFF):
            part_ref[layer, off:off + rows, :] = ref[layer].astype(BF)
        norm = jnp.concatenate([master_refs[-1][layer], jnp.zeros((PART_ROWS - NORM_OFF - gains, lanes), F32)], axis=0)
        part_ref[layer, NORM_OFF:, :] = dot_nn(norm.astype(BF), place).astype(BF)


def peer_tile(me, offset, side):
    row = lax.rem(me // side + offset // side, side)
    col = lax.rem(lax.rem(me, side) + offset % side, side)
    return row * side + col


def greet(peers):
    barrier = pltpu.get_barrier_semaphore()
    for peer in peers:
        pl.semaphore_signal(barrier, inc=1, device_id=peer, device_id_type=MESH_ID)


def greeted(count):
    pl.semaphore_wait(pltpu.get_barrier_semaphore(), count)


def tile_peers(tiles):
    me = lax.axis_index('sp')
    dp = lax.axis_index('dp')
    side = int(tiles ** 0.5)
    return [(peer_tile(me, offset, side), dp) for offset in far_first(tiles)]


def slot_copy(src_ref, dst_ref, sample, spot, send_sem, recv_sem, peer, me, live):
    rows = pl.ds(0, live)
    return pltpu.make_async_remote_copy(src_ref=src_ref.at[peer[0], sample, rows], dst_ref=dst_ref.at[me, sample, rows], send_sem=send_sem.at[sample, spot], recv_sem=recv_sem.at[sample, spot], device_id=peer, device_id_type=MESH_ID)


def clear_spare(ref):
    first = LIVE // 16 * 16
    ref[:, :, first:, :] = jnp.zeros(ref.shape[:2] + (ref.shape[2] - first, ref.shape[3]), BF)


def slots_start(src_ref, dst_ref, sample, send_sem, recv_sem, self_sem, tiles, live=SLOTS):
    me = lax.axis_index('sp')
    pltpu.make_async_copy(src_ref.at[me, sample], dst_ref.at[me, sample], self_sem.at[sample]).start()
    for spot, peer in enumerate(tile_peers(tiles)):
        slot_copy(src_ref, dst_ref, sample, spot, send_sem, recv_sem, peer, me, live).start()


def slots_wait(src_ref, dst_ref, sample, send_sem, recv_sem, self_sem, tiles, live=SLOTS):
    me = lax.axis_index('sp')
    pltpu.make_async_copy(src_ref.at[me, sample], dst_ref.at[me, sample], self_sem.at[sample]).wait()
    for spot, peer in enumerate(tile_peers(tiles)):
        slot_copy(src_ref, dst_ref, sample, spot, send_sem, recv_sem, peer, me, live).wait()


def slots_wait_all(src_ref, dst_ref, samples, send_sem, recv_sem, self_sem, tiles):
    def one(sample, carry):
        slots_wait(src_ref, dst_ref, sample, send_sem, recv_sem, self_sem, tiles)
        return carry
    lax.fori_loop(0, samples, one, 0)


def shard_peers(count):
    me = lax.axis_index('sp')
    dp = lax.axis_index('dp')
    return [(me, lax.rem(dp + offset, count)) for offset in line_first(count)]


def shard_copy(src_ref, dst_ref, spot, send_sem, recv_sem, peer, scatter):
    dp = lax.axis_index('dp')
    src = src_ref.at[peer[1]] if scatter else src_ref
    return pltpu.make_async_remote_copy(src_ref=src, dst_ref=dst_ref.at[dp], send_sem=send_sem.at[spot], recv_sem=recv_sem.at[spot], device_id=peer, device_id_type=MESH_ID)


def shards_start(src_ref, dst_ref, send_sem, recv_sem, self_sem, count, scatter):
    dp = lax.axis_index('dp')
    pltpu.make_async_copy(src_ref.at[dp] if scatter else src_ref, dst_ref.at[dp], self_sem).start()
    for spot, peer in enumerate(shard_peers(count)):
        shard_copy(src_ref, dst_ref, spot, send_sem, recv_sem, peer, scatter).start()


def shards_wait(src_ref, dst_ref, send_sem, recv_sem, self_sem, count, scatter):
    dp = lax.axis_index('dp')
    pltpu.make_async_copy(src_ref.at[dp] if scatter else src_ref, dst_ref.at[dp], self_sem).wait()
    for spot, peer in enumerate(shard_peers(count)):
        shard_copy(src_ref, dst_ref, spot, send_sem, recv_sem, peer, scatter).wait()


def chunk_maps(degree, mask_rows, mask_col):
    chunk = mask_rows.shape[1]
    nodes = chunk // degree
    sub_w = lax.broadcasted_iota(jnp.int32, (nodes, chunk), 0) * degree
    lane_w = lax.broadcasted_iota(jnp.int32, (nodes, chunk), 1)
    wide = (lane_w >= sub_w) & (lane_w < sub_w + degree)
    sub_t = lax.broadcasted_iota(jnp.int32, (chunk, nodes), 0)
    lane_t = lax.broadcasted_iota(jnp.int32, (chunk, nodes), 1) * degree
    tall = (sub_t >= lane_t) & (sub_t < lane_t + degree)
    out = dict(tall=to_bf(tall), wide=to_bf(wide), sum=jnp.where(wide, mask_rows[:1], 0.0).astype(BF))
    if mask_col is not None:
        out['spread'] = jnp.where(tall, jnp.concatenate([mask_col] * (nodes // LANES), axis=1), 0.0).astype(BF)
    return out


def make_tables(tiles, slots, tile_nodes, send_ids, mask_ref, gcol_ref, grow_ref, nrow_ref, mcol_ref, mrow_ref, pack_ref):
    me = lax.axis_index('sp')
    ids = send_ids[...]
    edges = ids.shape[1]
    tile_of = ids // tile_nodes
    local = (ids - tile_of * tile_nodes).astype(F32)
    row = lax.broadcasted_iota(jnp.int32, (tiles, edges), 0)
    is_me = row == me
    own_tile = jnp.sum(jnp.where(is_me, tile_of, 0), axis=0, keepdims=True)
    own_local = jnp.sum(jnp.where(is_me, local, 0.0), axis=0, keepdims=True)
    own = to_f(own_tile == row)
    inc = to_f((tile_of == me) & jnp.logical_not(is_me))
    both = jnp.concatenate([own, inc], axis=0).astype(BF)
    rank = jnp.zeros((2 * tiles, edges), F32)
    step = 256
    for blk in range(edges // step):
        first = lax.broadcasted_iota(jnp.int32, (step, edges), 0) + blk * step
        second = lax.broadcasted_iota(jnp.int32, (step, edges), 1)
        rank += dot_nn(both[:, blk * step:(blk + 1) * step], to_bf(first < second))
    slot_id = jnp.where(is_me, own_local, rank[:tiles] + (row * slots + tile_nodes).astype(F32))
    gidx = jnp.sum(own * slot_id, axis=0, keepdims=True)
    grow_ref[...] = jnp.broadcast_to(gidx, grow_ref.shape).astype(jnp.int32)
    gcol_ref[...] = jnp.transpose(jnp.broadcast_to(gidx, (LANES, edges))).astype(jnp.int32)
    mask = jnp.concatenate([mask_ref[line:line + 1, :] for line in range(mask_ref.shape[0])], axis=1).astype(F32)
    mrow_ref[...] = jnp.broadcast_to(mask, mrow_ref.shape)
    mcol_ref[...] = jnp.transpose(jnp.broadcast_to(mask, (LANES, edges)))
    slot_row = lax.broadcasted_iota(jnp.int32, (slots, edges), 0).astype(F32)
    cols = []
    for peer in range(tiles):
        hit = (slot_row == rank[tiles + peer:tiles + peer + 1]) & (inc[peer:peer + 1] > 0.5)
        found = jnp.sum(jnp.where(hit, local[peer:peer + 1] + 1.0, 0.0), axis=1, keepdims=True) - 1.0
        cols.append(jnp.broadcast_to(found, (slots, LANES)))
    ncol_f = jnp.concatenate(cols, axis=0)
    ncol = ncol_f.astype(jnp.int32)
    nrow_ref[...] = jnp.transpose(ncol_f)[:8].astype(jnp.int32)
    pack_ref[...] = onehot_cols(ncol, 0, tile_nodes)


def pack_sample(sample, node, pack_ref, out_ref, tiles, slots):
    def pack(i, carry):
        rows = 4 * slots
        base = pl.multiple_of(i * rows, rows)
        got = dot_nn(pack_ref[pl.ds(base, rows), :], node).astype(BF)
        out_ref[pl.ds(i * 4, 4), sample] = got.reshape(4, slots, got.shape[1])
        return carry
    lax.fori_loop(0, tiles // 4, pack, 0)


def fill_rows(rows_ref, node, got, tile_nodes):
    rows_ref[:tile_nodes, :] = node
    rows_ref[tile_nodes:, :] = got.reshape(got.shape[0] * got.shape[1], got.shape[2])


def build_pick(gcol_ref, pick_ref):
    step = 128 * 3

    def build(i, carry):
        base = pl.multiple_of(i * step, step)
        pick_ref[pl.ds(base, step), :] = onehot_cols(gcol_ref[pl.ds(base, step), :], 0, pick_ref.shape[1])
        return carry
    lax.fori_loop(0, pick_ref.shape[0] // step, build, 0)


def fwd_sample(maps, v_c, e_c, pick_ref, rows_ref, wts, norm_ref):
    w_e1, w_e2, w_n1, w_n2 = wts
    width = e_c.shape[-1]
    w_edge, w_send, w_recv = (w_e1[i * width:(i + 1) * width, :] for i in range(w_e1.shape[0] // width))
    sent = dot_nn(pick_ref[...], rows_ref[...]).astype(BF)
    recv = dot_nn(maps['tall'], v_c).astype(BF)
    pre = dot_nn(e_c, w_edge) + dot_nn(sent, w_send) + dot_nn(recv, w_recv)
    rows = [norm_ref[i:i + 1, :] for i in range(len(SHARD_ROWS))]
    branch, edge_s = branch_forward(pre, w_e2[...], rows[0], rows[1])
    e_new = (e_c.astype(F32) + branch).astype(BF)
    sums = dot_nn(maps['sum'], e_new).astype(BF)
    pre_n = dot_nn(v_c, w_n1[:width, :]) + dot_nn(sums, w_n1[width:, :])
    branch_n, node_s = branch_forward(pre_n, w_n2[...], rows[2], rows[3])
    return e_new, sums, branch_n, edge_s, node_s


def share_ids(peers, mine_ref, wide, ids_ref, most_ref, send_sem, recv_sem, tile_nodes):
    me = lax.axis_index('sp')
    wide[me] = mine_ref[...]
    copies = [pltpu.make_async_remote_copy(src_ref=mine_ref, dst_ref=wide.at[me], send_sem=send_sem.at[spot], recv_sem=recv_sem.at[spot], device_id=peer, device_id_type=MESH_ID) for spot, peer in enumerate(peers)]
    for copy in copies:
        copy.start()
    for copy in copies:
        copy.wait()
    tiles, lines, lanes = wide.shape
    for line in range(lines):
        ids_ref[:, line * lanes:(line + 1) * lanes] = wide[:, line, :]
    tile_of = ids_ref[...] // tile_nodes
    row = lax.broadcasted_iota(jnp.int32, (tiles, lanes), 0)
    most = jnp.zeros((tiles, lanes), F32)
    for peer in range(tiles):
        count = jnp.sum(to_f(tile_of == peer), axis=1, keepdims=True)
        most = jnp.maximum(most, jnp.where(row == peer, 0.0, count))
    most_ref[...] = jnp.broadcast_to(jnp.max(most, axis=0, keepdims=True), most_ref.shape)


def open_kernel(cfg, shards, mine_ref, mask_ref, nodes_ref, node_ref, edge_ref, dnode_ref, dedge_ref, m_e1, m_e2, m_n1, m_n2, m_norm,
                vout_ref, he_ref, ye_ref, sum_ref, hn_ref, yn_ref, de_ref, dloc_ref, sloc_ref, grad_ref, grow_ref, nrow_ref, mcol_ref, mrow_ref, w_e1, w_e2, w_n1, w_n2, norm_ref, most_ref, recv_out,
                wide, ids_ref, gcol_ref, pick_ref, drop_ref, pack_ref, rows_ref, dpre_ref, e_two, v_two, out_buf, in_buf, next_buf, in_two, part_ref, gat_ref,
                send_a, recv_a, self_a, send_b, recv_b, self_b, send_c, recv_c, self_c, send_w, recv_w, self_w, send_x, recv_x, self_x, send_i, recv_i):
    tiles, slots, tile_nodes, degree = cfg
    samples = nodes_ref.shape[0]
    all_wts = (w_e1, w_e2, w_n1, w_n2)
    step = pl.program_id(0)
    weight_sems = ((send_w, recv_w, self_w), (send_x, recv_x, self_x))

    def take_weights(layer):
        shards_wait(part_ref.at[layer], gat_ref.at[layer], *weight_sems[layer], shards, False)
        load_weights(gat_ref.at[layer], layer, all_wts, norm_ref)

    @pl.when(step == 0)
    def _():
        plane = tile_peers(tiles)
        peers = plane + shard_peers(shards)
        clear_spare(in_buf)
        greet(peers)
        cast_parts((m_e1, m_e2, m_n1, m_n2, m_norm), part_ref)
        greeted(len(peers))
        share_ids(plane, mine_ref, wide, ids_ref, most_ref, send_i, recv_i, tile_nodes)
        make_tables(tiles, slots, tile_nodes, ids_ref, mask_ref, gcol_ref, grow_ref, nrow_ref, mcol_ref, mrow_ref, pack_ref)
        for sample in range(samples):
            pack_sample(sample, nodes_ref[sample], pack_ref, out_buf, tiles, slots)
            slots_start(out_buf, in_buf, sample, send_a, recv_a, self_a, tiles, LIVE)
        for layer, sems in enumerate(weight_sems):
            shards_start(part_ref.at[layer], gat_ref.at[layer], *sems, shards, False)
        build_pick(gcol_ref, pick_ref)
        build_drop(grow_ref, drop_ref)
        grad_ref[...] = jnp.zeros_like(grad_ref)
        take_weights(0)

    @pl.when(step == samples - 1)
    def _():
        take_weights(1)

    @pl.when(step < samples)
    def _():
        slots_wait(out_buf, in_buf, step, send_a, recv_a, self_a, tiles, LIVE)
        fill_rows(rows_ref, node_ref[0], in_buf[:, step], tile_nodes)
        node, edge = node_ref[0], edge_ref[0]
        e_new, sums, branch_n, edge_s, node_s = fwd_sample(chunk_maps(degree, mrow_ref[...], None), node, edge, pick_ref, rows_ref, [ref.at[0] for ref in all_wts], norm_ref.at[0])
        v_new = (node.astype(F32) + branch_n).astype(BF)
        for ref, value in ((he_ref, edge_s[0]), (ye_ref, edge_s[-1]), (sum_ref, sums), (hn_ref, node_s[0]), (yn_ref, node_s[-1]), (vout_ref, v_new)):
            ref[0] = value
        e_two[step] = e_new
        v_two[step] = v_new
        pack_sample(step, v_new, pack_ref, next_buf, tiles, slots)
        slots_start(next_buf, in_two, step, send_b, recv_b, self_b, tiles)

    @pl.when(step >= samples)
    def _():
        sample = step - samples
        slots_wait(next_buf, in_two, sample, send_b, recv_b, self_b, tiles)
        node, edge = v_two[sample], e_two[sample]
        fill_rows(rows_ref, node, in_two[:, sample], tile_nodes)
        wts, norm = [ref.at[1] for ref in all_wts], norm_ref.at[1]
        maps = chunk_maps(degree, mrow_ref[...], mcol_ref[...])
        e_new, sums, branch_n, edge_s, node_s = fwd_sample(maps, node, edge, pick_ref, rows_ref, wts, norm)
        back_sample(maps, node, edge, sums, edge_s[:-1], node_s[:-1], dnode_ref[0].astype(F32), dedge_ref, wts, norm, grad_ref, dpre_ref, de_ref, dloc_ref)
        back_pack(dpre_ref, drop_ref, sloc_ref, out_buf, sample, tiles, slots, tile_nodes)
        slots_start(out_buf, recv_out, sample, send_c, recv_c, self_c, tiles)

    @pl.when(step == 2 * samples - 1)
    def _():
        slots_wait_all(out_buf, recv_out, samples, send_c, recv_c, self_c, tiles)


def back_sample(maps, v_c, e_c, sums, edge_s, node_s, d_node, dedge_ref, wts, norm_ref, grad_ref, dpre_ref, de_ref, dloc_ref):
    w_e1, w_e2, w_n1, w_n2 = wts
    width = e_c.shape[-1]
    w_edge, w_send, w_recv = (w_e1[i * width:(i + 1) * width, :] for i in range(w_e1.shape[0] // width))
    d_pre_n, d_wn2, d_gain_n, d_bias_n = branch_backward(d_node, *node_s, w_n2[...], norm_ref[2:3, :])
    d_in_v = dot_nt(d_pre_n, w_n1[:width, :])
    d_sum = dot_nt(d_pre_n, w_n1[width:, :]).astype(BF)
    d_res = (dedge_ref[0].astype(F32) + dot_nn(maps['spread'], d_sum)).astype(BF).astype(F32)
    d_pre, d_we2, d_gain_e, d_bias_e = branch_backward(d_res, *edge_s, w_e2[...], norm_ref[0:1, :])
    dpre_ref[...] = d_pre
    de_ref[0] = (d_res + dot_nt(d_pre, w_edge)).astype(BF)
    recv = split_three(dot_nn(maps['wide'], d_pre))
    dloc_ref[0] = d_node + d_in_v + sum(dot_nt(piece, w_recv) for piece in recv)
    blocks = [dot_tn(e_c, d_pre), None, sum(dot_tn(v_c, piece) for piece in recv), d_we2, dot_tn(v_c, d_pre_n), dot_tn(sums, d_pre_n), d_wn2]
    for i, block in enumerate(blocks):
        if block is not None:
            grad_ref[i * width:(i + 1) * width, :] += block
    rows = [d_gain_e, d_bias_e, d_gain_n, d_bias_n]
    grad_ref[len(blocks) * width:, :] += jnp.concatenate(rows + [jnp.zeros((len(rows), width), F32)], axis=0)


def back_pack(dpre_ref, drop_ref, sloc_ref, send_buf, step, tiles, slots, tile_nodes):
    sloc_ref[0] = dot_nn(drop_ref[:tile_nodes, :], dpre_ref[...])

    def pack(i, carry):
        rows = 4 * slots
        base = pl.multiple_of(tile_nodes + i * rows, 64)
        got = dot_nn(drop_ref[pl.ds(base, rows), :], dpre_ref[...]).astype(BF)
        send_buf[pl.ds(i * 4, 4), step] = got.reshape(4, slots, got.shape[1])
        return carry
    lax.fori_loop(0, tiles // 4, pack, 0)


def build_drop(grow_ref, drop_ref):
    step = 256

    def build(i, carry):
        base = pl.multiple_of(i * step, step)
        drop_ref[pl.ds(base, step), :] = onehot_rows(grow_ref[0:1, :], base, step)
        return carry
    lax.fori_loop(0, drop_ref.shape[0] // step, build, 0)


def again(pre_b, out_b):
    pre_f = pre_b.astype(F32)
    sig = jax.nn.sigmoid(pre_f)
    act = (pre_f * sig).astype(BF)
    normed, inv_std = norm_parts(out_b)
    return pre_b, act, sig, normed, inv_std


def close_kernel(cfg, shards, node_ref, edge_ref, he_ref, ye_ref, sum_ref, hn_ref, yn_ref, dedge_ref, nodes_ref, grow_ref, mrow_ref, mcol_ref, nrow_ref, w_e1, w_e2, w_n1, w_n2, norms_ref, vall_ref, dlall_ref, slall_ref, recv_ref, gtwo_ref,
                 de_ref, dv_out, both_ref,
                 grad_ref, dloc_ref, sloc_ref, in_buf, part_buf, drop_ref, dpre_ref, fold_ref, gsend_ref, dv_ref, full_ref, send_buf, half_buf, x_buf, own, rs_buf, piece, ws_buf, gath,
                 send_b, recv_b, self_b, send_w, recv_w, self_w, s0, r0, s1, r1, s2, r2, s3, r3, s4, r4, s5, r5, self_s):
    tiles, slots, tile_nodes, degree = cfg
    samples = vall_ref.shape[0]
    step = pl.program_id(0)
    me = lax.axis_index('sp')
    dp = lax.axis_index('dp')
    core = lax.rem(dp, 2)
    chip = dp // 2
    chips = shards // 2
    plane = tile_peers(tiles)
    others = shard_peers(shards)

    @pl.when(step == 0)
    def _():
        clear_spare(in_buf)
        greet(plane + others)
        fold_ref[...] = onehot_rows(nrow_ref[:1], 0, tile_nodes)
        gsend_ref[...] = jnp.zeros_like(gsend_ref)

        def finish(sample, carry):
            dv_ref[sample] = finish_sample(vall_ref[sample], dlall_ref[sample], slall_ref[sample], recv_ref[:, sample], fold_ref, gsend_ref, w_e1.at[1])
            return carry
        lax.fori_loop(0, samples, finish, 0)
        lay_grads(full_ref, gtwo_ref, gsend_ref)
        greeted(len(plane + others))
        shards_start(full_ref, part_buf, send_w, recv_w, self_w, shards, True)
        build_drop(grow_ref, drop_ref)
        grad_ref[...] = jnp.zeros_like(grad_ref)

    maps = chunk_maps(degree, mrow_ref[...], mcol_ref[...])
    edge_s = again(he_ref[0], ye_ref[0])
    node_s = again(hn_ref[0], yn_ref[0])
    back_sample(maps, node_ref[0], edge_ref[0], sum_ref[0], edge_s, node_s, dv_ref[step].astype(F32), dedge_ref, [ref.at[0] for ref in (w_e1, w_e2, w_n1, w_n2)], norms_ref.at[0], grad_ref, dpre_ref, de_ref, dloc_ref.at[pl.ds(step, 1)])
    back_pack(dpre_ref, drop_ref, sloc_ref.at[pl.ds(step, 1)], send_buf, step, tiles, slots, tile_nodes)
    slots_start(send_buf, in_buf, step, send_b, recv_b, self_b, tiles, LIVE)

    @pl.when(step == samples - 1)
    def _():
        away = line_first(chips)
        spots = [lax.rem(chip + offset, chips) for offset in away]
        line = [(me, spot * 2 + core) for spot in spots]
        shards_wait(full_ref, part_buf, send_w, recv_w, self_w, shards, True)
        gsend_ref[...] = jnp.zeros_like(gsend_ref)
        lay_grads(full_ref, grad_ref, gsend_ref)
        pair = [pltpu.make_async_remote_copy(src_ref=full_ref.at[spot * 2 + 1 - core], dst_ref=half_buf.at[spot], send_sem=s0.at[k], recv_sem=r0.at[k], device_id=(me, dp + 1 - 2 * core), device_id_type=MESH_ID) for k, spot in enumerate(spots + [chip])]
        for copy in pair:
            copy.start()
        own[1] = sum(part_buf[shard] for shard in range(shards))
        hops = []
        for k, spot in enumerate(spots):
            pair[k].wait()
            half_buf[spot] += full_ref[spot * 2 + core]
            hop = pltpu.make_async_remote_copy(src_ref=half_buf.at[spot], dst_ref=x_buf.at[chip], send_sem=s1.at[k], recv_sem=r1.at[k], device_id=line[k], device_id_type=MESH_ID)
            hop.start()
            hops.append(hop)
        pair[-1].wait()

        def finish(sample, carry):
            slots_wait(send_buf, in_buf, sample, send_b, recv_b, self_b, tiles, LIVE)
            dv_out[sample] = finish_sample(nodes_ref[sample], dloc_ref[sample], sloc_ref[sample], in_buf[:, sample], fold_ref, gsend_ref, w_e1.at[0])
            return carry
        lax.fori_loop(0, samples, finish, 0)
        own[2] = gsend_ref[...]
        total = half_buf[chip] + full_ref[dp]
        for hop, offset in zip(hops, away):
            hop.wait()
            total += x_buf[lax.rem(chip + chips - offset, chips)]
        own[0] = total

        rows = FULL_ROWS // tiles
        here = pl.ds(pl.multiple_of(me * rows, rows), rows)
        cuts = [pltpu.make_async_remote_copy(src_ref=own.at[:, pl.ds(pl.multiple_of(peer[0] * rows, rows), rows)], dst_ref=rs_buf.at[me], send_sem=s2.at[k], recv_sem=r2.at[k], device_id=peer, device_id_type=MESH_ID) for k, peer in enumerate(plane)]
        for cut in cuts:
            cut.start()
        for cut in cuts:
            cut.wait()
        piece[...] = own[:, here, :] + sum(rs_buf[lax.rem(me + offset, tiles)] for offset in range(1, tiles))
        shards_start(piece.at[2], ws_buf, s4, r4, self_s, shards, False)
        sends = [pltpu.make_async_remote_copy(src_ref=piece.at[:2], dst_ref=gath.at[:2, here], send_sem=s3.at[k], recv_sem=r3.at[k], device_id=peer, device_id_type=MESH_ID) for k, peer in enumerate(plane)]
        for send in sends:
            send.start()
        shards_wait(piece.at[2], ws_buf, s4, r4, self_s, shards, False)
        mine = rs_buf.at[me, 2]
        mine[...] = sum(ws_buf[shard] for shard in range(shards))
        more = [pltpu.make_async_remote_copy(src_ref=mine, dst_ref=gath.at[2, here], send_sem=s5.at[k], recv_sem=r5.at[k], device_id=peer, device_id_type=MESH_ID) for k, peer in enumerate(plane)]
        for send in more:
            send.start()
        gath[:2, here, :] = piece[:2]
        gath[2, here, :] = mine[...]
        for send in sends + more:
            send.wait()
        both_ref[...] = gath[...]


def finish_sample(node, d_loc, s_loc, got, fold_ref, gsend_ref, w_e1):
    width = node.shape[-1]
    total = s_loc + dot_nn(fold_ref[...], got.reshape(got.shape[0] * got.shape[1], width))
    pieces = split_three(total)
    w_send = w_e1[width:2 * width, :]
    gsend_ref[...] += sum(dot_tn(node, piece) for piece in pieces)
    return (d_loc + sum(dot_nt(piece, w_send) for piece in pieces)).astype(BF)


def lay_grads(full_ref, grad_ref, gsend_ref):
    shards, rows_all, width = full_ref.shape
    sources = ((grad_ref, 0), (gsend_ref, 0), (grad_ref, 2 * width))
    for shard in range(shards):
        row = SHARD_ROWS[0] * shard
        last = row + SHARD_ROWS[0]
        spot = 0
        while row < last:
            block = row // width
            count = min(last, (block + 1) * width) - row
            ref, base = sources[block]
            base = base + row - block * width
            full_ref[shard, spot:spot + count, :] = ref[base:base + count, :]
            row += count
            spot += count
        first = 3 * width
        for rows, off in zip(SHARD_ROWS[1:], SHARD_OFF[1:]):
            full_ref[shard, off:off + rows, :] = grad_ref[first + shard * rows:first + (shard + 1) * rows, :]
            first += rows * shards
        full_ref[shard, NORM_OFF:NORM_OFF + 8, :] = grad_ref[first:first + 8, :]
        full_ref[shard, NORM_OFF + 8:, :] = jnp.zeros((rows_all - NORM_OFF - 8, width), F32)


def adam_kernel(shards, both_ref, dnode_ref, dedge_ref, *refs):
    count = (len(refs) - 7) // 2
    node_out, edge_out = refs[count:count + 2]
    refs = refs[:count] + refs[count + 2:]
    extra, node_buf, edge_buf, sems_in, sems_out = refs[-5:]
    moves = []
    for k, (src, buf, dst) in enumerate(((dedge_ref, edge_buf, edge_out), (dnode_ref, node_buf, node_out))):
        for sample in range(src.shape[0]):
            moves.append((pltpu.make_async_copy(src.at[sample], buf.at[sample], sems_in.at[k, sample]), pltpu.make_async_copy(buf.at[sample], dst.at[sample], sems_out.at[k, sample])))
    for load, store in moves:
        load.start()
    for load, store in moves:
        load.wait()
        store.start()
    dp = lax.axis_index('dp')
    masters, ones, twos, new_masters, new_ones, new_twos = (refs[i:i + 5] for i in range(0, len(refs) - 5, 5))
    layers, gains, lanes = masters[-1].shape
    norm = both_ref[:2, NORM_OFF:NORM_OFF + gains, :lanes]
    for shard in range(1, shards):
        norm = jnp.where(dp == shard, both_ref[:2, NORM_OFF:NORM_OFF + gains, shard * lanes:(shard + 1) * lanes], norm)
    sums = [both_ref[:2, off:off + rows, :] for rows, off in zip(SHARD_ROWS, SHARD_OFF)] + [norm]
    rows, width = SHARD_ROWS[0], extra.shape[1]
    extra[...] = jnp.zeros_like(extra)
    extra[width:2 * width, :] = both_ref[2]
    sums[0] = jnp.stack([sums[0][0] + extra[pl.ds(pl.multiple_of(dp * rows, rows), rows), :], sums[0][1]])
    for slot, grad_sum in enumerate(sums):
        results = adamw_update(masters[slot][...], grad_sum, ones[slot][...], twos[slot][...])
        for ref, value in zip((new_masters[slot], new_ones[slot], new_twos[slot]), results):
            ref[...] = value
    for load, store in moves:
        store.wait()


def whole(shape):
    zeros = (0,) * len(shape)
    return pl.BlockSpec(shape, lambda s: zeros)


def per_sample(rows, width):
    return pl.BlockSpec((1, rows, width), lambda s: (s, 0, 0))


def slot_spec(tiles, slots, width):
    return pl.BlockSpec((tiles, 1, slots, width), lambda s: (0, s, 0, 0))


PARAMS = dict(vmem_limit_bytes=63 << 20)


def grid_params():
    return pltpu.CompilerParams(dimension_semantics=("arbitrary",), **PARAMS)


def remote_params(number):
    return pltpu.CompilerParams(collective_id=number, has_side_effects=True, **PARAMS)


def slot_sems(samples, tiles):
    return [pltpu.SemaphoreType.DMA((samples, tiles)), pltpu.SemaphoreType.DMA((samples, tiles)), pltpu.SemaphoreType.DMA((samples,))]


def shard_sems(shards):
    return [pltpu.SemaphoreType.DMA((shards,)), pltpu.SemaphoreType.DMA((shards,)), pltpu.SemaphoreType.DMA]


def solution(mesh):
    lat_spec = P('dp', 'sp', None)
    edge_spec = P('sp')
    mat_spec = P(None, 'dp', None)
    norm_spec = P(None, None, 'dp')
    param_specs = (mat_spec, mat_spec, mat_spec, mat_spec, norm_spec)
    tiles = mesh.shape['sp']
    dp_size = mesh.shape['dp']

    def spread(value, axis):
        count = mesh.shape[axis]
        return lax.all_to_all(jnp.broadcast_to(value[None], (count,) + value.shape), axis, 0, 0, tiled=True)

    def join(stacked, dim):
        moved = jnp.moveaxis(stacked, 0, dim)
        return moved.reshape(moved.shape[:dim] + (moved.shape[dim] * moved.shape[dim + 1],) + moved.shape[dim + 2:])

    def scatter_sum(value, axis, dim):
        count = mesh.shape[axis]
        split = value.reshape(value.shape[:dim] + (count, value.shape[dim] // count) + value.shape[dim + 1:])
        return jnp.sum(lax.all_to_all(jnp.moveaxis(split, dim, 0), axis, 0, 0, tiled=True), axis=0)

    def gather_weights(masters, layer_idx):
        mat_list = [join(spread(master[layer_idx].astype(BF), 'dp'), 0) for master in masters[:4]]
        norm_rows = join(spread(masters[4][layer_idx].astype(BF), 'dp'), 1).astype(F32)
        return mat_list[0], mat_list[1], mat_list[2], mat_list[3], norm_rows

    def reduce_grads(grads):
        parts = [scatter_sum(grad_full, 'dp', 0) for grad_full in grads[:4]] + [scatter_sum(grads[4], 'dp', 1)]
        return tuple(jnp.sum(spread(part, 'sp'), axis=0) for part in parts)

    def general_step(node_lat, edge_lat, senders, edge_mask, node_cot, edge_cot, masters):
        batch_size, tile_nodes, lat_width = node_lat.shape
        degree = edge_lat.shape[1] // tile_nodes
        layers = masters[0].shape[0]
        mask_f = edge_mask.astype(F32).reshape(tile_nodes, degree)
        mask_b = mask_f.astype(BF)
        node_x = node_lat
        edge_x = edge_lat.reshape(batch_size, tile_nodes, degree, lat_width)
        records = []
        for layer_idx in range(layers):
            layer_wts = gather_weights(masters, layer_idx)
            node_all = join(spread(node_x, 'sp'), 1)
            node_new, edge_new, saved = layer_forward(node_x, node_all, edge_x, senders, mask_b, layer_wts)
            records.append((node_x, edge_x, saved))
            node_x = node_new
            edge_x = edge_new
        d_node = node_cot
        d_edge = edge_cot.reshape(batch_size, tile_nodes, degree, lat_width)
        grads_rev = []
        for layer_idx in reversed(range(layers)):
            layer_wts = gather_weights(masters, layer_idx)
            node_in, edge_in, saved = records[layer_idx]
            d_local, scattered, d_edge, grads = layer_backward(d_node, d_edge, node_in, edge_in, senders, mask_f, saved, layer_wts, tile_nodes * tiles)
            returned = scatter_sum(scattered, 'sp', 1)
            d_node = (d_local + returned).astype(BF)
            grads_rev.append(reduce_grads(grads))
        layer_grads = grads_rev[::-1]
        sums = tuple(jnp.stack([per_layer[slot] for per_layer in layer_grads], axis=0) for slot in range(5))
        return sums + (d_node, d_edge.reshape(edge_lat.shape))

    def compact_step(node_lat, edge_lat, senders, edge_mask, node_cot, edge_cot, masters):
        samples, tile_nodes, width = node_lat.shape
        edges = edge_lat.shape[1]
        cfg = (tiles, SLOTS, tile_nodes, edges // tile_nodes)
        cols = tile_nodes + tiles * SLOTS
        layers = masters[0].shape[0]
        sd = jax.ShapeDtypeStruct
        vmem = pl.BlockSpec(memory_space=pltpu.VMEM)
        hbm = pl.BlockSpec(memory_space=pl.ANY)
        last = samples - 1

        def early(rows):
            return pl.BlockSpec((1, rows, width), lambda s: (jnp.minimum(s, last), 0, 0))

        def late(rows):
            return pl.BlockSpec((1, rows, width), lambda s: (jnp.maximum(s - samples, 0), 0, 0))

        node_b = sd((samples, tile_nodes, width), BF)
        node_f = sd((samples, tile_nodes, width), F32)
        edge_b = sd((samples, edges, width), BF)
        grad_f = sd((GRAD_ROWS, width), F32)
        slot_b = sd((tiles, samples, SLOTS, width), BF)
        full_f = sd((dp_size, FULL_ROWS, width), F32)
        grow_b = sd((8, edges), jnp.int32)
        nrow_b = sd((8, tiles * SLOTS), jnp.int32)
        mcol_b = sd((edges, LANES), F32)
        mrow_b = sd((8, edges), F32)
        lines = edges // LANES
        most_b = sd((8, LANES), F32)
        few = pltpu.SemaphoreType.DMA((tiles,))
        weights_b = [sd((layers, rows * dp_size, width), BF) for rows in SHARD_ROWS] + [sd((layers, 8, width), F32)]

        def full_specs(shapes):
            return [whole(item.shape) for item in shapes]

        def scratch(shape, kind=BF):
            return pltpu.VMEM(shape, kind)

        slot_v = scratch(slot_b.shape)
        drop_v = scratch((cols, edges))
        dpre_v = scratch((edges, width))
        fold_v = scratch((tile_nodes, tiles * SLOTS))
        gsend_v = scratch((width, width), F32)
        tables_b = [grow_b, nrow_b, mcol_b, mrow_b]
        outs = pl.pallas_call(
            functools.partial(open_kernel, cfg, dp_size), grid=(2 * samples,),
            out_shape=[node_b, edge_b, edge_b, node_b, node_b, node_b, edge_b, node_f, node_f, grad_f] + tables_b + weights_b + [most_b, slot_b],
            in_specs=[whole((lines, LANES)), whole((lines, LANES)), whole(node_b.shape), early(tile_nodes), early(edges), late(tile_nodes), late(edges)] + [whole(master.shape) for master in masters],
            out_specs=[early(tile_nodes), early(edges), early(edges), early(tile_nodes), early(tile_nodes), early(tile_nodes), late(edges), late(tile_nodes), late(tile_nodes)] + full_specs([grad_f] + tables_b + weights_b + [most_b]) + [hbm],
            scratch_shapes=[scratch((tiles, lines, LANES), jnp.int32), scratch((tiles, edges), jnp.int32), scratch(mcol_b.shape, jnp.int32), scratch((edges, cols)), drop_v, scratch((tiles * SLOTS, tile_nodes)), scratch((cols, width)), dpre_v, scratch(edge_b.shape), scratch(node_b.shape),
                            slot_v, slot_v, slot_v, slot_v, scratch((layers, PART_ROWS, width)), scratch((layers, dp_size, PART_ROWS, width))]
            + slot_sems(samples, tiles) + slot_sems(samples, tiles) + slot_sems(samples, tiles) + shard_sems(dp_size) + shard_sems(dp_size) + [few, few],
            name='open', compiler_params=remote_params(1))(senders.reshape(lines, LANES), edge_mask.reshape(lines, LANES), node_lat, node_lat, edge_lat, node_cot, edge_cot, *masters)
        v_one, h_e, y_e, sums, h_n, y_n, d_edge, d_loc, s_loc, grad_two, grow, nrow, mcol, mrow = outs[:14]
        weights = outs[14:-2]
        most, recv_three = outs[-2:]

        node_s = per_sample(tile_nodes, width)
        edge_s = per_sample(edges, width)
        rows = FULL_ROWS // tiles
        groups = layers + 1
        both_f = (groups, FULL_ROWS, width)
        half_v = scratch((dp_size // 2, FULL_ROWS, width), F32)
        d_edge0, d_node, both = pl.pallas_call(
            functools.partial(close_kernel, cfg, dp_size), grid=(samples,),
            out_shape=(edge_b, node_b, sd(both_f, F32)),
            in_specs=[node_s, edge_s, edge_s, edge_s, node_s, node_s, node_s, edge_s] + full_specs([node_b, grow_b, mrow_b, mcol_b, nrow_b] + weights_b + [node_b, node_f, node_f, slot_b, grad_f]),
            out_specs=[edge_s] + full_specs([node_b, sd(both_f, F32)]),
            scratch_shapes=[scratch(grad_f.shape, F32), scratch(node_f.shape, F32), scratch(node_f.shape, F32), slot_v, scratch(full_f.shape, F32), drop_v, dpre_v, fold_v, gsend_v, scratch(node_b.shape), scratch(full_f.shape, F32), slot_v,
                            half_v, half_v, scratch(both_f, F32), scratch((tiles, groups, rows, width), F32), scratch((groups, rows, width), F32), scratch((dp_size, rows, width), F32), scratch(both_f, F32)]
            + slot_sems(samples, tiles) + shard_sems(dp_size) + [few] * 12 + [pltpu.SemaphoreType.DMA],
            name='close', compiler_params=remote_params(2))(node_lat, edge_lat, h_e, y_e, sums, h_n, y_n, d_edge, node_lat, grow, mrow, mcol, nrow, *weights, v_one, d_loc, s_loc, recv_three, grad_two)
        return most[0, 0] <= LIVE, both, d_node, d_edge0

    def general_both(*args):
        result = general_step(*args)
        lanes = result[4].shape[-1]
        first = result[0]
        norm = lax.dynamic_update_slice(jnp.zeros((first.shape[0], FULL_ROWS - NORM_OFF, first.shape[-1]), F32), result[4], (0, 0, lax.axis_index('dp') * lanes))
        both = jnp.concatenate(result[:4] + (norm,), axis=1)
        return jnp.concatenate([both, jnp.zeros_like(both[:1])], axis=0), result[5], result[6]

    def train_step(node_lat, edge_lat, senders, edge_mask, node_cot, edge_cot, w_edge1, w_edge2, w_node1, w_node2, norm_par, mom_edge1, mom_edge2, mom_node1, mom_node2, mom_norm, vel_edge1, vel_edge2, vel_node1, vel_node2, vel_norm):
        masters = (w_edge1, w_edge2, w_node1, w_node2, norm_par)
        moments_one = (mom_edge1, mom_edge2, mom_node1, mom_node2, mom_norm)
        moments_two = (vel_edge1, vel_edge2, vel_node1, vel_node2, vel_norm)
        tile_nodes = node_lat.shape[1]
        vmem = pl.BlockSpec(memory_space=pltpu.VMEM)
        hbm = pl.BlockSpec(memory_space=pl.ANY)

        def unsettled(state):
            return jnp.logical_not(state[0])

        def settle(state):
            held = tuple(master * jnp.logical_not(state[0]).astype(F32) for master in masters)
            args = (node_lat, edge_lat, senders, edge_mask, node_cot, edge_cot, held)
            return (True,) + jax.tree.map(row_major, general_both(*jax.tree.map(row_major, args)))

        state = compact_step(node_lat, edge_lat, senders, edge_mask, node_cot, edge_cot, masters)
        both, d_node, d_edge = lax.while_loop(unsettled, settle, state)[1:]
        state = masters + moments_one + moments_two
        passed = [jax.ShapeDtypeStruct(item.shape, item.dtype) for item in (d_node, d_edge)]
        width = w_edge2.shape[-1]
        sems = pltpu.SemaphoreType.DMA((2, d_node.shape[0]))
        new_state = pl.pallas_call(
            functools.partial(adam_kernel, dp_size), out_shape=passed + [jax.ShapeDtypeStruct(item.shape, F32) for item in state],
            in_specs=[vmem, hbm, hbm] + [vmem] * len(state), out_specs=[hbm, hbm] + [vmem] * len(state),
            scratch_shapes=[pltpu.VMEM((w_edge1.shape[1] * dp_size, width), F32), pltpu.VMEM(d_node.shape, BF), pltpu.VMEM(d_edge.shape, BF), sems, sems],
            name='adam', compiler_params=pltpu.CompilerParams(**PARAMS))(both, d_node, d_edge, *state)
        return tuple(new_state[2:]) + tuple(new_state[:2])

    return jax.shard_map(train_step, mesh=mesh, in_specs=(lat_spec, lat_spec, edge_spec, edge_spec, lat_spec, lat_spec) + param_specs + param_specs + param_specs, out_specs=param_specs + param_specs + param_specs + (lat_spec, lat_spec), check_vma=False)
```
